32 devices in a mesh: shard: 4 (over y, x), rep: 8 (over z, core).
Axes of the slice: x: 2, y: 2, z: 4, core: 2. Of those that a mesh axis runs over, the one named last changes fastest.
Arguments:
- activations: bfloat16 [8, 512, 2048], P('rep', 'shard'), may hold values from -16 to 16
- segments: int32 [8, 512], P('rep'), may hold values from 0 to 3, never falling along the last dimension, each value on 1 to 256 neighbouring positions
- attn_gain: float32 [2048], replicated, may hold values from 0.25 to 1.75
- query_weight: bfloat16 [2048, 2048], P('shard'), may hold values from -0.125 to 0.125
- key_weight: bfloat16 [2048, 1024], P('shard'), may hold values from -0.125 to 0.125
- value_weight: bfloat16 [2048, 1024], P('shard'), may hold values from -0.125 to 0.125
- query_gain: float32 [128], replicated, may hold values from 0.5 to 5.5
- key_gain: float32 [128], replicated, may hold values from 0.5 to 5.5
- out_weight: bfloat16 [2048, 2048], P('shard'), may hold values from -0.75 to 0.75
- mlp_gain: float32 [2048], replicated, may hold values from 0.25 to 1.75
- gate_weight: bfloat16 [2048, 6144], P('shard'), may hold values from -0.125 to 0.125
- up_weight: bfloat16 [2048, 6144], P('shard'), may hold values from -0.125 to 0.125
- down_weight: bfloat16 [6144, 2048], P('shard'), may hold values from -0.078125 to 0.078125
- cotangent: bfloat16 [8, 512, 2048], P('rep', 'shard'), may hold values from -11.1 to 11.1
Outputs:
- output: bfloat16 [8, 512, 2048], P('rep', 'shard')
- grad_input: float32 [8, 512, 2048], P('rep', 'shard')
- grad_attn_gain: float32 [2048], replicated
- grad_query_weight: float32 [2048, 2048], P('shard')
- grad_key_weight: float32 [2048, 1024], P('shard')
- grad_value_weight: float32 [2048, 1024], P('shard')
- grad_query_gain: float32 [128], replicated
- grad_key_gain: float32 [128], replicated
- grad_out_weight: float32 [2048, 2048], P('shard')
- grad_mlp_gain: float32 [2048], replicated
- grad_gate_weight: float32 [2048, 6144], P('shard')
- grad_up_weight: float32 [2048, 6144], P('shard')
- grad_down_weight: float32 [6144, 2048], P('shard')
The draws below stay inside these ranges and needn't reach their ends.
Inputs may be any that keep to these rules, and one draw needn't show every extreme that they name: `segments`: within each sequence the document numbers never fall; each document has 1 to 256 tokens, and one has exactly 256.
All inputs are finite; a program needn't handle non-finite values.
Results may differ from the reference program's by a relative error of at most 0.02.
The reference program's roundings to bfloat16 on the way count: a program that leaves them out, or rounds other values in their place, can miss the bound.
Values may be sent and summed in bfloat16 or wider, within the bound.
A program may use at most 384 MiB of HBM per device.

```python
import math
import jax
import jax.numpy as jnp
import numpy as np
from jax import lax

D = 2048
HQ = 16
HK = 8
HD = 128
FF = 6144
LEN = 512
SEQS = 8


def draw_activations(key, part):
    noise_key = jax.random.fold_in(key, 0)
    col_key = jax.random.fold_in(key, 2)
    full_shape = (SEQS, LEN, D)
    noise_part = jax.random.truncated_normal(noise_key, -4.0, 4.0, full_shape, jnp.float32)
    col_scale = jnp.exp(jax.random.uniform(col_key, (1, 1, D), jnp.float32, math.log(0.5), math.log(2.0)))
    return (noise_part * col_scale).astype(jnp.bfloat16)


def head_gains(key):
    return jnp.exp(jax.random.uniform(key, (HD,), jnp.float32, math.log(0.5), math.log(2.0)))


def draw_query_gain(key, part):
    return head_gains(jax.random.fold_in(key, 11))


def draw_key_gain(key, part):
    return head_gains(jax.random.fold_in(key, 23))


def draw_cotangent(key, part):
    noise_key = jax.random.fold_in(jax.random.fold_in(key, 37), 0)
    full_shape = (SEQS, LEN, D)
    seq_rise = 0.6 + 1.2 * jnp.arange(SEQS, dtype=jnp.float32) / max(SEQS - 1, 1)
    pos_rise = 0.6 + 1.2 * jnp.arange(LEN, dtype=jnp.float32) / max(LEN - 1, 1)
    rising = seq_rise[:, None, None] * pos_rise[None, :, None]
    return (rising * jax.random.truncated_normal(noise_key, -3.0, 3.0, full_shape, jnp.float32)).astype(jnp.bfloat16)


def levels(stream_key, extent, cuts, low, largest):
    loudness = 1.0
    for axis_at, parts in cuts:
        draws = jax.random.uniform(jax.random.fold_in(jax.random.fold_in(stream_key, 6), axis_at), (parts,), jnp.float32, low / len(cuts), largest / len(cuts))
        loudness = loudness * jnp.repeat(jnp.exp(draws), extent[axis_at] // parts).reshape((-1,) + (1,) * (len(extent) - 1 - axis_at))
    return loudness


def length_profile(amount, total, limit, slope):
    weights = [(1 << 20) // math.isqrt(standing ** slope) + 1 for standing in range(2, amount + 1)]
    surplus, given = total - limit - (amount - 1), [1] * (amount - 1)
    while surplus > 0:
        free = [i for i in range(amount - 1) if given[i] < limit]
        mass, remaining = sum([weights[i] for i in free]), surplus
        for i in free:
            extra = min(limit - given[i], max(1, remaining * weights[i] // mass), surplus)
            given[i] = given[i] + extra
            surplus = surplus - extra
    return np.array([limit] + given)


def ragged_sizes(key, number_of, total, most, lean):
    if number_of == 2:
        one = jax.random.randint(key, (), max(1, total - most), min(most, total - 1) + 1)
        return jnp.stack([one, total - one])
    lengths = jnp.asarray(length_profile(number_of, total, most, lean), jnp.int32)
    pairs = (number_of - 1) // 2
    giver, sink = lengths[1:1 + 2 * pairs:2], lengths[2:2 + 2 * pairs:2]
    slack = jnp.minimum(giver - 1, most - sink)
    passed = jax.random.randint(jax.random.fold_in(key, 1), (pairs,), 0, 1 << 20) % (slack + 1)
    lengths = lengths.at[1:1 + 2 * pairs:2].set(giver - passed).at[2:2 + 2 * pairs:2].set(sink + passed)
    return lengths[jax.random.permutation(jax.random.fold_in(key, 2), number_of)]


def scatter_about(stream_key, dims, width, limit, shards=(), held_as=jnp.bfloat16):
    gain = levels(stream_key, dims, shards, -0.22, 0.18) if shards else 1.0
    values = jax.random.normal(stream_key, dims, jnp.float32) * width * gain
    return jnp.minimum(jnp.maximum(values, -limit), limit).astype(held_as)


def setup_inputs(seed: int = 0) -> dict:
    arg_keys = jax.random.split(jax.random.key(seed), 15)
    activations = draw_activations(jax.random.fold_in(arg_keys[14], 71), 0)
    segments = jax.vmap(lambda own: jnp.searchsorted(jnp.cumsum(ragged_sizes(own, max(4, LEN // 512), LEN, LEN // 2, 1)), jnp.arange(LEN), side="right"))(jax.random.split(arg_keys[1], SEQS)).reshape((SEQS, LEN)).astype(jnp.int32)
    attn_gain = jnp.clip(1.0 + 0.15 * jax.random.normal(arg_keys[2], (D,), jnp.float32), 0.25, 1.75)
    query_weight = scatter_about(arg_keys[3], (D, HQ * HD), D ** -0.5, 0.125, ((0, 4),))
    key_weight = scatter_about(arg_keys[4], (D, HK * HD), D ** -0.5, 0.125, ((0, 4),))
    value_weight = scatter_about(arg_keys[5], (D, HK * HD), D ** -0.5, 0.125, ((0, 4),))
    query_gain = draw_query_gain(jax.random.fold_in(arg_keys[14], 71), 0)
    key_gain = draw_key_gain(jax.random.fold_in(arg_keys[14], 71), 0)
    out_weight = scatter_about(arg_keys[8], (HQ * HD, D), (max(1, HQ * HD // 32)) ** -0.5, 0.75, ((0, 4),))
    mlp_gain = jnp.clip(1.0 + 0.15 * jax.random.normal(arg_keys[9], (D,), jnp.float32), 0.25, 1.75)
    gate_weight = scatter_about(arg_keys[10], (D, FF), D ** -0.5, 0.125, ((0, 4),))
    up_weight = scatter_about(arg_keys[11], (D, FF), D ** -0.5, 0.125, ((0, 4),))
    down_weight = scatter_about(arg_keys[12], (FF, D), FF ** -0.5, 0.078125, ((0, 4),))
    cotangent = draw_cotangent(jax.random.fold_in(arg_keys[14], 71), 0)
    return dict(activations=activations, segments=segments, attn_gain=attn_gain, query_weight=query_weight, key_weight=key_weight, value_weight=value_weight, query_gain=query_gain, key_gain=key_gain, out_weight=out_weight, mlp_gain=mlp_gain, gate_weight=gate_weight, up_weight=up_weight, down_weight=down_weight, cotangent=cotangent)


EPSILON = 1e-06
ROPE_BASE = 1000000.0
MASKED = -1e+30
PRECISE = lax.Precision.HIGHEST

@jax.custom_vjp
def low(v):
    return lax.optimization_barrier(v.astype(jnp.bfloat16)).astype(jnp.float32)

@jax.custom_vjp
def low_back(v):
    return v

def low_keep(v):
    return (low(v), None)

def low_pass(kept, grad):
    return (grad,)

def back_keep(v):
    return (v, None)

def back_low(kept, grad):
    return (low(grad),)
low.defvjp(low_keep, low_pass)
low_back.defvjp(back_keep, back_low)

def matmul_hi(left_op, right_op):
    return jnp.dot(left_op, right_op, preferred_element_type=jnp.float32, precision=PRECISE)

def positions(seg_ids):
    token_index = jnp.arange(seg_ids.shape[0], dtype=jnp.int32)
    before = jnp.concatenate([jnp.full((1,), -1, jnp.int32), seg_ids[:-1]])
    starts = lax.cummax(jnp.where(seg_ids != before, token_index, jnp.zeros_like(token_index)), axis=0)
    return (token_index - starts).astype(jnp.float32)

def rotary(pos_float):
    half_width = HD // 2
    inv_freq = 1.0 / ROPE_BASE ** (jnp.arange(half_width, dtype=jnp.float32) * (2.0 / HD))
    angles = pos_float[:, None] * inv_freq[None, :]
    return (jnp.cos(angles), jnp.sin(angles))

def rotate(values_in, cosine, sine_part):
    half_width = values_in.shape[-1] // 2
    first_half = values_in[..., :half_width]
    second_half = values_in[..., half_width:]
    cos_b = cosine[:, None, :]
    sin_b = sine_part[:, None, :]
    return jnp.concatenate([first_half * cos_b - second_half * sin_b, second_half * cos_b + first_half * sin_b], -1)

def head_norm(values_in, gain_vec):
    return values_in * lax.rsqrt(lax.optimization_barrier(jnp.mean(values_in * values_in, -1, keepdims=True)) + EPSILON) * gain_vec

def layer(weights, inputs, seg_ids, cosine, sine_part):
    attn_gain, query_weight, key_weight, value_weight, query_gain, key_gain, out_weight, mlp_gain, gate_weight, up_weight, down_weight = weights
    length = inputs.shape[0]
    groups = HQ // HK
    score_scale = 1.0 / math.sqrt(HD)
    normed = low(inputs * lax.rsqrt(lax.optimization_barrier(jnp.mean(inputs * inputs, -1, keepdims=True)) + EPSILON) * attn_gain)
    queries = low_back(matmul_hi(normed, query_weight)).reshape(length, HQ, HD)
    keys_raw = low_back(matmul_hi(normed, key_weight)).reshape(length, HK, HD)
    values_low = low(low_back(matmul_hi(normed, value_weight))).reshape(length, HK, HD)
    queries = low(rotate(head_norm(queries, query_gain), cosine, sine_part))
    keys_rot = low(rotate(head_norm(keys_raw, key_gain), cosine, sine_part))
    block_rows = min(512, length)
    query_blocks = queries.reshape(length // block_rows, block_rows, HK, groups, HD)
    block_starts = jnp.arange(length // block_rows, dtype=jnp.int32) * block_rows
    key_index = jnp.arange(length, dtype=jnp.int32)

    def attend(block_item):
        query_part, block_start = block_item
        query_rows = block_start + jnp.arange(block_rows, dtype=jnp.int32)
        seg_rows = lax.dynamic_slice_in_dim(seg_ids, block_start, block_rows)
        visible = (key_index[None, :] <= query_rows[:, None]) & (seg_ids[None, :] == seg_rows[:, None])
        scores = low_back(jnp.einsum('qhgd,khd->hgqk', query_part, keys_rot, precision=PRECISE) * score_scale)
        scores = jnp.where(visible[None, None], scores, MASKED)
        row_max = lax.optimization_barrier(jnp.max(scores, -1, keepdims=True))
        exp_scores = jnp.exp(scores - row_max)
        softmax_out = low(exp_scores / lax.optimization_barrier(jnp.sum(exp_scores, -1, keepdims=True)))
        head_out = jnp.einsum('hgqk,khd->qhgd', softmax_out, values_low, precision=PRECISE)
        return head_out.reshape(block_rows, HQ * HD)
    attn_out = lax.map(jax.checkpoint(attend), (query_blocks, block_starts)).reshape(length, HQ * HD)
    attn_out = low(low_back(attn_out))
    hidden = inputs + low_back(matmul_hi(attn_out, out_weight))
    normed_mlp = low(hidden * lax.rsqrt(lax.optimization_barrier(jnp.mean(hidden * hidden, -1, keepdims=True)) + EPSILON) * mlp_gain)
    gate_pre = low_back(matmul_hi(normed_mlp, gate_weight))
    up_pre = low_back(matmul_hi(normed_mlp, up_weight))
    activated = low(jax.nn.silu(gate_pre) * up_pre)
    return hidden + low_back(matmul_hi(activated, down_weight))

def reference(activations, segments, attn_gain, query_weight, key_weight, value_weight, query_gain, key_gain, out_weight, mlp_gain, gate_weight, up_weight, down_weight, cotangent):
    params = tuple((weight_arr.astype(jnp.float32) for weight_arr in (attn_gain, query_weight, key_weight, value_weight, query_gain, key_gain, out_weight, mlp_gain, gate_weight, up_weight, down_weight)))

    def per_sequence(totals, seq_item):
        seq_input, seg_ids, seq_grad = seq_item
        cosine, sine_part = rotary(positions(seg_ids))

        def forward_fn(inputs, weights):
            return layer(weights, inputs, seg_ids, cosine, sine_part)
        layer_out, pull_back = jax.vjp(forward_fn, seq_input.astype(jnp.float32), params)
        grad_in, grad_params = pull_back(seq_grad.astype(jnp.float32))
        totals = tuple((running + added for running, added in zip(totals, grad_params)))
        return (totals, (layer_out.astype(jnp.bfloat16), grad_in))
    zero_grads = tuple((jnp.zeros_like(weight_arr) for weight_arr in params))
    totals, (outputs, grad_inputs) = lax.scan(per_sequence, zero_grads, (activations, segments, cotangent))
    return (outputs, grad_inputs, totals[0], totals[1], totals[2], totals[3], totals[4], totals[5], totals[6], totals[7], totals[8], totals[9], totals[10])
```

```python
from functools import partial
import math

import jax
import jax.numpy as jnp
from jax import lax
from jax.experimental import pallas as pl
from jax.experimental.pallas import tpu as pltpu
from jax.sharding import PartitionSpec as P

HQ = 16
HK = 8
HD = 128
FF = 6144
GROUPS = HQ // HK

EPSILON = 1e-06
ROPE_BASE = 1000000.0
MASKED = -1e30
BF = jnp.bfloat16
F32 = jnp.float32
AXES = ("shard", "rep")


def dot(a, b):
    return jnp.dot(a, b, preferred_element_type=F32)


def dot_last(a, b):
    return lax.dot_general(a, b, (((1,), (1,)), ((), ())), preferred_element_type=F32)


def dot_first(a, b):
    return lax.dot_general(a, b, (((0,), (0,)), ((), ())), preferred_element_type=F32)


def positions(seg_ids):
    token_index = jnp.arange(seg_ids.shape[0], dtype=jnp.int32)
    before = jnp.concatenate([jnp.full((1,), -1, jnp.int32), seg_ids[:-1]])
    starts = lax.cummax(
        jnp.where(seg_ids != before, token_index, jnp.zeros_like(token_index)), axis=0
    )
    return (token_index - starts).astype(F32)


def head_rope(raw, gain, cos2, sin2):
    rstat = lax.rsqrt(jnp.mean(raw * raw, -1, keepdims=True) + EPSILON)
    scaled = raw * rstat * gain
    return scaled * cos2 + pltpu.roll(scaled, HD // 2, 1) * sin2


def attend_kernel(
    q_ref, k_ref, v_ref, qg_ref, kg_ref, cos_ref, sin_ref, trow_ref, tcol_ref,
    o_ref, qr_ref, kr_ref, vb_ref, *, scale, block
):
    cos2 = cos_ref[...]
    sin2 = sin_ref[...]
    kr = head_rope(k_ref[...], kg_ref[...], cos2, sin2).astype(BF)
    vb = v_ref[...].astype(BF)
    kr_ref[...] = kr
    vb_ref[...] = vb
    length = kr.shape[0]
    for g in range(GROUPS):
        cols = slice(g * HD, (g + 1) * HD)
        qr = head_rope(q_ref[:, cols], qg_ref[...], cos2, sin2).astype(BF)
        qr_ref[:, cols] = qr
        for b in range(length // block):
            rows = slice(b * block, (b + 1) * block)
            s = dot_last(qr[rows], kr) * scale
            seen = (tcol_ref[0:1, :] <= trow_ref[rows, 0:1]) & (
                tcol_ref[1:2, :] == trow_ref[rows, 1:2]
            )
            s = jnp.where(seen, s, MASKED)
            e = jnp.exp(s - jnp.max(s, -1, keepdims=True))
            p = (e / jnp.sum(e, -1, keepdims=True)).astype(BF)
            o_ref[rows, cols] = dot(p, vb).astype(BF)


def head_back(grad_rot, raw, gain, cos2, sin2):
    back = grad_rot * cos2 - pltpu.roll(grad_rot, HD // 2, 1) * sin2
    rstat = lax.rsqrt(jnp.mean(raw * raw, -1, keepdims=True) + EPSILON)
    scaled = raw * rstat
    gain_part = jnp.sum(back * scaled, 0, keepdims=True)
    b = back * gain
    return rstat * (b - scaled * jnp.mean(b * scaled, -1, keepdims=True)), gain_part


def attend_back_kernel(
    q_ref, k_ref, qr_ref, kr_ref, vb_ref, do_ref, qg_ref, kg_ref, cos_ref, sin_ref,
    trow_ref, tcol_ref, dq_ref, dk_ref, dv_ref, gq_ref, gk_ref, *, scale, block
):
    cos2 = cos_ref[...]
    sin2 = sin_ref[...]
    kr = kr_ref[...]
    vb = vb_ref[...]
    length = kr.shape[0]
    dkr = jnp.zeros((length, HD), F32)
    dv = jnp.zeros((length, HD), F32)
    gq = jnp.zeros((1, HD), F32)
    for g in range(GROUPS):
        cols = slice(g * HD, (g + 1) * HD)
        dqr = []
        for b in range(length // block):
            rows = slice(b * block, (b + 1) * block)
            qr = qr_ref[rows, cols]
            do = do_ref[rows, cols]
            s = dot_last(qr, kr) * scale
            seen = (tcol_ref[0:1, :] <= trow_ref[rows, 0:1]) & (
                tcol_ref[1:2, :] == trow_ref[rows, 1:2]
            )
            s = jnp.where(seen, s, MASKED)
            e = jnp.exp(s - jnp.max(s, -1, keepdims=True))
            p = e / jnp.sum(e, -1, keepdims=True)
            dp = dot_last(do, vb)
            ds = (p * (dp - jnp.sum(p * dp, -1, keepdims=True))).astype(BF)
            dqr.append(dot(ds, kr) * scale)
            dkr += dot_first(ds, qr)
            dv += dot_first(p.astype(BF), do)
        dqr = dqr[0] if len(dqr) == 1 else jnp.concatenate(dqr, 0)
        dq, part = head_back(dqr, q_ref[:, cols], qg_ref[...], cos2, sin2)
        dq_ref[:, cols] = dq.astype(BF)
        gq += part
    dk, gk = head_back(dkr * scale, k_ref[...], kg_ref[...], cos2, sin2)
    dk_ref[...] = dk.astype(BF)
    dv_ref[...] = dv.astype(BF)
    gq_ref[...] = jnp.broadcast_to(gq[None], gq_ref.shape)
    gk_ref[...] = jnp.broadcast_to(gk[None], gk_ref.shape)


def const_spec(shape):
    return pl.BlockSpec(shape, lambda j: (0,) * len(shape))


def attention(qkv, nq, nk, qg, kg, cos2, sin2, trow, tcol):
    length = qkv.shape[0]
    block = min(length, 512)
    wide = GROUPS * HD
    col = lambda width, off: pl.BlockSpec((length, width), lambda j: (0, off + j))
    return pl.pallas_call(
        partial(attend_kernel, scale=1.0 / math.sqrt(HD), block=block),
        grid=(nk,),
        out_shape=(
            jax.ShapeDtypeStruct((length, nq * HD), BF),
            jax.ShapeDtypeStruct((length, nq * HD), BF),
            jax.ShapeDtypeStruct((length, nk * HD), BF),
            jax.ShapeDtypeStruct((length, nk * HD), BF),
        ),
        in_specs=[
            col(wide, 0), col(HD, nq), col(HD, nq + nk),
            const_spec((1, HD)), const_spec((1, HD)),
            const_spec((length, HD)), const_spec((length, HD)),
            const_spec((length, 2)), const_spec((2, length)),
        ],
        out_specs=(col(wide, 0), col(wide, 0), col(HD, 0), col(HD, 0)),
        compiler_params=pltpu.CompilerParams(vmem_limit_bytes=48 << 20),
        name="attend",
    )(qkv, qkv, qkv, qg, kg, cos2, sin2, trow, tcol)


def attention_back(qkv, qr, kr, vb, do, nq, nk, qg, kg, cos2, sin2, trow, tcol):
    length = qkv.shape[0]
    block = min(length, 512)
    wide = GROUPS * HD
    col = lambda width, off: pl.BlockSpec((length, width), lambda j: (0, off + j))
    gain_spec = pl.BlockSpec((1, 8, HD), lambda j: (j, 0, 0))
    return pl.pallas_call(
        partial(attend_back_kernel, scale=1.0 / math.sqrt(HD), block=block),
        grid=(nk,),
        out_shape=(
            jax.ShapeDtypeStruct((length, nq * HD), BF),
            jax.ShapeDtypeStruct((length, nk * HD), BF),
            jax.ShapeDtypeStruct((length, nk * HD), BF),
            jax.ShapeDtypeStruct((nk, 8, HD), F32),
            jax.ShapeDtypeStruct((nk, 8, HD), F32),
        ),
        in_specs=[
            col(wide, 0), col(HD, nq), col(wide, 0), col(HD, 0), col(HD, 0), col(wide, 0),
            const_spec((1, HD)), const_spec((1, HD)),
            const_spec((length, HD)), const_spec((length, HD)),
            const_spec((length, 2)), const_spec((2, length)),
        ],
        out_specs=(col(wide, 0), col(HD, 0), col(HD, 0), gain_spec, gain_spec),
        compiler_params=pltpu.CompilerParams(vmem_limit_bytes=48 << 20),
        name="attend_back",
    )(qkv, qkv, qr, kr, vb, do, qg, kg, cos2, sin2, trow, tcol)


def build(n, reps):
    m = reps // 2

    def pairs(move):
        out = []
        for s in range(n):
            for r in range(reps):
                to = move(s, r)
                if to is not None:
                    out.append((s * reps + r, to[0] * reps + to[1]))
        return out

    peer_pairs = [pairs(lambda s, r, k=k: (s ^ k, r)) for k in range(n)]
    sibling_pairs = pairs(lambda s, r: (s, r ^ 1))

    def to_peer(v, k):
        return lax.ppermute(v, AXES, peer_pairs[k])

    def to_sibling(v):
        return lax.ppermute(v, AXES, sibling_pairs)

    def line_up(v, senders):
        return lax.ppermute(
            v, AXES, pairs(lambda s, r: (s, r + 2) if r // 2 in senders else None)
        )

    def line_down(v, senders):
        return lax.ppermute(
            v, AXES, pairs(lambda s, r: (s, r - 2) if r // 2 in senders else None)
        )

    def gather(v):
        return jnp.concatenate([v] + [to_peer(v, k) for k in range(1, n)], 0)

    def scatter_sum(v):
        total = v[0]
        for k in range(1, n):
            total = total + to_peer(v[k].astype(BF), k).astype(F32)
        return total

    def line_scatter(v):
        i = lax.axis_index("rep") // 2
        pick = lambda j: lax.dynamic_index_in_dim(v, jnp.clip(j, 0, m - 1), 0, keepdims=False)
        up = down = None
        for t in range(m - 1):
            mine = pick(m - 1 - t + i)
            if up is not None:
                mine = jnp.where(i > 0, mine.astype(F32) + up.astype(F32), mine.astype(F32))
            up = line_up(mine.astype(BF), range(0, t + 1))
            other = pick(i - (m - 1 - t))
            if down is not None:
                other = jnp.where(i < m - 1, other.astype(F32) + down.astype(F32), other.astype(F32))
            down = line_down(other.astype(BF), range(m - 1 - t, m))
        total = pick(i).astype(F32)
        if up is not None:
            total = total + jnp.where(i > 0, up.astype(F32), 0.0)
            total = total + jnp.where(i < m - 1, down.astype(F32), 0.0)
        return total

    def line_gather(v):
        i = lax.axis_index("rep") // 2
        out = jnp.zeros((m,) + v.shape, v.dtype)
        out = lax.dynamic_update_index_in_dim(out, v, i, 0)
        up = down = v
        for t in range(m - 1):
            up = line_up(up, range(t, m - 1))
            down = line_down(down, range(1, m - t))
            j = i - 1 - t
            spare = lax.dynamic_index_in_dim(out, jnp.clip(j, 0, m - 1), 0, keepdims=False)
            out = lax.dynamic_update_index_in_dim(
                out, jnp.where(j >= 0, up, spare), jnp.clip(j, 0, m - 1), 0
            )
            j = i + 1 + t
            spare = lax.dynamic_index_in_dim(out, jnp.clip(j, 0, m - 1), 0, keepdims=False)
            out = lax.dynamic_update_index_in_dim(
                out, jnp.where(j < m, down, spare), jnp.clip(j, 0, m - 1), 0
            )
        return out

    def per_device(
        activations, segments, attn_gain, query_weight, key_weight, value_weight,
        query_gain, key_gain, out_weight, mlp_gain, gate_weight, up_weight, down_weight,
        cotangent,
    ):
        rows, width = activations.shape[1], activations.shape[2]
        length = segments.shape[1]
        shard = lax.axis_index("shard")
        core = lax.axis_index("rep") % 2
        own = width // n
        half = own // 2
        nq, nk = HQ // n, HK // n
        ffl = FF // n
        owner = [shard ^ k for k in range(n)]

        def cut(v, start, size, axis):
            return lax.dynamic_slice_in_dim(v, start, size, axis)

        def reorder(v):
            return jnp.concatenate(
                [
                    cut(v, owner[k] * own + (core ^ h) * half, half, 1)
                    for h in range(2)
                    for k in range(n)
                ],
                1,
            )

        def restore(v):
            return jnp.concatenate(
                [
                    cut(v, ((core ^ h) * n + owner[b]) * half, half, 1)
                    for b in range(n)
                    for h in range(2)
                ],
                1,
            )

        def exchange_weights(weights):
            def piece(k, h):
                return jnp.concatenate(
                    [
                        cut(
                            cut(w, (core ^ h) * half, half, 0),
                            owner[k] * (w.shape[1] // n),
                            w.shape[1] // n,
                            1,
                        )
                        for w in weights
                    ],
                    1,
                )

            got = [to_peer(piece(k, 0), k) for k in range(1, n)]
            other = [to_sibling(v) for v in got]
            return jnp.concatenate([piece(0, 0)] + got + [piece(0, 1)] + other, 0)

        inputs = activations[0].astype(F32)
        all_inputs = gather(activations[0])
        w_qkv = exchange_weights([query_weight, key_weight, value_weight])
        w_mlp = exchange_weights([gate_weight, up_weight])
        all_grads = gather(cotangent[0])

        seg_ids = segments[0]
        pos = positions(seg_ids)
        tokens = jnp.arange(length, dtype=jnp.int32)
        shuffle = lambda v: jnp.concatenate([cut(v, owner[k] * rows, rows, 0) for k in range(n)])
        index, seg_ids, pos = shuffle(tokens), shuffle(seg_ids), shuffle(pos)
        inv_freq = 1.0 / ROPE_BASE ** (jnp.arange(HD // 2, dtype=F32) * (2.0 / HD))
        angles = pos[:, None] * inv_freq[None, :]
        cosine, sine = jnp.cos(angles), jnp.sin(angles)
        cos2 = jnp.concatenate([cosine, cosine], 1)
        sin2 = jnp.concatenate([-sine, sine], 1)
        tcol = jnp.stack([index, seg_ids], 0)
        trow = jnp.stack([index, seg_ids], 1)
        qg, kg = query_gain[None], key_gain[None]

        wide = all_inputs.astype(F32)
        r1 = lax.rsqrt(jnp.mean(wide * wide, -1, keepdims=True) + EPSILON)
        normed = reorder((wide * r1 * attn_gain).astype(BF))
        qkv = dot(normed, w_qkv)
        attn_out, qr, kr, vb = attention(qkv, nq, nk, qg, kg, cos2, sin2, trow, tcol)

        hidden = inputs + scatter_sum(dot(attn_out, out_weight).reshape(n, rows, width))
        r2 = lax.rsqrt(jnp.mean(hidden * hidden, -1, keepdims=True) + EPSILON)
        normed_mlp = reorder(gather((hidden * r2 * mlp_gain).astype(BF)))
        pre = dot(normed_mlp, w_mlp)
        gate_pre, up_pre = pre[:, :ffl], pre[:, ffl:]
        sig = jax.nn.sigmoid(gate_pre)
        activated = (gate_pre * sig * up_pre).astype(BF)
        grad_act = dot_last(all_grads, down_weight)
        grad_gate = (grad_act * up_pre * sig * (1.0 + gate_pre * (1.0 - sig))).astype(BF)
        grad_up = (grad_act * gate_pre * sig).astype(BF)
        grad_pre = jnp.concatenate([grad_gate, grad_up], 1)
        dhn = scatter_sum(restore(dot_last(grad_pre, w_mlp)).reshape(n, rows, width))
        output = (
            hidden + scatter_sum(dot(activated, down_weight).reshape(n, rows, width))
        ).astype(BF)[None]

        hh = hidden * r2
        grad_mlp_gain = jnp.sum(dhn * hh, 0)
        weighted = dhn * mlp_gain
        grad_hidden = cotangent[0].astype(F32) + r2 * (
            weighted - hh * jnp.mean(weighted * hh, -1, keepdims=True)
        )
        grad_branch = gather(grad_hidden.astype(BF))
        do = dot_last(grad_branch, out_weight).astype(BF)
        dq, dk, dv, gq, gk = attention_back(
            qkv, qr, kr, vb, do, nq, nk, qg, kg, cos2, sin2, trow, tcol
        )
        dqkv = jnp.concatenate([dq, dk, dv], 1)
        dnormed = scatter_sum(restore(dot_last(dqkv, w_qkv)).reshape(n, rows, width))
        r1_own = lax.rsqrt(jnp.mean(inputs * inputs, -1, keepdims=True) + EPSILON)
        xh = inputs * r1_own
        grad_attn_gain = jnp.sum(dnormed * xh, 0)
        weighted = dnormed * attn_gain
        grad_input = (
            grad_hidden + r1_own * (weighted - xh * jnp.mean(weighted * xh, -1, keepdims=True))
        )[None]
        gains = lax.psum(
            jnp.concatenate(
                [grad_attn_gain, grad_mlp_gain, jnp.sum(gq[:, 0], 0), jnp.sum(gk[:, 0], 0)]
            ),
            AXES,
        )
        grad_attn_gain, grad_mlp_gain = gains[:width], gains[width : 2 * width]
        grad_query_gain = gains[2 * width : 2 * width + HD]
        grad_key_gain = gains[2 * width + HD :]

        def pair_sum(left, right):
            both = left.shape[1] // 2
            away = to_sibling(dot_first(left[:, both:], right).astype(BF))
            return dot_first(left[:, :both], right) + away.astype(F32)

        def halves(v):
            both = v.shape[1] // 2
            return jnp.concatenate(
                [cut(v, core * both, both, 1), cut(v, (1 - core) * both, both, 1)], 1
            )

        def reduce_rows(v):
            part = line_scatter(v.reshape(m, v.shape[0] // m, v.shape[1])).astype(BF)
            mine = line_gather(part).reshape(v.shape)
            return by_core(mine, to_sibling(mine))

        def by_core(mine, other):
            both = jnp.stack([mine, other], 0)
            return jnp.concatenate(
                [lax.dynamic_index_in_dim(both, core ^ h, 0, keepdims=False) for h in range(2)], 0
            ).astype(F32)

        def reduce_cols(v, widths):
            cols = v.shape[1]
            q = half // m
            v = v.reshape(n, m, q, cols).transpose(1, 0, 2, 3)
            part = line_scatter(v).astype(BF)
            part = jnp.stack([part[0]] + [to_peer(part[k], k) for k in range(1, n)], 0)
            mine = line_gather(part)
            other = to_sibling(mine)
            both = jnp.stack([mine, other], 0)
            outs, at = [], 0
            for w in widths:
                block = both[..., at : at + w]
                at += w
                halves_out = []
                for h in range(2):
                    one = lax.dynamic_index_in_dim(block, core ^ h, 0, keepdims=False)
                    cols_out = [
                        lax.dynamic_index_in_dim(one, owner[b], 1, keepdims=False).reshape(half, w)
                        for b in range(n)
                    ]
                    halves_out.append(jnp.concatenate(cols_out, 1))
                outs.append(jnp.concatenate(halves_out, 0).astype(F32))
            return outs

        grad_down = reduce_rows(pair_sum(halves(activated), all_grads))
        grad_gate_weight, grad_up_weight = reduce_cols(
            pair_sum(normed_mlp, grad_pre), [ffl, ffl]
        )
        grad_out_weight = reduce_rows(pair_sum(halves(attn_out), grad_branch))
        grad_query_weight, grad_key_weight, grad_value_weight = reduce_cols(
            pair_sum(normed, dqkv), [nq * HD, nk * HD, nk * HD]
        )
        return (
            output,
            grad_input,
            grad_attn_gain,
            grad_query_weight,
            grad_key_weight,
            grad_value_weight,
            grad_query_gain,
            grad_key_gain,
            grad_out_weight,
            grad_mlp_gain,
            grad_gate_weight,
            grad_up_weight,
            grad_down,
        )

    return per_device


def solution(mesh):
    tok = P("rep", "shard", None)
    row = P("shard", None)
    return jax.shard_map(
        build(mesh.shape["shard"], mesh.shape["rep"]),
        mesh=mesh,
        in_specs=(
            tok, P("rep", None), P(), row, row, row, P(), P(), row, P(), row, row, row, tok,
        ),
        out_specs=(tok, tok, P(), row, row, row, P(), P(), row, P(), row, row, row),
        check_vma=False,
    )
```

```python
from functools import partial
import math

import jax
import jax.numpy as jnp
from jax import lax
from jax.experimental import pallas as pl
from jax.experimental.pallas import tpu as pltpu
from jax.sharding import PartitionSpec as P

HQ = 16
HK = 8
HD = 128
FF = 6144
GROUPS = HQ // HK

EPSILON = 1e-06
ROPE_BASE = 1000000.0
MASKED = -1e30
BF = jnp.bfloat16
F32 = jnp.float32
AXES = ("shard", "rep")


def dot(a, b):
    return jnp.dot(a, b, preferred_element_type=F32)


def dot_last(a, b):
    return lax.dot_general(a, b, (((1,), (1,)), ((), ())), preferred_element_type=F32)


def dot_first(a, b):
    return lax.dot_general(a, b, (((0,), (0,)), ((), ())), preferred_element_type=F32)


def positions(seg_ids):
    token_index = jnp.arange(seg_ids.shape[0], dtype=jnp.int32)
    before = jnp.concatenate([jnp.full((1,), -1, jnp.int32), seg_ids[:-1]])
    starts = lax.cummax(
        jnp.where(seg_ids != before, token_index, jnp.zeros_like(token_index)), axis=0
    )
    return (token_index - starts).astype(F32)


def head_rope(raw, gain, cos2, sin2):
    rstat = lax.rsqrt(jnp.mean(raw * raw, -1, keepdims=True) + EPSILON)
    scaled = raw * rstat * gain
    return scaled * cos2 + pltpu.roll(scaled, HD // 2, 1) * sin2


def attend_kernel(
    q_ref, k_ref, v_ref, qg_ref, kg_ref, cos_ref, sin_ref, trow_ref, tcol_ref,
    o_ref, qr_ref, kr_ref, vb_ref, *, scale, block
):
    cos2 = cos_ref[...]
    sin2 = sin_ref[...]
    kr = head_rope(k_ref[...], kg_ref[...], cos2, sin2).astype(BF)
    vb = v_ref[...].astype(BF)
    kr_ref[...] = kr
    vb_ref[...] = vb
    length = kr.shape[0]
    for g in range(GROUPS):
        cols = slice(g * HD, (g + 1) * HD)
        qr = head_rope(q_ref[:, cols], qg_ref[...], cos2, sin2).astype(BF)
        qr_ref[:, cols] = qr
        for b in range(length // block):
            rows = slice(b * block, (b + 1) * block)
            s = dot_last(qr[rows], kr) * scale
            seen = (tcol_ref[0:1, :] <= trow_ref[rows, 0:1]) & (
                tcol_ref[1:2, :] == trow_ref[rows, 1:2]
            )
            s = jnp.where(seen, s, MASKED)
            e = jnp.exp(s - jnp.max(s, -1, keepdims=True))
            p = (e / jnp.sum(e, -1, keepdims=True)).astype(BF)
            o_ref[rows, cols] = dot(p, vb).astype(BF)


def head_back(grad_rot, raw, gain, cos2, sin2):
    back = grad_rot * cos2 - pltpu.roll(grad_rot, HD // 2, 1) * sin2
    rstat = lax.rsqrt(jnp.mean(raw * raw, -1, keepdims=True) + EPSILON)
    scaled = raw * rstat
    gain_part = jnp.sum(back * scaled, 0, keepdims=True)
    b = back * gain
    return rstat * (b - scaled * jnp.mean(b * scaled, -1, keepdims=True)), gain_part


def attend_back_kernel(
    q_ref, k_ref, qr_ref, kr_ref, vb_ref, do_ref, qg_ref, kg_ref, cos_ref, sin_ref,
    trow_ref, tcol_ref, dq_ref, dk_ref, dv_ref, gq_ref, gk_ref, *, scale, block
):
    cos2 = cos_ref[...]
    sin2 = sin_ref[...]
    kr = kr_ref[...]
    vb = vb_ref[...]
    length = kr.shape[0]
    dkr = jnp.zeros((length, HD), F32)
    dv = jnp.zeros((length, HD), F32)
    gq = jnp.zeros((1, HD), F32)
    for g in range(GROUPS):
        cols = slice(g * HD, (g + 1) * HD)
        dqr = []
        for b in range(length // block):
            rows = slice(b * block, (b + 1) * block)
            qr = qr_ref[rows, cols]
            do = do_ref[rows, cols]
            s = dot_last(qr, kr) * scale
            seen = (tcol_ref[0:1, :] <= trow_ref[rows, 0:1]) & (
                tcol_ref[1:2, :] == trow_ref[rows, 1:2]
            )
            s = jnp.where(seen, s, MASKED)
            e = jnp.exp(s - jnp.max(s, -1, keepdims=True))
            p = e / jnp.sum(e, -1, keepdims=True)
            dp = dot_last(do, vb)
            ds = (p * (dp - jnp.sum(p * dp, -1, keepdims=True))).astype(BF)
            dqr.append(dot(ds, kr) * scale)
            dkr += dot_first(ds, qr)
            dv += dot_first(p.astype(BF), do)
        dqr = dqr[0] if len(dqr) == 1 else jnp.concatenate(dqr, 0)
        dq, part = head_back(dqr, q_ref[:, cols], qg_ref[...], cos2, sin2)
        dq_ref[:, cols] = dq.astype(BF)
        gq += part
    dk, gk = head_back(dkr * scale, k_ref[...], kg_ref[...], cos2, sin2)
    dk_ref[...] = dk.astype(BF)
    dv_ref[...] = dv.astype(BF)
    gq_ref[...] = jnp.broadcast_to(gq[None], gq_ref.shape)
    gk_ref[...] = jnp.broadcast_to(gk[None], gk_ref.shape)


def const_spec(shape):
    return pl.BlockSpec(shape, lambda j: (0,) * len(shape))


def attention(qkv, nq, nk, qg, kg, cos2, sin2, trow, tcol):
    length = qkv.shape[0]
    block = min(length, 512)
    wide = GROUPS * HD
    col = lambda width, off: pl.BlockSpec((length, width), lambda j: (0, off + j))
    return pl.pallas_call(
        partial(attend_kernel, scale=1.0 / math.sqrt(HD), block=block),
        grid=(nk,),
        out_shape=(
            jax.ShapeDtypeStruct((length, nq * HD), BF),
            jax.ShapeDtypeStruct((length, nq * HD), BF),
            jax.ShapeDtypeStruct((length, nk * HD), BF),
            jax.ShapeDtypeStruct((length, nk * HD), BF),
        ),
        in_specs=[
            col(wide, 0), col(HD, nq), col(HD, nq + nk),
            const_spec((1, HD)), const_spec((1, HD)),
            const_spec((length, HD)), const_spec((length, HD)),
            const_spec((length, 2)), const_spec((2, length)),
        ],
        out_specs=(col(wide, 0), col(wide, 0), col(HD, 0), col(HD, 0)),
        compiler_params=pltpu.CompilerParams(vmem_limit_bytes=48 << 20),
        name="attend",
    )(qkv, qkv, qkv, qg, kg, cos2, sin2, trow, tcol)


def attention_back(qkv, qr, kr, vb, do, nq, nk, qg, kg, cos2, sin2, trow, tcol):
    length = qkv.shape[0]
    block = min(length, 512)
    wide = GROUPS * HD
    col = lambda width, off: pl.BlockSpec((length, width), lambda j: (0, off + j))
    gain_spec = pl.BlockSpec((1, 8, HD), lambda j: (j, 0, 0))
    return pl.pallas_call(
        partial(attend_back_kernel, scale=1.0 / math.sqrt(HD), block=block),
        grid=(nk,),
        out_shape=(
            jax.ShapeDtypeStruct((length, nq * HD), BF),
            jax.ShapeDtypeStruct((length, nk * HD), BF),
            jax.ShapeDtypeStruct((length, nk * HD), BF),
            jax.ShapeDtypeStruct((nk, 8, HD), F32),
            jax.ShapeDtypeStruct((nk, 8, HD), F32),
        ),
        in_specs=[
            col(wide, 0), col(HD, nq), col(wide, 0), col(HD, 0), col(HD, 0), col(wide, 0),
            const_spec((1, HD)), const_spec((1, HD)),
            const_spec((length, HD)), const_spec((length, HD)),
            const_spec((length, 2)), const_spec((2, length)),
        ],
        out_specs=(col(wide, 0), col(HD, 0), col(HD, 0), gain_spec, gain_spec),
        compiler_params=pltpu.CompilerParams(vmem_limit_bytes=48 << 20),
        name="attend_back",
    )(qkv, qkv, qr, kr, vb, do, qg, kg, cos2, sin2, trow, tcol)


def assemble_kernel(counts, order_ref, *refs):
    n_rows, n_cols = counts
    total = n_rows + n_cols
    mine, other, outs = refs[:total], refs[total : 2 * total], refs[2 * total :]

    def fill(sources):
        for src, out in zip(sources, outs):
            m, places, q, width = src.shape
            for a in range(places):
                out[a * m * q : (a + 1) * m * q, :] = (
                    src[:, a].reshape(m * q, width).astype(F32)
                )

    pl.when(pl.program_id(0) == 0)(lambda: fill(mine))
    pl.when(pl.program_id(0) == 1)(lambda: fill(other))


def assemble(rows, cols, core, owner):
    n = len(owner)
    order = jnp.stack(list(owner) + [core]).astype(jnp.int32)
    in_specs, out_specs, shapes, operands = [[], []], [], [], [[], []]
    size = 0
    for mine, other in rows:
        m, places, q, width = mine.shape
        block = (m, places, q, width // n)
        in_specs[0].append(
            pl.BlockSpec(block, lambda g, b, o: (0, 0, 0, jnp.where(g == 0, b, n - 1)))
        )
        in_specs[1].append(
            pl.BlockSpec(block, lambda g, b, o: (0, 0, 0, jnp.where(g == 0, 0, b)))
        )
        out_specs.append(
            pl.BlockSpec((places * m * q, width // n), lambda g, b, o: (g ^ o[n], b))
        )
        shapes.append(jax.ShapeDtypeStruct((2 * places * m * q, width), F32))
        operands[0].append(mine)
        operands[1].append(other)
        size += mine.size
    for mine, other, at, width in cols:
        m, _, q, _ = mine.shape
        block = (m, 1, q, width)
        in_specs[0].append(
            pl.BlockSpec(block, lambda g, b, o, at=at: (0, o[jnp.where(g == 0, b, n - 1)], 0, at))
        )
        in_specs[1].append(
            pl.BlockSpec(block, lambda g, b, o, at=at: (0, o[jnp.where(g == 0, 0, b)], 0, at))
        )
        out_specs.append(pl.BlockSpec((m * q, width), lambda g, b, o: (g ^ o[n], b)))
        shapes.append(jax.ShapeDtypeStruct((2 * m * q, n * width), F32))
        operands[0].append(mine)
        operands[1].append(other)
        size += m * n * q * width
    return pl.pallas_call(
        partial(assemble_kernel, (len(rows), len(cols))),
        out_shape=tuple(shapes),
        grid_spec=pltpu.PrefetchScalarGridSpec(
            num_scalar_prefetch=1,
            grid=(2, n),
            in_specs=in_specs[0] + in_specs[1],
            out_specs=tuple(out_specs),
        ),
        compiler_params=pltpu.CompilerParams(vmem_limit_bytes=56 << 20),
        cost_estimate=pl.CostEstimate(flops=0, bytes_accessed=12 * size, transcendentals=0),
        name="assemble",
    )(order, *operands[0], *operands[1])


MESH_ID = pl.DeviceIdType.MESH


def reduce_kernel(n, m, parts, *refs):
    count = 4
    gain_ref, refs = refs[0], refs[1:]
    gain_out, refs = refs[2 * count], refs[: 2 * count] + refs[2 * count + 1 :]
    sends, keeps = refs[:count], refs[count : 2 * count]
    mines, others = refs[2 * count : 3 * count], refs[3 * count : 4 * count]
    refs = refs[4 * count :]
    keep_v, away_v = refs[:count], refs[count : 2 * count]
    (ups, downs, tots, fins, load_sem, pair_s, pair_r, up_s, up_r, down_s, down_r,
     peer_s, peer_r, gup_s, gup_r, gdown_s, gdown_r, sib_s, sib_r, own_sem, gain_pair, gain_group, gain_line,
     gain_s, gain_r) = refs[2 * count :]
    shard, rep = lax.axis_index("shard"), lax.axis_index("rep")
    i = rep // 2
    core = lax.rem(rep, 2)
    sibling = {"rep": 2 * i + 1 - core}
    above, below = {"rep": rep + 2}, {"rep": rep - 2}
    peers = [None] + [{"shard": shard ^ k} for k in range(1, n)]
    has_up, has_down = i < m - 1, i > 0

    barrier = pltpu.get_barrier_semaphore()

    def greet(dev):
        pl.semaphore_signal(barrier, inc=1, device_id=dev, device_id_type=MESH_ID)

    greet(sibling)
    for k in range(1, n):
        greet(peers[k])
    line = [None] + [{"rep": 2 * lax.rem(i + d, m) + core} for d in range(1, m)]
    for d in range(1, m):
        greet(line[d])
    pl.semaphore_wait(barrier, n + m - 1)

    def remote(src, dst, ssem, rsem, dev):
        return pltpu.make_async_remote_copy(
            src_ref=src, dst_ref=dst, send_sem=ssem, recv_sem=rsem,
            device_id=dev, device_id_type=MESH_ID,
        )

    def chunk(ref, part, j):
        seg, at, _ = part
        return ref[seg].at[at, j]

    def out(ref, part, j):
        seg, at, _ = part
        return ref[seg].at[j, at]

    def pair_copy(p):
        seg, at, _ = parts[p]
        return remote(sends[seg].at[at], away_v[seg].at[at], pair_s.at[p], pair_r.at[p], sibling)

    def load_copy(p):
        seg, at, _ = parts[p]
        return pltpu.make_async_copy(keeps[seg].at[at], keep_v[seg].at[at], load_sem.at[p])

    def slot(ref, p, t):
        return ref[parts[p][0]].at[parts[p][1], t]

    def up_copy(p, t, src):
        return remote(src, slot(ups, p, t), up_s.at[p, t], up_r.at[p, t], above)

    def down_copy(p, t, src):
        return remote(src, slot(downs, p, t), down_s.at[p, t], down_r.at[p, t], below)

    def add_into(ref, other):
        ref[...] = (ref[...].astype(F32) + other[...].astype(F32)).astype(BF)

    def scatter_step(p, t):
        part = parts[p]
        if t > 0:

            @pl.when((i > 0) & (i <= t) & has_up)
            def _():
                up_copy(p, t - 1, slot(ups, p, t - 1)).wait_recv()
                add_into(slot(ups, p, t - 1), chunk(keep_v, part, m - 1 - t + i))

            @pl.when((i < m - 1) & (i >= m - 1 - t) & has_down)
            def _():
                down_copy(p, t - 1, slot(downs, p, t - 1)).wait_recv()
                add_into(slot(downs, p, t - 1), chunk(keep_v, part, i - (m - 1 - t)))

            pl.when((i > 0) & (i <= t) & has_up)(
                lambda: up_copy(p, t, slot(ups, p, t - 1)).start()
            )
            pl.when((i < m - 1) & (i >= m - 1 - t) & has_down)(
                lambda: down_copy(p, t, slot(downs, p, t - 1)).start()
            )
        pl.when(i == 0)(lambda: up_copy(p, t, chunk(keep_v, part, m - 1 - t)).start())
        pl.when(i == m - 1)(lambda: down_copy(p, t, chunk(keep_v, part, t)).start())

    def peer_copy(p):
        seg, at, k = parts[p]
        return remote(tots[seg].at[at], fins[seg].at[at], peer_s.at[p], peer_r.at[p], peers[k])

    def total(p):
        seg, at, k = parts[p]
        part = parts[p]
        pl.when(has_down)(lambda: up_copy(p, m - 2, slot(ups, p, m - 2)).wait_recv())
        pl.when(has_up)(lambda: down_copy(p, m - 2, slot(downs, p, m - 2)).wait_recv())
        where = fins[seg].at[at] if k == 0 else tots[seg].at[at]

        def put(*extra):
            value = chunk(keep_v, part, i)[...].astype(F32)
            for e in extra:
                value = value + e[...].astype(F32)
            where[...] = value.astype(BF)

        u, d = slot(ups, p, m - 2), slot(downs, p, m - 2)
        pl.when(has_up & has_down)(lambda: put(u, d))
        pl.when(has_up & (i == 0))(lambda: put(d))
        pl.when(has_down & (i == m - 1))(lambda: put(u))
        if k != 0:
            peer_copy(p).start()

    def gup_copy(p, t, j, src):
        return remote(src, out(mines, parts[p], j), gup_s.at[p, t], gup_r.at[p, t], above)

    def gdown_copy(p, t, j, src):
        return remote(src, out(mines, parts[p], j), gdown_s.at[p, t], gdown_r.at[p, t], below)

    def sib_copy(p, j, src):
        return remote(src, out(others, parts[p], j), sib_s.at[p, j], sib_r.at[p, j], sibling)

    def gather_step(p, t):
        part = parts[p]
        if t == 0:
            seg, at, k = part
            if k != 0:
                peer_copy(p).wait_recv()
            fin = fins[seg].at[at]
            pl.when(has_up)(lambda: gup_copy(p, 0, i, fin).start())
            pl.when(has_down)(lambda: gdown_copy(p, 0, i, fin).start())
            sib_copy(p, i, fin).start()
            pltpu.make_async_copy(fin, out(mines, part, i), own_sem.at[p]).start()
            return

        @pl.when(i - t >= 0)
        def _():
            here = out(mines, part, i - t)
            gup_copy(p, t - 1, i - t, here).wait_recv()
            if t < m - 1:
                pl.when(has_up)(lambda: gup_copy(p, t, i - t, here).start())
            sib_copy(p, i - t, here).start()

        @pl.when(i + t < m)
        def _():
            here = out(mines, part, i + t)
            gdown_copy(p, t - 1, i + t, here).wait_recv()
            if t < m - 1:
                pl.when(has_down)(lambda: gdown_copy(p, t, i + t, here).start())
            sib_copy(p, i + t, here).start()

    def gain_copies(level):
        if level == 0:
            return [remote(gain_ref, gain_pair, gain_s.at[0], gain_r.at[0], sibling)]
        if level == 1:
            return [
                remote(
                    gain_group.at[shard], gain_group.at[shard], gain_s.at[k], gain_r.at[k], peers[k]
                )
                for k in range(1, n)
            ]
        return [
            remote(
                gain_line.at[i], gain_line.at[i], gain_s.at[n - 1 + d], gain_r.at[n - 1 + d], line[d]
            )
            for d in range(1, m)
        ]

    def gains(level):
        if level > 0:
            for copy in gain_copies(level - 1):
                copy.wait_recv()
        if level == 1:
            gain_group[shard] = gain_ref[...] + gain_pair[...]
        elif level == 2:
            value = gain_group[0]
            for k in range(1, n):
                value = value + gain_group[k]
            gain_line[i] = value
        elif level == 3:
            value = gain_line[0]
            for k in range(1, m):
                value = value + gain_line[k]
            gain_out[...] = value
        if level < 3:
            for copy in gain_copies(level):
                copy.start()

    def first(p):
        seg, at, _ = parts[p]
        load_copy(p).wait()
        pair_copy(p).wait_recv()
        for j in range(m):
            add_into(keep_v[seg].at[at, j], away_v[seg].at[at, j])
        scatter_step(p, 0)

    stages = [first] + [lambda p, t=t: scatter_step(p, t) for t in range(1, m - 1)]
    stages += [total] + [lambda p, t=t: gather_step(p, t) for t in range(m)]

    for p in range(len(parts)):
        pair_copy(p).start()
        load_copy(p).start()
    for tick in range(len(parts) + len(stages) - 1):
        if tick < 4:
            gains(tick)
        for st in range(len(stages) - 1, -1, -1):
            p = tick - st
            if 0 <= p < len(parts):
                stages[st](p)

    for level in range(3):
        for copy in gain_copies(level):
            copy.wait_send()
    for p in range(len(parts)):
        part = parts[p]
        seg, at, k = part
        pair_copy(p).wait_send()
        if k != 0:
            peer_copy(p).wait_send()
        pltpu.make_async_copy(fins[seg].at[at], out(mines, part, i), own_sem.at[p]).wait()
        for t in range(m - 1):
            pl.when((i <= t) & has_up)(lambda: up_copy(p, t, slot(ups, p, t)).wait_send())
            pl.when((i >= m - 1 - t) & has_down)(
                lambda: down_copy(p, t, slot(downs, p, t)).wait_send()
            )
            pl.when((i - t >= 0) & has_up)(
                lambda: gup_copy(p, t, i, fins[seg].at[at]).wait_send()
            )
            pl.when((i + t < m) & has_down)(
                lambda: gdown_copy(p, t, i, fins[seg].at[at]).wait_send()
            )
        for j in range(m):
            copy = sib_copy(p, j, fins[seg].at[at])
            copy.wait_send()
            copy.wait_recv()


def reduce_gradients(n, m, gains, sends, keeps, parts):
    count, total = len(keeps), len(parts)
    dma = pltpu.SemaphoreType.DMA
    hbm = pl.BlockSpec(memory_space=pl.ANY)

    def slots(extra):
        return [
            pltpu.VMEM((v.shape[0],) + extra + v.shape[2:], BF) for v in keeps
        ]

    outs = [
        jax.ShapeDtypeStruct((m, v.shape[0]) + v.shape[2:], BF) for v in keeps
    ]
    sent = sum(v.size for v in keeps) * 2
    return pl.pallas_call(
        partial(reduce_kernel, n, m, parts),
        out_shape=tuple([jax.ShapeDtypeStruct(gains.shape, F32)] + outs + outs),
        in_specs=[pl.BlockSpec(memory_space=pltpu.VMEM)] + [hbm] * (2 * count),
        out_specs=tuple([pl.BlockSpec(memory_space=pltpu.VMEM)] + [hbm] * (2 * count)),
        scratch_shapes=[pltpu.VMEM(v.shape, BF) for v in keeps]
        + [pltpu.VMEM(v.shape, BF) for v in keeps]
        + [slots((m - 1,)), slots((m - 1,)), slots(()), slots(())]
        + [
            dma((total,)), dma((total,)), dma((total,)),
            dma((total, m - 1)), dma((total, m - 1)), dma((total, m - 1)), dma((total, m - 1)),
            dma((total,)), dma((total,)),
            dma((total, m - 1)), dma((total, m - 1)), dma((total, m - 1)), dma((total, m - 1)),
            dma((total, m)), dma((total, m)), dma((total,)),
            pltpu.VMEM(gains.shape, F32), pltpu.VMEM((n,) + gains.shape, F32),
            pltpu.VMEM((m,) + gains.shape, F32), dma((n + m,)), dma((n + m,)),
        ],
        compiler_params=pltpu.CompilerParams(
            collective_id=3, has_side_effects=True, vmem_limit_bytes=60 << 20
        ),
        cost_estimate=pl.CostEstimate(flops=0, bytes_accessed=4 * sent, transcendentals=0),
        name="reduce_gradients",
    )(gains, *sends, *keeps)


def build(n, reps):
    m = reps // 2

    def pairs(move):
        out = []
        for s in range(n):
            for r in range(reps):
                to = move(s, r)
                if to is not None:
                    out.append((s * reps + r, to[0] * reps + to[1]))
        return out

    peer_pairs = [pairs(lambda s, r, k=k: (s ^ k, r)) for k in range(n)]
    sibling_pairs = pairs(lambda s, r: (s, r ^ 1))

    def to_peer(v, k):
        return lax.ppermute(v, AXES, peer_pairs[k])

    def to_sibling(v):
        return lax.ppermute(v, AXES, sibling_pairs)

    def line_up(v, senders):
        return lax.ppermute(
            v, AXES, pairs(lambda s, r: (s, r + 2) if r // 2 in senders else None)
        )

    def line_down(v, senders):
        return lax.ppermute(
            v, AXES, pairs(lambda s, r: (s, r - 2) if r // 2 in senders else None)
        )

    def gather(v):
        return jnp.concatenate([v] + [to_peer(v, k) for k in range(1, n)], 0)

    def scatter_sum(v):
        total = v[0].astype(F32)
        for k in range(1, n):
            total = total + to_peer(v[k].astype(BF), k).astype(F32)
        return total

    def line_scatter(v, axis):
        i = lax.axis_index("rep") // 2

        def pick(j):
            return lax.dynamic_index_in_dim(
                v, jnp.clip(j, 0, m - 1), axis, keepdims=False
            ).astype(F32)

        up = down = None
        for t in range(m - 1):
            mine, other = pick(m - 1 - t + i), pick(i - (m - 1 - t))
            if t > 0:
                mine, other = mine + up.astype(F32), other + down.astype(F32)
            up = line_up(mine.astype(BF), range(0, t + 1))
            down = line_down(other.astype(BF), range(m - 1 - t, m))
        total = pick(i)
        if m > 1:
            total = total + up.astype(F32) + down.astype(F32)
        return total

    def line_gather(v):
        i = lax.axis_index("rep") // 2
        up, down = [v], [v]
        for t in range(m - 1):
            up.append(line_up(up[-1], range(t, m - 1)))
            down.append(line_down(down[-1], range(1, m - t)))
        return [v] + [jnp.where(t <= i, up[t], down[m - t]) for t in range(1, m)]

    def place(buffer, chunks, axis):
        i = lax.axis_index("rep") // 2
        for p, chunk in enumerate(chunks):
            buffer = lax.dynamic_update_index_in_dim(buffer, chunk, (i - p) % m, axis)
        return buffer

    def per_device(
        activations, segments, attn_gain, query_weight, key_weight, value_weight,
        query_gain, key_gain, out_weight, mlp_gain, gate_weight, up_weight, down_weight,
        cotangent,
    ):
        rows, width = activations.shape[1], activations.shape[2]
        length = segments.shape[1]
        shard = lax.axis_index("shard")
        core = lax.axis_index("rep") % 2
        own = width // n
        half = own // 2
        nq, nk = HQ // n, HK // n
        ffl = FF // n
        owner = [shard ^ k for k in range(n)]

        def cut(v, start, size, axis):
            return lax.dynamic_slice_in_dim(v, start, size, axis)

        def reorder(v):
            return jnp.concatenate(
                [
                    cut(v, owner[k] * own + (core ^ h) * half, half, 1)
                    for h in range(2)
                    for k in range(n)
                ],
                1,
            )

        def restore(v):
            return jnp.concatenate(
                [
                    cut(v, ((core ^ h) * n + owner[b]) * half, half, 1)
                    for b in range(n)
                    for h in range(2)
                ],
                1,
            )

        def exchange_weights(weights):
            q = half // m
            place_i = lax.axis_index("rep") // 2

            def piece(k, start, size):
                return jnp.concatenate(
                    [
                        cut(
                            cut(w, start, size, 0),
                            owner[k] * (w.shape[1] // n),
                            w.shape[1] // n,
                            1,
                        )
                        for w in weights
                    ],
                    1,
                )

            got = jnp.stack(
                [
                    to_peer(piece(k, core * half + place_i * q, q), k)
                    for k in range(1, n)
                ],
                0,
            )
            chunks = line_gather(got)
            cols = got.shape[-1]
            block = lax.dynamic_update_slice(
                jnp.zeros((n, m, q, cols), BF),
                piece(0, core * half, half).reshape(1, m, q, cols),
                (0, 0, 0, 0),
            )
            for p, chunk in enumerate(chunks):
                block = lax.dynamic_update_slice(
                    block, chunk[:, None], (1, (place_i - p) % m, 0, 0)
                )
            block = block.reshape(n * half, cols)
            return block, to_sibling(block)

        def times(v, w):
            both = v.shape[1] // 2
            return dot(v[:, :both], w[0]) + dot(v[:, both:], w[1])

        def times_back(v, w):
            return jnp.concatenate(
                [dot_last(v, w[0]).astype(BF), dot_last(v, w[1]).astype(BF)], 1
            )

        def pair_parts(left, right, places, q):
            both = left.shape[1] // 2
            return [
                dot_first(v, right).astype(BF).reshape(places, m, q, right.shape[1])
                for v in (left[:, both:], left[:, :both])
            ]

        def rows_parts(left, right):
            q = half // m
            both = left.shape[1] // 2
            out = []
            for h in (1, 0):
                v = left[:, h * both : (h + 1) * both]
                g = dot_first(v, right).astype(BF)
                out.append(g.reshape(both // (m * q), m, q, right.shape[1]))
            return out

        def halves(v):
            both = v.shape[1] // 2
            return jnp.concatenate(
                [cut(v, core * both, both, 1), cut(v, (1 - core) * both, both, 1)], 1
            )

        inputs = activations[0].astype(F32)
        all_inputs = gather(activations[0])
        w_qkv = exchange_weights([query_weight, key_weight, value_weight])
        w_mlp = exchange_weights([gate_weight, up_weight])
        all_grads = gather(cotangent[0])

        seg_ids = segments[0]
        pos = positions(seg_ids)
        tokens = jnp.arange(length, dtype=jnp.int32)
        shuffle = lambda v: jnp.concatenate([cut(v, owner[k] * rows, rows, 0) for k in range(n)])
        index, seg_ids, pos = shuffle(tokens), shuffle(seg_ids), shuffle(pos)
        inv_freq = 1.0 / ROPE_BASE ** (jnp.arange(HD // 2, dtype=F32) * (2.0 / HD))
        angles = pos[:, None] * inv_freq[None, :]
        cosine, sine = jnp.cos(angles), jnp.sin(angles)
        cos2 = jnp.concatenate([cosine, cosine], 1)
        sin2 = jnp.concatenate([-sine, sine], 1)
        tcol = jnp.stack([index, seg_ids], 0)
        trow = jnp.stack([index, seg_ids], 1)
        qg, kg = query_gain[None], key_gain[None]

        wide = all_inputs.astype(F32)
        r1 = lax.rsqrt(jnp.mean(wide * wide, -1, keepdims=True) + EPSILON)
        normed = reorder((wide * r1 * attn_gain).astype(BF))
        qkv = times(normed, w_qkv)
        attn_out, qr, kr, vb = attention(qkv, nq, nk, qg, kg, cos2, sin2, trow, tcol)

        hidden = inputs + scatter_sum(dot(attn_out, out_weight).reshape(n, rows, width))
        r2 = lax.rsqrt(jnp.mean(hidden * hidden, -1, keepdims=True) + EPSILON)
        normed_mlp = reorder(gather((hidden * r2 * mlp_gain).astype(BF)))
        pre = times(normed_mlp, w_mlp)
        gate_pre, up_pre = pre[:, :ffl], pre[:, ffl:]
        sig = jax.nn.sigmoid(gate_pre)
        activated = (gate_pre * sig * up_pre).astype(BF)
        down_pair = rows_parts(halves(activated), all_grads)
        grad_act = dot_last(all_grads, down_weight)
        grad_gate = (grad_act * up_pre * sig * (1.0 + gate_pre * (1.0 - sig))).astype(BF)
        grad_up = (grad_act * gate_pre * sig).astype(BF)
        grad_pre = jnp.concatenate([grad_gate, grad_up], 1)
        mlp_pair = pair_parts(normed_mlp, grad_pre, n, half // m)
        dhn = scatter_sum(restore(times_back(grad_pre, w_mlp)).reshape(n, rows, width))
        output = (
            hidden + scatter_sum(dot(activated, down_weight).reshape(n, rows, width))
        ).astype(BF)[None]

        hh = hidden * r2
        grad_mlp_gain = jnp.sum(dhn * hh, 0)
        weighted = dhn * mlp_gain
        grad_hidden = cotangent[0].astype(F32) + r2 * (
            weighted - hh * jnp.mean(weighted * hh, -1, keepdims=True)
        )
        grad_branch = gather(grad_hidden.astype(BF))
        do = dot_last(grad_branch, out_weight).astype(BF)
        dq, dk, dv, gq, gk = attention_back(
            qkv, qr, kr, vb, do, nq, nk, qg, kg, cos2, sin2, trow, tcol
        )
        dqkv = jnp.concatenate([dq, dk, dv], 1)
        dnormed = scatter_sum(restore(times_back(dqkv, w_qkv)).reshape(n, rows, width))
        r1_own = lax.rsqrt(jnp.mean(inputs * inputs, -1, keepdims=True) + EPSILON)
        xh = inputs * r1_own
        grad_attn_gain = jnp.sum(dnormed * xh, 0)
        weighted = dnormed * attn_gain
        grad_input = (
            grad_hidden + r1_own * (weighted - xh * jnp.mean(weighted * xh, -1, keepdims=True))
        )[None]
        gains = jnp.concatenate(
            [grad_attn_gain, grad_mlp_gain, jnp.sum(gq[:, 0], 0), jnp.sum(gk[:, 0], 0)]
        )
        gains = jnp.pad(gains, (0, -gains.size % (8 * HD))).reshape(-1, HD)

        segments_of = [
            down_pair,
            mlp_pair,
            rows_parts(halves(attn_out), grad_branch),
            pair_parts(normed, dqkv, n, half // m),
        ]
        places = [v[0].shape[0] for v in segments_of]
        parts = [(0, a, 0) for a in range(places[0])] + [(1, k, k) for k in range(n)]
        parts += [(2, a, 0) for a in range(places[2])] + [(3, k, k) for k in range(n)]
        gains, *summed = reduce_gradients(
            n, m, gains, [v[0] for v in segments_of], [v[1] for v in segments_of], parts
        )
        mines, others = summed[:4], summed[4:]

        pick = lambda seg, at=None, width=None: (
            (mines[seg], others[seg]) if at is None else (mines[seg], others[seg], at, width)
        )
        (
            grad_down, grad_out_weight, grad_gate_weight, grad_up_weight,
            grad_query_weight, grad_key_weight, grad_value_weight,
        ) = assemble(
            [pick(0), pick(2)],
            [
                pick(1, 0, ffl), pick(1, 1, ffl), pick(3, 0, nq * HD),
                pick(3, nq // nk, nk * HD), pick(3, nq // nk + 1, nk * HD),
            ],
            core,
            owner,
        )
        gains = gains.reshape(-1)
        grad_attn_gain, grad_mlp_gain = gains[:width], gains[width : 2 * width]
        grad_query_gain = gains[2 * width : 2 * width + HD]
        grad_key_gain = gains[2 * width + HD : 2 * width + 2 * HD]
        return (
            output,
            grad_input,
            grad_attn_gain,
            grad_query_weight,
            grad_key_weight,
            grad_value_weight,
            grad_query_gain,
            grad_key_gain,
            grad_out_weight,
            grad_mlp_gain,
            grad_gate_weight,
            grad_up_weight,
            grad_down,
        )

    return per_device


def solution(mesh):
    tok = P("rep", "shard", None)
    row = P("shard", None)
    return jax.shard_map(
        build(mesh.shape["shard"], mesh.shape["rep"]),
        mesh=mesh,
        in_specs=(
            tok, P("rep", None), P(), row, row, row, P(), P(), row, P(), row, row, row, tok,
        ),
        out_specs=(tok, tok, P(), row, row, row, P(), P(), row, P(), row, row, row),
        check_vma=False,
    )
```

```python
from functools import partial
import math

import jax
import jax.numpy as jnp
from jax import lax
from jax.experimental import pallas as pl
from jax.experimental.pallas import tpu as pltpu
from jax.sharding import PartitionSpec as P

HQ = 16
HK = 8
HD = 128
FF = 6144
GROUPS = HQ // HK

EPSILON = 1e-06
ROPE_BASE = 1000000.0
MASKED = -1e30
BF = jnp.bfloat16
F32 = jnp.float32
AXES = ("shard", "rep")


def dot(a, b):
    return jnp.dot(a, b, preferred_element_type=F32)


def dot_last(a, b):
    return lax.dot_general(a, b, (((1,), (1,)), ((), ())), preferred_element_type=F32)


def dot_first(a, b):
    return lax.dot_general(a, b, (((0,), (0,)), ((), ())), preferred_element_type=F32)


def positions(seg_ids):
    token_index = jnp.arange(seg_ids.shape[0], dtype=jnp.int32)
    before = jnp.concatenate([jnp.full((1,), -1, jnp.int32), seg_ids[:-1]])
    starts = lax.cummax(
        jnp.where(seg_ids != before, token_index, jnp.zeros_like(token_index)), axis=0
    )
    return (token_index - starts).astype(F32)


def head_rope(raw, gain, cos2, sin2):
    rstat = lax.rsqrt(jnp.mean(raw * raw, -1, keepdims=True) + EPSILON)
    scaled = raw * rstat * gain
    return scaled * cos2 + pltpu.roll(scaled, HD // 2, 1) * sin2


def attend_pair(qkv, j, nq, nk, qg, kg, cos2, sin2, trow, tcol, o_ref, qr_ref, kr_ref, vb_ref, scale):
    length = qkv.shape[0]
    block = min(length, 512)
    own = slice(j * HD, (j + 1) * HD)
    at = (nq + j) * HD
    kr = head_rope(qkv[:, at : at + HD], kg[...], cos2[...], sin2[...]).astype(BF)
    at = (nq + nk + j) * HD
    vb = qkv[:, at : at + HD].astype(BF)
    kr_ref[:, own] = kr
    vb_ref[:, own] = vb
    for g in range(GROUPS):
        cols = slice((j * GROUPS + g) * HD, (j * GROUPS + g + 1) * HD)
        qr_ref[:, cols] = head_rope(qkv[:, cols], qg[...], cos2[...], sin2[...]).astype(BF)
        for b in range(length // block):
            rows = slice(b * block, (b + 1) * block)
            s = dot_last(qr_ref[rows, cols], kr) * scale
            seen = (tcol[0:1, :] <= trow[rows, 0:1]) & (tcol[1:2, :] == trow[rows, 1:2])
            s = jnp.where(seen, s, MASKED)
            e = jnp.exp(s - jnp.max(s, -1, keepdims=True))
            p = (e / jnp.sum(e, -1, keepdims=True)).astype(BF)
            o_ref[rows, cols] = dot(p, vb).astype(BF)


def head_back(grad_rot, raw, gain, cos2, sin2):
    back = grad_rot * cos2 - pltpu.roll(grad_rot, HD // 2, 1) * sin2
    rstat = lax.rsqrt(jnp.mean(raw * raw, -1, keepdims=True) + EPSILON)
    scaled = raw * rstat
    gain_part = jnp.sum(back * scaled, 0, keepdims=True)
    b = back * gain
    return rstat * (b - scaled * jnp.mean(b * scaled, -1, keepdims=True)), gain_part


def attend_back_kernel(
    q_ref, k_ref, qr_ref, kr_ref, vb_ref, do_ref, qg_ref, kg_ref, cos_ref, sin_ref,
    trow_ref, tcol_ref, dq_ref, dk_ref, dv_ref, gq_ref, gk_ref, *, scale, block
):
    cos2 = cos_ref[...]
    sin2 = sin_ref[...]
    kr = kr_ref[...]
    vb = vb_ref[...]
    length = kr.shape[0]
    dkr = jnp.zeros((length, HD), F32)
    dv = jnp.zeros((length, HD), F32)
    gq = jnp.zeros((1, HD), F32)
    for g in range(GROUPS):
        cols = slice(g * HD, (g + 1) * HD)
        dqr = []
        for b in range(length // block):
            rows = slice(b * block, (b + 1) * block)
            qr = qr_ref[rows, cols]
            do = do_ref[rows, cols]
            s = dot_last(qr, kr) * scale
            seen = (tcol_ref[0:1, :] <= trow_ref[rows, 0:1]) & (
                tcol_ref[1:2, :] == trow_ref[rows, 1:2]
            )
            s = jnp.where(seen, s, MASKED)
            e = jnp.exp(s - jnp.max(s, -1, keepdims=True))
            p = e / jnp.sum(e, -1, keepdims=True)
            dp = dot_last(do, vb)
            ds = (p * (dp - jnp.sum(p * dp, -1, keepdims=True))).astype(BF)
            dqr.append(dot(ds, kr) * scale)
            dkr += dot_first(ds, qr)
            dv += dot_first(p.astype(BF), do)
        dqr = dqr[0] if len(dqr) == 1 else jnp.concatenate(dqr, 0)
        dq, part = head_back(dqr, q_ref[:, cols], qg_ref[...], cos2, sin2)
        dq_ref[:, cols] = dq.astype(BF)
        gq += part
    dk, gk = head_back(dkr * scale, k_ref[...], kg_ref[...], cos2, sin2)
    dk_ref[...] = dk.astype(BF)
    dv_ref[...] = dv.astype(BF)
    gq_ref[...] = jnp.broadcast_to(gq[None], gq_ref.shape)
    gk_ref[...] = jnp.broadcast_to(gk[None], gk_ref.shape)


def const_spec(shape):
    return pl.BlockSpec(shape, lambda j: (0,) * len(shape))


def attention_back(qkv, qr, kr, vb, do, nq, nk, qg, kg, cos2, sin2, trow, tcol):
    length = qkv.shape[0]
    block = min(length, 512)
    wide = GROUPS * HD
    col = lambda width, off: pl.BlockSpec((length, width), lambda j: (0, off + j))
    gain_spec = pl.BlockSpec((1, 8, HD), lambda j: (j, 0, 0))
    return pl.pallas_call(
        partial(attend_back_kernel, scale=1.0 / math.sqrt(HD), block=block),
        grid=(nk,),
        out_shape=(
            jax.ShapeDtypeStruct((length, nq * HD), BF),
            jax.ShapeDtypeStruct((length, nk * HD), BF),
            jax.ShapeDtypeStruct((length, nk * HD), BF),
            jax.ShapeDtypeStruct((nk, 8, HD), F32),
            jax.ShapeDtypeStruct((nk, 8, HD), F32),
        ),
        in_specs=[
            col(wide, 0), col(HD, nq), col(wide, 0), col(HD, 0), col(HD, 0), col(wide, 0),
            const_spec((1, HD)), const_spec((1, HD)),
            const_spec((length, HD)), const_spec((length, HD)),
            const_spec((length, 2)), const_spec((2, length)),
        ],
        out_specs=(col(wide, 0), col(HD, 0), col(HD, 0), gain_spec, gain_spec),
        compiler_params=pltpu.CompilerParams(vmem_limit_bytes=48 << 20),
        name="attend_back",
    )(qkv, qkv, qr, kr, vb, do, qg, kg, cos2, sin2, trow, tcol)


def assemble_kernel(counts, order_ref, *refs):
    n_rows, n_cols = counts
    total = n_rows + n_cols
    mine, other, outs = refs[:total], refs[total : 2 * total], refs[2 * total :]

    def fill(sources):
        for src, out in zip(sources, outs):
            m, places, q, width = src.shape
            for a in range(places):
                out[a * m * q : (a + 1) * m * q, :] = (
                    src[:, a].reshape(m * q, width).astype(F32)
                )

    pl.when(pl.program_id(0) == 0)(lambda: fill(mine))
    pl.when(pl.program_id(0) == 1)(lambda: fill(other))


def assemble(rows, cols, core, owner):
    n = len(owner)
    order = jnp.stack(list(owner) + [core]).astype(jnp.int32)
    in_specs, out_specs, shapes, operands = [[], []], [], [], [[], []]
    size = 0
    for mine, other in rows:
        m, places, q, width = mine.shape
        block = (m, places, q, width // n)
        in_specs[0].append(
            pl.BlockSpec(block, lambda g, b, o: (0, 0, 0, jnp.where(g == 0, b, n - 1)))
        )
        in_specs[1].append(
            pl.BlockSpec(block, lambda g, b, o: (0, 0, 0, jnp.where(g == 0, 0, b)))
        )
        out_specs.append(
            pl.BlockSpec((places * m * q, width // n), lambda g, b, o: (g ^ o[n], b))
        )
        shapes.append(jax.ShapeDtypeStruct((2 * places * m * q, width), F32))
        operands[0].append(mine)
        operands[1].append(other)
        size += mine.size
    for mine, other, at, width in cols:
        m, _, q, _ = mine.shape
        block = (m, 1, q, width)
        in_specs[0].append(
            pl.BlockSpec(block, lambda g, b, o, at=at: (0, o[jnp.where(g == 0, b, n - 1)], 0, at))
        )
        in_specs[1].append(
            pl.BlockSpec(block, lambda g, b, o, at=at: (0, o[jnp.where(g == 0, 0, b)], 0, at))
        )
        out_specs.append(pl.BlockSpec((m * q, width), lambda g, b, o: (g ^ o[n], b)))
        shapes.append(jax.ShapeDtypeStruct((2 * m * q, n * width), F32))
        operands[0].append(mine)
        operands[1].append(other)
        size += m * n * q * width
    return pl.pallas_call(
        partial(assemble_kernel, (len(rows), len(cols))),
        out_shape=tuple(shapes),
        grid_spec=pltpu.PrefetchScalarGridSpec(
            num_scalar_prefetch=1,
            grid=(2, n),
            in_specs=in_specs[0] + in_specs[1],
            out_specs=tuple(out_specs),
        ),
        compiler_params=pltpu.CompilerParams(vmem_limit_bytes=56 << 20),
        cost_estimate=pl.CostEstimate(flops=0, bytes_accessed=12 * size, transcendentals=0),
        name="assemble",
    )(order, *operands[0], *operands[1])


MESH_ID = pl.DeviceIdType.MESH


def reduce_kernel(n, m, parts, *refs):
    count = 4
    gain_ref, refs = refs[0], refs[1:]
    gain_out, refs = refs[2 * count], refs[: 2 * count] + refs[2 * count + 1 :]
    sends, keeps = refs[:count], refs[count : 2 * count]
    mines, others = refs[2 * count : 3 * count], refs[3 * count : 4 * count]
    refs = refs[4 * count :]
    keep_v, away_v = refs[:count], refs[count : 2 * count]
    (ups, downs, tots, fins, load_sem, pair_s, pair_r, up_s, up_r, down_s, down_r,
     peer_s, peer_r, gup_s, gup_r, gdown_s, gdown_r, sib_s, sib_r, own_sem, gain_pair, gain_group, gain_line,
     gain_s, gain_r) = refs[2 * count :]
    shard, rep = lax.axis_index("shard"), lax.axis_index("rep")
    i = rep // 2
    core = lax.rem(rep, 2)
    sibling = {"rep": 2 * i + 1 - core}
    above, below = {"rep": rep + 2}, {"rep": rep - 2}
    peers = [None] + [{"shard": shard ^ k} for k in range(1, n)]
    has_up, has_down = i < m - 1, i > 0

    barrier = pltpu.get_barrier_semaphore()

    def greet(dev):
        pl.semaphore_signal(barrier, inc=1, device_id=dev, device_id_type=MESH_ID)

    greet(sibling)
    for k in range(1, n):
        greet(peers[k])
    line = [None] + [{"rep": 2 * lax.rem(i + d, m) + core} for d in range(1, m)]
    for d in range(1, m):
        greet(line[d])
    pl.semaphore_wait(barrier, n + m - 1)

    def remote(src, dst, ssem, rsem, dev):
        return pltpu.make_async_remote_copy(
            src_ref=src, dst_ref=dst, send_sem=ssem, recv_sem=rsem,
            device_id=dev, device_id_type=MESH_ID,
        )

    def chunk(ref, part, j):
        seg, at, _ = part
        return ref[seg].at[at, j]

    def out(ref, part, j):
        seg, at, _ = part
        return ref[seg].at[j, at]

    def pair_copy(p):
        seg, at, _ = parts[p]
        return remote(sends[seg].at[at], away_v[seg].at[at], pair_s.at[p], pair_r.at[p], sibling)

    def load_copy(p):
        seg, at, _ = parts[p]
        return pltpu.make_async_copy(keeps[seg].at[at], keep_v[seg].at[at], load_sem.at[p])

    def slot(ref, p, t):
        return ref[parts[p][0]].at[parts[p][1], t]

    def up_copy(p, t, src):
        return remote(src, slot(ups, p, t), up_s.at[p, t], up_r.at[p, t], above)

    def down_copy(p, t, src):
        return remote(src, slot(downs, p, t), down_s.at[p, t], down_r.at[p, t], below)

    def add_into(ref, other):
        ref[...] = (ref[...].astype(F32) + other[...].astype(F32)).astype(BF)

    def scatter_step(p, t):
        part = parts[p]
        if t > 0:

            @pl.when((i > 0) & (i <= t) & has_up)
            def _():
                up_copy(p, t - 1, slot(ups, p, t - 1)).wait_recv()
                add_into(slot(ups, p, t - 1), chunk(keep_v, part, m - 1 - t + i))

            @pl.when((i < m - 1) & (i >= m - 1 - t) & has_down)
            def _():
                down_copy(p, t - 1, slot(downs, p, t - 1)).wait_recv()
                add_into(slot(downs, p, t - 1), chunk(keep_v, part, i - (m - 1 - t)))

            pl.when((i > 0) & (i <= t) & has_up)(
                lambda: up_copy(p, t, slot(ups, p, t - 1)).start()
            )
            pl.when((i < m - 1) & (i >= m - 1 - t) & has_down)(
                lambda: down_copy(p, t, slot(downs, p, t - 1)).start()
            )
        pl.when(i == 0)(lambda: up_copy(p, t, chunk(keep_v, part, m - 1 - t)).start())
        pl.when(i == m - 1)(lambda: down_copy(p, t, chunk(keep_v, part, t)).start())

    def peer_copy(p):
        seg, at, k = parts[p]
        return remote(tots[seg].at[at], fins[seg].at[at], peer_s.at[p], peer_r.at[p], peers[k])

    def total(p):
        seg, at, k = parts[p]
        part = parts[p]
        pl.when(has_down)(lambda: up_copy(p, m - 2, slot(ups, p, m - 2)).wait_recv())
        pl.when(has_up)(lambda: down_copy(p, m - 2, slot(downs, p, m - 2)).wait_recv())
        where = fins[seg].at[at] if k == 0 else tots[seg].at[at]

        def put(*extra):
            value = chunk(keep_v, part, i)[...].astype(F32)
            for e in extra:
                value = value + e[...].astype(F32)
            where[...] = value.astype(BF)

        u, d = slot(ups, p, m - 2), slot(downs, p, m - 2)
        pl.when(has_up & has_down)(lambda: put(u, d))
        pl.when(has_up & (i == 0))(lambda: put(d))
        pl.when(has_down & (i == m - 1))(lambda: put(u))
        if k != 0:
            peer_copy(p).start()

    def gup_copy(p, t, j, src):
        return remote(src, out(mines, parts[p], j), gup_s.at[p, t], gup_r.at[p, t], above)

    def gdown_copy(p, t, j, src):
        return remote(src, out(mines, parts[p], j), gdown_s.at[p, t], gdown_r.at[p, t], below)

    def sib_copy(p, j, src):
        return remote(src, out(others, parts[p], j), sib_s.at[p, j], sib_r.at[p, j], sibling)

    def gather_step(p, t):
        part = parts[p]
        if t == 0:
            seg, at, k = part
            if k != 0:
                peer_copy(p).wait_recv()
            fin = fins[seg].at[at]
            pl.when(has_up)(lambda: gup_copy(p, 0, i, fin).start())
            pl.when(has_down)(lambda: gdown_copy(p, 0, i, fin).start())
            sib_copy(p, i, fin).start()
            pltpu.make_async_copy(fin, out(mines, part, i), own_sem.at[p]).start()
            return

        @pl.when(i - t >= 0)
        def _():
            here = out(mines, part, i - t)
            gup_copy(p, t - 1, i - t, here).wait_recv()
            if t < m - 1:
                pl.when(has_up)(lambda: gup_copy(p, t, i - t, here).start())
            sib_copy(p, i - t, here).start()

        @pl.when(i + t < m)
        def _():
            here = out(mines, part, i + t)
            gdown_copy(p, t - 1, i + t, here).wait_recv()
            if t < m - 1:
                pl.when(has_down)(lambda: gdown_copy(p, t, i + t, here).start())
            sib_copy(p, i + t, here).start()

    def gain_copies(level):
        if level == 0:
            return [remote(gain_ref, gain_pair, gain_s.at[0], gain_r.at[0], sibling)]
        if level == 1:
            return [
                remote(
                    gain_group.at[shard], gain_group.at[shard], gain_s.at[k], gain_r.at[k], peers[k]
                )
                for k in range(1, n)
            ]
        return [
            remote(
                gain_line.at[i], gain_line.at[i], gain_s.at[n - 1 + d], gain_r.at[n - 1 + d], line[d]
            )
            for d in range(1, m)
        ]

    def gains(level):
        if level > 0:
            for copy in gain_copies(level - 1):
                copy.wait_recv()
        if level == 1:
            gain_group[shard] = gain_ref[...] + gain_pair[...]
        elif level == 2:
            value = gain_group[0]
            for k in range(1, n):
                value = value + gain_group[k]
            gain_line[i] = value
        elif level == 3:
            value = gain_line[0]
            for k in range(1, m):
                value = value + gain_line[k]
            gain_out[...] = value
        if level < 3:
            for copy in gain_copies(level):
                copy.start()

    def first(p):
        seg, at, _ = parts[p]
        load_copy(p).wait()
        pair_copy(p).wait_recv()
        for j in range(m):
            add_into(keep_v[seg].at[at, j], away_v[seg].at[at, j])
        scatter_step(p, 0)

    stages = [first] + [lambda p, t=t: scatter_step(p, t) for t in range(1, m - 1)]
    stages += [total] + [lambda p, t=t: gather_step(p, t) for t in range(m)]

    for p in range(len(parts)):
        pair_copy(p).start()
        load_copy(p).start()
    for tick in range(len(parts) + len(stages) - 1):
        if tick < 4:
            gains(tick)
        for st in range(len(stages) - 1, -1, -1):
            p = tick - st
            if 0 <= p < len(parts):
                stages[st](p)

    for level in range(3):
        for copy in gain_copies(level):
            copy.wait_send()
    for p in range(len(parts)):
        part = parts[p]
        seg, at, k = part
        pair_copy(p).wait_send()
        if k != 0:
            peer_copy(p).wait_send()
        pltpu.make_async_copy(fins[seg].at[at], out(mines, part, i), own_sem.at[p]).wait()
        for t in range(m - 1):
            pl.when((i <= t) & has_up)(lambda: up_copy(p, t, slot(ups, p, t)).wait_send())
            pl.when((i >= m - 1 - t) & has_down)(
                lambda: down_copy(p, t, slot(downs, p, t)).wait_send()
            )
            pl.when((i - t >= 0) & has_up)(
                lambda: gup_copy(p, t, i, fins[seg].at[at]).wait_send()
            )
            pl.when((i + t < m) & has_down)(
                lambda: gdown_copy(p, t, i, fins[seg].at[at]).wait_send()
            )
        for j in range(m):
            copy = sib_copy(p, j, fins[seg].at[at])
            copy.wait_send()
            copy.wait_recv()


def reduce_gradients(n, m, gains, sends, keeps, parts):
    count, total = len(keeps), len(parts)
    dma = pltpu.SemaphoreType.DMA
    hbm = pl.BlockSpec(memory_space=pl.ANY)

    def slots(extra):
        return [
            pltpu.VMEM((v.shape[0],) + extra + v.shape[2:], BF) for v in keeps
        ]

    outs = [
        jax.ShapeDtypeStruct((m, v.shape[0]) + v.shape[2:], BF) for v in keeps
    ]
    sent = sum(v.size for v in keeps) * 2
    return pl.pallas_call(
        partial(reduce_kernel, n, m, parts),
        out_shape=tuple([jax.ShapeDtypeStruct(gains.shape, F32)] + outs + outs),
        in_specs=[pl.BlockSpec(memory_space=pltpu.VMEM)] + [hbm] * (2 * count),
        out_specs=tuple([pl.BlockSpec(memory_space=pltpu.VMEM)] + [hbm] * (2 * count)),
        scratch_shapes=[pltpu.VMEM(v.shape, BF) for v in keeps]
        + [pltpu.VMEM(v.shape, BF) for v in keeps]
        + [slots((m - 1,)), slots((m - 1,)), slots(()), slots(())]
        + [
            dma((total,)), dma((total,)), dma((total,)),
            dma((total, m - 1)), dma((total, m - 1)), dma((total, m - 1)), dma((total, m - 1)),
            dma((total,)), dma((total,)),
            dma((total, m - 1)), dma((total, m - 1)), dma((total, m - 1)), dma((total, m - 1)),
            dma((total, m)), dma((total, m)), dma((total,)),
            pltpu.VMEM(gains.shape, F32), pltpu.VMEM((n,) + gains.shape, F32),
            pltpu.VMEM((m,) + gains.shape, F32), dma((n + m,)), dma((n + m,)),
        ],
        compiler_params=pltpu.CompilerParams(
            collective_id=3, has_side_effects=True, vmem_limit_bytes=60 << 20
        ),
        cost_estimate=pl.CostEstimate(flops=0, bytes_accessed=4 * sent, transcendentals=0),
        name="reduce_gradients",
    )(gains, *sends, *keeps)


def front_kernel(
    n, m, nq, nk, scale,
    x_hbm, dy_hbm, wq, wk, wv, wg, wu, wo_hbm,
    ag, qg, kg, mg, cos2, sin2, trow, tcol,
    normed, qkv, qr, kr, vb, o, hidden, hn, qkv_mine, qkv_other, mlp_mine, mlp_other, dy_all,
    x_all, wo, bounce, dy_v, hn_all, part_own, part_s, part_r,
    x_ss, x_rs, w_ss, w_rs, up_ss, up_rs, down_ss, down_rs, sib_ss, sib_rs,
    own_sem, back_sem, load_sem, part_ss, part_rs, hn_ss, hn_rs, dy_ss, dy_rs
):
    shard, rep = lax.axis_index("shard"), lax.axis_index("rep")
    i = rep // 2
    core = lax.rem(rep, 2)
    sibling = {"rep": 2 * i + 1 - core}
    above, below = {"rep": rep + 2}, {"rep": rep - 2}
    peers = [None] + [{"shard": shard ^ k} for k in range(1, n)]
    has_up, has_down = i < m - 1, i > 0
    rows, width = x_all.shape[1], x_all.shape[2]
    own = width // n
    half = own // 2

    barrier = pltpu.get_barrier_semaphore()

    def greet(dev):
        pl.semaphore_signal(barrier, inc=1, device_id=dev, device_id_type=MESH_ID)

    greet(sibling)
    for k in range(1, n):
        greet(peers[k])
    for d in range(1, m):
        greet({"rep": 2 * lax.rem(i + d, m) + core})
    pl.semaphore_wait(barrier, n + m - 1)

    def remote(src, dst, ssem, rsem, dev):
        return pltpu.make_async_remote_copy(
            src_ref=src, dst_ref=dst, send_sem=ssem, recv_sem=rsem,
            device_id=dev, device_id_type=MESH_ID,
        )

    groups = [
        ([wq, wk, wv], qkv_mine, qkv_other),
        ([wg, wu], mlp_mine, mlp_other),
    ]

    def fields(weights):
        at = 0
        for w in weights:
            size = w.shape[3] // n
            yield w, at, size
            at += size

    def cols_of(k, size):
        return pl.ds(pl.multiple_of((shard ^ k) * size, size), size)

    def piece_copies(g, k):
        weights, mine, _ = groups[g]
        return [
            remote(
                w.at[core, i, :, cols_of(k, size)],
                mine.at[k, i, :, pl.ds(at, size)],
                w_ss.at[g, k, f], w_rs.at[g, k, f], peers[k],
            )
            for f, (w, at, size) in enumerate(fields(weights))
        ]

    def own_copies(g):
        weights, mine, other = groups[g]
        out = []
        for h, dst in enumerate((mine, other)):
            for f, (w, at, size) in enumerate(fields(weights)):
                to = dst.at[0, :, :, pl.ds(at, size)] if g == 0 else bounce.at[h, :, :, pl.ds(at, size)]
                src = w.at[core if h == 0 else 1 - core, :, :, cols_of(0, size)]
                out.append(pltpu.make_async_copy(src, to, own_sem.at[g, h, f]))
        return out

    def back_copies():
        return [
            pltpu.make_async_copy(bounce.at[h], dst.at[0], back_sem.at[h])
            for h, dst in enumerate((mlp_mine, mlp_other))
        ]

    def region(ref, j):
        return ref.at[pl.ds(1, n - 1), j]

    def up_copy(g, t, j):
        r = region(groups[g][1], j)
        return remote(r, r, up_ss.at[g, t], up_rs.at[g, t], above)

    def down_copy(g, t, j):
        r = region(groups[g][1], j)
        return remote(r, r, down_ss.at[g, t], down_rs.at[g, t], below)

    def sib_copy(g, j):
        _, mine, other = groups[g]
        return remote(region(mine, j), region(other, j), sib_ss.at[g, j], sib_rs.at[g, j], sibling)

    def gather_weights(g, t):
        if t == 0:
            for k in range(1, n):
                for copy in piece_copies(g, k):
                    copy.wait_recv()
            pl.when(has_up)(lambda: up_copy(g, 0, i).start())
            pl.when(has_down)(lambda: down_copy(g, 0, i).start())
            sib_copy(g, i).start()
            return

        @pl.when(i - t >= 0)
        def _():
            up_copy(g, t - 1, i - t).wait_recv()
            if t < m - 1:
                pl.when(has_up)(lambda: up_copy(g, t, i - t).start())
            sib_copy(g, i - t).start()

        @pl.when(i + t < m)
        def _():
            down_copy(g, t - 1, i + t).wait_recv()
            if t < m - 1:
                pl.when(has_down)(lambda: down_copy(g, t, i + t).start())
            sib_copy(g, i + t).start()

    def x_copy(k):
        return remote(x_hbm, x_all.at[k], x_ss.at[k], x_rs.at[k], peers[k])

    def dy_copy(k):
        return remote(dy_hbm, dy_all.at[k], dy_ss.at[k], dy_rs.at[k], peers[k])

    def hn_copy(k):
        return remote(hn_all.at[0], hn_all.at[k], hn_ss.at[k], hn_rs.at[k], peers[k])

    def part_copy(k):
        return remote(part_s.at[k], part_r.at[k], part_ss.at[k], part_rs.at[k], peers[k])

    load_x = pltpu.make_async_copy(x_hbm, x_all.at[0], load_sem.at[0])
    load_wo = pltpu.make_async_copy(wo_hbm, wo, load_sem.at[1])
    load_dy = pltpu.make_async_copy(dy_hbm, dy_v, load_sem.at[2])
    keep_dy = pltpu.make_async_copy(dy_v, dy_all.at[0], load_sem.at[3])

    load_x.start()
    for k in range(1, n):
        for copy in piece_copies(0, k):
            copy.start()
    for k in range(1, n):
        x_copy(k).start()
    for copy in own_copies(0):
        copy.start()
    for k in range(1, n):
        for copy in piece_copies(1, k):
            copy.start()
    for copy in own_copies(1):
        copy.start()
    load_wo.start()
    load_dy.start()

    def place(k, h, kk):
        return pl.ds(
            pl.multiple_of((shard ^ kk) * own + (core if h == 0 else 1 - core) * half, half), half
        )

    gather_weights(0, 0)
    for k in range(n):
        if k == 0:
            load_x.wait()
        else:
            x_copy(k).wait_recv()
        v = x_all[k].astype(F32)
        r = lax.rsqrt(jnp.mean(v * v, -1, keepdims=True) + EPSILON)
        for h in range(2):
            for kk in range(n):
                at = place(k, h, kk)
                normed[k * rows : (k + 1) * rows, (h * n + kk) * half : (h * n + kk + 1) * half] = (
                    x_all[k, :, at].astype(F32) * r * ag[:, at]
                ).astype(BF)
    for t in range(1, m - 1):
        gather_weights(0, t)
    gather_weights(1, 0)
    gather_weights(0, m - 1)
    for copy in own_copies(0):
        copy.wait()
    for j in range(m):
        sib_copy(0, j).wait_recv()

    cols = qkv.shape[1]
    step = min(cols, 256)

    @pl.loop(0, cols // step)
    def _(b):
        at = pl.ds(pl.multiple_of(b * step, step), step)
        both = n * half
        qkv[:, at] = dot(
            normed[:, :both], qkv_mine[:, :, :, at].reshape(both, step)
        ) + dot(normed[:, both:], qkv_other[:, :, :, at].reshape(both, step))

    hop = 1
    for copy in own_copies(1):
        copy.wait()
    for copy in back_copies():
        copy.start()
    load_dy.wait()
    keep_dy.start()
    for j in range(nk):
        attend_pair(qkv, j, nq, nk, qg, kg, cos2, sin2, trow, tcol, o, qr, kr, vb, scale)
        if j == 0 and hop < m - 1:
            gather_weights(1, hop)
            hop += 1

    load_wo.wait()
    step = min(width, 512)

    @pl.loop(0, width // step)
    def _(b):
        at = pl.ds(pl.multiple_of(b * step, step), step)
        for k in range(n):
            value = dot(o[k * rows : (k + 1) * rows, :], wo[:, at])
            if k == 0:
                part_own[:, at] = value
            else:
                part_s[k, :, at] = value.astype(BF)

    for k in range(1, n):
        part_copy(k).start()
    if hop < m - 1:
        gather_weights(1, hop)
        hop += 1
    total = x_all[0].astype(F32) + part_own[...]
    for k in range(1, n):
        part_copy(k).wait_recv()
        total = total + part_r[k].astype(F32)
    hidden[...] = total
    r = lax.rsqrt(jnp.mean(total * total, -1, keepdims=True) + EPSILON)
    hn_all[0] = (total * r * mg[...]).astype(BF)
    for k in range(1, n):
        hn_copy(k).start()
    for k in range(1, n):
        dy_copy(k).start()
    while hop < m - 1:
        gather_weights(1, hop)
        hop += 1
    for k in range(n):
        if k > 0:
            hn_copy(k).wait_recv()
        for h in range(2):
            for kk in range(n):
                hn[k * rows : (k + 1) * rows, (h * n + kk) * half : (h * n + kk + 1) * half] = (
                    hn_all[k, :, place(k, h, kk)]
                )
    gather_weights(1, m - 1)

    for copy in back_copies():
        copy.wait()
    keep_dy.wait()
    for k in range(1, n):
        for g in range(2):
            for copy in piece_copies(g, k):
                copy.wait_send()
        x_copy(k).wait_send()
        part_copy(k).wait_send()
        hn_copy(k).wait_send()
        dy_copy(k).wait_send()
        dy_copy(k).wait_recv()
    for g in range(2):
        for j in range(m):
            sib_copy(g, j).wait_send()
            if g == 1:
                sib_copy(g, j).wait_recv()
        for t in range(m - 1):
            pl.when((i - t >= 0) & has_up)(lambda: up_copy(g, t, i).wait_send())
            pl.when((i + t < m) & has_down)(lambda: down_copy(g, t, i).wait_send())


def front(n, m, nq, nk, x, dy, weights, wo, gains, tables):
    rows, width = x.shape
    length = n * rows
    q = weights[0].shape[2]
    cols = [sum(w.shape[3] // n for w in ws) for ws in (weights[:3], weights[3:])]
    vmem, hbm = pl.BlockSpec(memory_space=pltpu.VMEM), pl.BlockSpec(memory_space=pl.ANY)
    dma = pltpu.SemaphoreType.DMA
    sd = jax.ShapeDtypeStruct
    outs = [
        (sd((length, width), BF), vmem),
        (sd((length, cols[0]), F32), vmem),
        (sd((length, nq * HD), BF), vmem),
        (sd((length, nk * HD), BF), vmem),
        (sd((length, nk * HD), BF), vmem),
        (sd((length, nq * HD), BF), vmem),
        (sd((rows, width), F32), vmem),
        (sd((length, width), BF), vmem),
        (sd((n, m, q, cols[0]), BF), vmem),
        (sd((n, m, q, cols[0]), BF), vmem),
        (sd((n, m, q, cols[1]), BF), hbm),
        (sd((n, m, q, cols[1]), BF), hbm),
        (sd((n, rows, width), BF), hbm),
    ]
    return pl.pallas_call(
        partial(front_kernel, n, m, nq, nk, 1.0 / math.sqrt(HD)),
        out_shape=tuple(v[0] for v in outs),
        in_specs=[hbm] * 8 + [vmem] * 8,
        out_specs=tuple(v[1] for v in outs),
        scratch_shapes=[
            pltpu.VMEM((n, rows, width), BF),
            pltpu.VMEM(wo.shape, BF),
            pltpu.VMEM((2, m, q, cols[1]), BF),
            pltpu.VMEM((rows, width), BF),
            pltpu.VMEM((n, rows, width), BF),
            pltpu.VMEM((rows, width), F32),
            pltpu.VMEM((n, rows, width), BF),
            pltpu.VMEM((n, rows, width), BF),
            dma((n,)), dma((n,)),
            dma((2, n, 3)), dma((2, n, 3)),
            dma((2, m)), dma((2, m)), dma((2, m)), dma((2, m)), dma((2, m)), dma((2, m)),
            dma((2, 2, 3)), dma((2,)), dma((4,)),
            dma((n,)), dma((n,)), dma((n,)), dma((n,)), dma((n,)), dma((n,)),
        ],
        compiler_params=pltpu.CompilerParams(
            collective_id=1, has_side_effects=True, vmem_limit_bytes=60 << 20
        ),
        name="front",
    )(x, dy, *weights, wo, *gains, *tables)


def build(n, reps):
    m = reps // 2

    def pairs(move):
        out = []
        for s in range(n):
            for r in range(reps):
                to = move(s, r)
                if to is not None:
                    out.append((s * reps + r, to[0] * reps + to[1]))
        return out

    peer_pairs = [pairs(lambda s, r, k=k: (s ^ k, r)) for k in range(n)]

    def to_peer(v, k):
        return lax.ppermute(v, AXES, peer_pairs[k])

    def gather(v):
        return jnp.concatenate([v] + [to_peer(v, k) for k in range(1, n)], 0)

    def scatter_sum(v):
        total = v[0].astype(F32)
        for k in range(1, n):
            total = total + to_peer(v[k].astype(BF), k).astype(F32)
        return total

    def per_device(
        activations, segments, attn_gain, query_weight, key_weight, value_weight,
        query_gain, key_gain, out_weight, mlp_gain, gate_weight, up_weight, down_weight,
        cotangent,
    ):
        rows, width = activations.shape[1], activations.shape[2]
        length = segments.shape[1]
        shard = lax.axis_index("shard")
        core = lax.axis_index("rep") % 2
        own = width // n
        half = own // 2
        nq, nk = HQ // n, HK // n
        ffl = FF // n
        owner = [shard ^ k for k in range(n)]

        def cut(v, start, size, axis):
            return lax.dynamic_slice_in_dim(v, start, size, axis)

        def reorder(v):
            return jnp.concatenate(
                [
                    cut(v, owner[k] * own + (core ^ h) * half, half, 1)
                    for h in range(2)
                    for k in range(n)
                ],
                1,
            )

        def restore(v):
            return jnp.concatenate(
                [
                    cut(v, ((core ^ h) * n + owner[b]) * half, half, 1)
                    for b in range(n)
                    for h in range(2)
                ],
                1,
            )

        def times(v, w):
            both = v.shape[1] // 2
            return dot(v[:, :both], w[0]) + dot(v[:, both:], w[1])

        def times_back(v, w):
            return jnp.concatenate(
                [dot_last(v, w[0]).astype(BF), dot_last(v, w[1]).astype(BF)], 1
            )

        def pair_parts(left, right, places, q):
            both = left.shape[1] // 2
            return [
                dot_first(v, right).astype(BF).reshape(places, m, q, right.shape[1])
                for v in (left[:, both:], left[:, :both])
            ]

        def rows_parts(left, right):
            q = half // m
            both = left.shape[1] // 2
            out = []
            for h in (1, 0):
                v = left[:, h * both : (h + 1) * both]
                g = dot_first(v, right).astype(BF)
                out.append(g.reshape(both // (m * q), m, q, right.shape[1]))
            return out

        def halves(v):
            both = v.shape[1] // 2
            return jnp.concatenate(
                [cut(v, core * both, both, 1), cut(v, (1 - core) * both, both, 1)], 1
            )

        inputs = activations[0].astype(F32)
        seg_ids = segments[0]
        pos = positions(seg_ids)
        tokens = jnp.arange(length, dtype=jnp.int32)
        shuffle = lambda v: jnp.concatenate([cut(v, owner[k] * rows, rows, 0) for k in range(n)])
        index, seg_ids, pos = shuffle(tokens), shuffle(seg_ids), shuffle(pos)
        inv_freq = 1.0 / ROPE_BASE ** (jnp.arange(HD // 2, dtype=F32) * (2.0 / HD))
        angles = pos[:, None] * inv_freq[None, :]
        cosine, sine = jnp.cos(angles), jnp.sin(angles)
        cos2 = jnp.concatenate([cosine, cosine], 1)
        sin2 = jnp.concatenate([-sine, sine], 1)
        tcol = jnp.stack([index, seg_ids], 0)
        trow = jnp.stack([index, seg_ids], 1)
        qg, kg = query_gain[None], key_gain[None]

        cut_rows = lambda w: w.reshape(2, m, half // m, w.shape[1])
        (
            normed, qkv, qr, kr, vb, attn_out, hidden, normed_mlp,
            qkv_mine, qkv_other, mlp_mine, mlp_other, all_grads,
        ) = front(
            n, m, nq, nk, activations[0], cotangent[0],
            [cut_rows(w) for w in (query_weight, key_weight, value_weight, gate_weight, up_weight)],
            out_weight,
            [attn_gain[None], qg, kg, mlp_gain[None]],
            [cos2, sin2, trow, tcol],
        )
        w_qkv = [v.reshape(n * half, -1) for v in (qkv_mine, qkv_other)]
        w_mlp = [v.reshape(n * half, -1) for v in (mlp_mine, mlp_other)]
        all_grads = all_grads.reshape(length, width)
        r2 = lax.rsqrt(jnp.mean(hidden * hidden, -1, keepdims=True) + EPSILON)
        pre = times(normed_mlp, w_mlp)
        gate_pre, up_pre = pre[:, :ffl], pre[:, ffl:]
        sig = jax.nn.sigmoid(gate_pre)
        activated = (gate_pre * sig * up_pre).astype(BF)
        down_pair = rows_parts(halves(activated), all_grads)
        grad_act = dot_last(all_grads, down_weight)
        grad_gate = (grad_act * up_pre * sig * (1.0 + gate_pre * (1.0 - sig))).astype(BF)
        grad_up = (grad_act * gate_pre * sig).astype(BF)
        grad_pre = jnp.concatenate([grad_gate, grad_up], 1)
        mlp_pair = pair_parts(normed_mlp, grad_pre, n, half // m)
        dhn = scatter_sum(restore(times_back(grad_pre, w_mlp)).reshape(n, rows, width))
        output = (
            hidden + scatter_sum(dot(activated, down_weight).reshape(n, rows, width))
        ).astype(BF)[None]

        hh = hidden * r2
        grad_mlp_gain = jnp.sum(dhn * hh, 0)
        weighted = dhn * mlp_gain
        grad_hidden = cotangent[0].astype(F32) + r2 * (
            weighted - hh * jnp.mean(weighted * hh, -1, keepdims=True)
        )
        grad_branch = gather(grad_hidden.astype(BF))
        do = dot_last(grad_branch, out_weight).astype(BF)
        dq, dk, dv, gq, gk = attention_back(
            qkv, qr, kr, vb, do, nq, nk, qg, kg, cos2, sin2, trow, tcol
        )
        dqkv = jnp.concatenate([dq, dk, dv], 1)
        dnormed = scatter_sum(restore(times_back(dqkv, w_qkv)).reshape(n, rows, width))
        r1_own = lax.rsqrt(jnp.mean(inputs * inputs, -1, keepdims=True) + EPSILON)
        xh = inputs * r1_own
        grad_attn_gain = jnp.sum(dnormed * xh, 0)
        weighted = dnormed * attn_gain
        grad_input = (
            grad_hidden + r1_own * (weighted - xh * jnp.mean(weighted * xh, -1, keepdims=True))
        )[None]
        gains = jnp.concatenate(
            [grad_attn_gain, grad_mlp_gain, jnp.sum(gq[:, 0], 0), jnp.sum(gk[:, 0], 0)]
        )
        gains = jnp.pad(gains, (0, -gains.size % (8 * HD))).reshape(-1, HD)

        segments_of = [
            down_pair,
            mlp_pair,
            rows_parts(halves(attn_out), grad_branch),
            pair_parts(normed, dqkv, n, half // m),
        ]
        places = [v[0].shape[0] for v in segments_of]
        parts = [(0, a, 0) for a in range(places[0])] + [(1, k, k) for k in range(n)]
        parts += [(2, a, 0) for a in range(places[2])] + [(3, k, k) for k in range(n)]
        gains, *summed = reduce_gradients(
            n, m, gains, [v[0] for v in segments_of], [v[1] for v in segments_of], parts
        )
        mines, others = summed[:4], summed[4:]

        pick = lambda seg, at=None, width=None: (
            (mines[seg], others[seg]) if at is None else (mines[seg], others[seg], at, width)
        )
        (
            grad_down, grad_out_weight, grad_gate_weight, grad_up_weight,
            grad_query_weight, grad_key_weight, grad_value_weight,
        ) = assemble(
            [pick(0), pick(2)],
            [
                pick(1, 0, ffl), pick(1, 1, ffl), pick(3, 0, nq * HD),
                pick(3, nq // nk, nk * HD), pick(3, nq // nk + 1, nk * HD),
            ],
            core,
            owner,
        )
        gains = gains.reshape(-1)
        grad_attn_gain, grad_mlp_gain = gains[:width], gains[width : 2 * width]
        grad_query_gain = gains[2 * width : 2 * width + HD]
        grad_key_gain = gains[2 * width + HD : 2 * width + 2 * HD]
        return (
            output,
            grad_input,
            grad_attn_gain,
            grad_query_weight,
            grad_key_weight,
            grad_value_weight,
            grad_query_gain,
            grad_key_gain,
            grad_out_weight,
            grad_mlp_gain,
            grad_gate_weight,
            grad_up_weight,
            grad_down,
        )

    return per_device


def solution(mesh):
    tok = P("rep", "shard", None)
    row = P("shard", None)
    return jax.shard_map(
        build(mesh.shape["shard"], mesh.shape["rep"]),
        mesh=mesh,
        in_specs=(
            tok, P("rep", None), P(), row, row, row, P(), P(), row, P(), row, row, row, tok,
        ),
        out_specs=(tok, tok, P(), row, row, row, P(), P(), row, P(), row, row, row),
        check_vma=False,
    )
```

```python
from functools import partial
import math

import jax
import jax.numpy as jnp
from jax import lax
from jax.experimental import pallas as pl
from jax.experimental.pallas import tpu as pltpu
from jax.sharding import PartitionSpec as P

HQ = 16
HK = 8
HD = 128
FF = 6144
GROUPS = HQ // HK

EPSILON = 1e-06
ROPE_BASE = 1000000.0
MASKED = -1e30
BF = jnp.bfloat16
F32 = jnp.float32
AXES = ("shard", "rep")

HOOK_TICKS = (1, 3, 3, 3, 4, 5, 5, 5, 6, 8, 9, 10, 11, 12)


def dot(a, b):
    return jnp.dot(a, b, preferred_element_type=F32)


def dot_last(a, b):
    return lax.dot_general(a, b, (((1,), (1,)), ((), ())), preferred_element_type=F32)


def dot_first(a, b):
    return lax.dot_general(a, b, (((0,), (0,)), ((), ())), preferred_element_type=F32)


def positions(seg_ids):
    token_index = jnp.arange(seg_ids.shape[0], dtype=jnp.int32)
    before = jnp.concatenate([jnp.full((1,), -1, jnp.int32), seg_ids[:-1]])
    starts = lax.cummax(
        jnp.where(seg_ids != before, token_index, jnp.zeros_like(token_index)), axis=0
    )
    return (token_index - starts).astype(F32)


def head_rope(raw, gain, cos2, sin2):
    rstat = lax.rsqrt(jnp.mean(raw * raw, -1, keepdims=True) + EPSILON)
    scaled = raw * rstat * gain
    return scaled * cos2 + pltpu.roll(scaled, HD // 2, 1) * sin2


def attend_pair(qkv, j, nq, nk, qg, kg, cos2, sin2, trow, tcol, o_ref, qr_ref, kr_ref, vb_ref, scale):
    length = qkv.shape[0]
    block = min(length, 512)
    own = slice(j * HD, (j + 1) * HD)
    at = (nq + j) * HD
    kr = head_rope(qkv[:, at : at + HD], kg[...], cos2[...], sin2[...]).astype(BF)
    at = (nq + nk + j) * HD
    vb = qkv[:, at : at + HD].astype(BF)
    kr_ref[:, own] = kr
    vb_ref[:, own] = vb
    for g in range(GROUPS):
        cols = slice((j * GROUPS + g) * HD, (j * GROUPS + g + 1) * HD)
        qr_ref[:, cols] = head_rope(qkv[:, cols], qg[...], cos2[...], sin2[...]).astype(BF)
        for b in range(length // block):
            rows = slice(b * block, (b + 1) * block)
            s = dot_last(qr_ref[rows, cols], kr) * scale
            seen = (tcol[0:1, :] <= trow[rows, 0:1]) & (tcol[1:2, :] == trow[rows, 1:2])
            s = jnp.where(seen, s, MASKED)
            e = jnp.exp(s - jnp.max(s, -1, keepdims=True))
            p = (e / jnp.sum(e, -1, keepdims=True)).astype(BF)
            o_ref[rows, cols] = dot(p, vb).astype(BF)


def head_back(grad_rot, raw, gain, cos2, sin2):
    back = grad_rot * cos2 - pltpu.roll(grad_rot, HD // 2, 1) * sin2
    rstat = lax.rsqrt(jnp.mean(raw * raw, -1, keepdims=True) + EPSILON)
    scaled = raw * rstat
    gain_part = jnp.sum(back * scaled, 0, keepdims=True)
    b = back * gain
    return rstat * (b - scaled * jnp.mean(b * scaled, -1, keepdims=True)), gain_part


def attend_back_pair(
    j, nq, nk, qkv, qr_ref, kr_ref, vb_ref, do_ref, dqkv, qg, kg, cos_ref, sin_ref, trow, tcol, scale
):
    cos2, sin2 = cos_ref[...], sin_ref[...]
    own = slice(j * HD, (j + 1) * HD)
    length = qkv.shape[0]
    block = min(length, 256)
    kr, vb = kr_ref[:, own], vb_ref[:, own]
    dkr = jnp.zeros((length, HD), F32)
    dv = jnp.zeros((length, HD), F32)
    gq = jnp.zeros((1, HD), F32)
    for g in range(GROUPS):
        cols = slice((j * GROUPS + g) * HD, (j * GROUPS + g + 1) * HD)
        dqr = []
        for b in range(length // block):
            rows = slice(b * block, (b + 1) * block)
            qr, do = qr_ref[rows, cols], do_ref[rows, cols]
            s = dot_last(qr, kr) * scale
            seen = (tcol[0:1, :] <= trow[rows, 0:1]) & (tcol[1:2, :] == trow[rows, 1:2])
            s = jnp.where(seen, s, MASKED)
            e = jnp.exp(s - jnp.max(s, -1, keepdims=True))
            p = e / jnp.sum(e, -1, keepdims=True)
            dp = dot_last(do, vb)
            ds = (p * (dp - jnp.sum(p * dp, -1, keepdims=True))).astype(BF)
            dqr.append(dot(ds, kr) * scale)
            dkr += dot_first(ds, qr)
            dv += dot_first(p.astype(BF), do)
        dqr = dqr[0] if len(dqr) == 1 else jnp.concatenate(dqr, 0)
        dq, part = head_back(dqr, qkv[:, cols], qg[...], cos2, sin2)
        dqkv[:, cols] = dq.astype(BF)
        gq += part
    at = (nq + j) * HD
    dk, gk = head_back(dkr * scale, qkv[:, at : at + HD], kg[...], cos2, sin2)
    dqkv[:, at : at + HD] = dk.astype(BF)
    at = (nq + nk + j) * HD
    dqkv[:, at : at + HD] = dv.astype(BF)
    return gq, gk


def assemble_kernel(counts, order_ref, *refs):
    n_rows, n_cols = counts
    total = n_rows + n_cols
    mine, other, outs = refs[:total], refs[total : 2 * total], refs[2 * total :]

    def fill(sources):
        for src, out in zip(sources, outs):
            m, places, q, width = src.shape
            for a in range(places):
                out[a * m * q : (a + 1) * m * q, :] = (
                    src[:, a].reshape(m * q, width).astype(F32)
                )

    pl.when(pl.program_id(0) == 0)(lambda: fill(mine))
    pl.when(pl.program_id(0) == 1)(lambda: fill(other))


def assemble(rows, cols, core, owner):
    n = len(owner)
    order = jnp.stack(list(owner) + [core]).astype(jnp.int32)
    in_specs, out_specs, shapes, operands = [[], []], [], [], [[], []]
    size = 0
    for mine, other in rows:
        m, places, q, width = mine.shape
        block = (m, places, q, width // n)
        in_specs[0].append(
            pl.BlockSpec(block, lambda g, b, o: (0, 0, 0, jnp.where(g == 0, b, n - 1)))
        )
        in_specs[1].append(
            pl.BlockSpec(block, lambda g, b, o: (0, 0, 0, jnp.where(g == 0, 0, b)))
        )
        out_specs.append(
            pl.BlockSpec((places * m * q, width // n), lambda g, b, o: (g ^ o[n], b))
        )
        shapes.append(jax.ShapeDtypeStruct((2 * places * m * q, width), F32))
        operands[0].append(mine)
        operands[1].append(other)
        size += mine.size
    for mine, other, at, width in cols:
        m, _, q, _ = mine.shape
        block = (m, 1, q, width)
        in_specs[0].append(
            pl.BlockSpec(block, lambda g, b, o, at=at: (0, o[jnp.where(g == 0, b, n - 1)], 0, at))
        )
        in_specs[1].append(
            pl.BlockSpec(block, lambda g, b, o, at=at: (0, o[jnp.where(g == 0, 0, b)], 0, at))
        )
        out_specs.append(pl.BlockSpec((m * q, width), lambda g, b, o: (g ^ o[n], b)))
        shapes.append(jax.ShapeDtypeStruct((2 * m * q, n * width), F32))
        operands[0].append(mine)
        operands[1].append(other)
        size += m * n * q * width
    return pl.pallas_call(
        partial(assemble_kernel, (len(rows), len(cols))),
        out_shape=tuple(shapes),
        grid_spec=pltpu.PrefetchScalarGridSpec(
            num_scalar_prefetch=1,
            grid=(2, n),
            in_specs=in_specs[0] + in_specs[1],
            out_specs=tuple(out_specs),
        ),
        compiler_params=pltpu.CompilerParams(vmem_limit_bytes=56 << 20),
        cost_estimate=pl.CostEstimate(flops=0, bytes_accessed=12 * size, transcendentals=0),
        name="assemble",
    )(order, *operands[0], *operands[1])


MESH_ID = pl.DeviceIdType.MESH


def back_kernel(n, m, nq, nk, scale, parts, *refs):
    (dhn_hbm, x_hbm, dy_hbm, hidden_hbm, wo_hbm, wm_hbm, wx_hbm, qkv_hbm, qr_hbm, kr_hbm, vb_hbm,
     o_hbm, normed_hbm, ag, mg, qg, kg, cos2, sin2, trow, tcol,
     send_down, send_mlp, keep_down, keep_mlp, grad_in, gain_out) = refs[:27]
    mines, others, refs = refs[27:31], refs[31:35], refs[35:]
    away_v, refs = refs[:4], refs[4:]
    (ups, downs, fins, stage, send_out, send_qkv,
     x_v, dy_v, hidden, wo, qkv, qr, kr, vb, o, normed, part_own, part_r, part_s, dz_all, do, dqkv,
     wtile, gain_ref,
     load_sem, pair_s, pair_r, up_s, up_r, down_s, down_r,
     peer_s, peer_r, gup_s, gup_r, gdown_s, gdown_r, sib_s, sib_r, own_sem, gain_pair, gain_group,
     gain_line, gain_s, gain_r, in_sem, wt_sem, dhn_s, dhn_r, dz_s, dz_r, dn_s, dn_r) = refs
    sends = (send_down, send_mlp, send_out, send_qkv)
    keeps = (keep_down, keep_mlp)
    rows, width = x_v.shape
    own = width // n
    half = own // 2
    shard, rep = lax.axis_index("shard"), lax.axis_index("rep")
    i = rep // 2
    core = lax.rem(rep, 2)
    sibling = {"rep": 2 * i + 1 - core}
    above, below = {"rep": rep + 2}, {"rep": rep - 2}
    peers = [None] + [{"shard": shard ^ k} for k in range(1, n)]
    has_up, has_down = i < m - 1, i > 0

    barrier = pltpu.get_barrier_semaphore()

    def greet(dev):
        pl.semaphore_signal(barrier, inc=1, device_id=dev, device_id_type=MESH_ID)

    greet(sibling)
    for k in range(1, n):
        greet(peers[k])
    line = [None] + [{"rep": 2 * lax.rem(i + d, m) + core} for d in range(1, m)]
    for d in range(1, m):
        greet(line[d])
    pl.semaphore_wait(barrier, n + m - 1)

    def remote(src, dst, ssem, rsem, dev):
        return pltpu.make_async_remote_copy(
            src_ref=src, dst_ref=dst, send_sem=ssem, recv_sem=rsem,
            device_id=dev, device_id_type=MESH_ID,
        )

    def chunk(ref, part, j):
        seg, at, _ = part
        return ref[seg].at[at, j]

    def out(ref, part, j):
        seg, at, _ = part
        return ref[seg].at[j, at]

    def pair_copy(p):
        seg, at, _ = parts[p]
        return remote(sends[seg].at[at], away_v[seg].at[at], pair_s.at[p], pair_r.at[p], sibling)

    def load_copy(p):
        seg, at, _ = parts[p]
        cols = keeps[seg].shape[3]
        return pltpu.make_async_copy(
            keeps[seg].at[at], stage.at[p % 2, :, :, pl.ds(0, cols)], load_sem.at[p]
        )

    def slot(ref, p, t):
        return ref[parts[p][0]].at[parts[p][1], t]

    def up_copy(p, t, src):
        return remote(src, slot(ups, p, t), up_s.at[p, t], up_r.at[p, t], above)

    def down_copy(p, t, src):
        return remote(src, slot(downs, p, t), down_s.at[p, t], down_r.at[p, t], below)

    def add_into(ref, other):
        ref[...] = (ref[...].astype(F32) + other[...].astype(F32)).astype(BF)

    def scatter_step(p, t):
        part = parts[p]
        if t > 0:

            @pl.when((i > 0) & (i <= t) & has_up)
            def _():
                up_copy(p, t - 1, slot(ups, p, t - 1)).wait_recv()
                add_into(slot(ups, p, t - 1), chunk(away_v, part, m - 1 - t + i))

            @pl.when((i < m - 1) & (i >= m - 1 - t) & has_down)
            def _():
                down_copy(p, t - 1, slot(downs, p, t - 1)).wait_recv()
                add_into(slot(downs, p, t - 1), chunk(away_v, part, i - (m - 1 - t)))

            pl.when((i > 0) & (i <= t) & has_up)(
                lambda: up_copy(p, t, slot(ups, p, t - 1)).start()
            )
            pl.when((i < m - 1) & (i >= m - 1 - t) & has_down)(
                lambda: down_copy(p, t, slot(downs, p, t - 1)).start()
            )
        pl.when(i == 0)(lambda: up_copy(p, t, chunk(away_v, part, m - 1 - t)).start())
        pl.when(i == m - 1)(lambda: down_copy(p, t, chunk(away_v, part, t)).start())

    def peer_copy(p):
        seg, at, k = parts[p]
        return remote(away_v[seg].at[at, i], fins[seg].at[at], peer_s.at[p], peer_r.at[p], peers[k])

    def total(p):
        seg, at, k = parts[p]
        part = parts[p]
        pl.when(has_down)(lambda: up_copy(p, m - 2, slot(ups, p, m - 2)).wait_recv())
        pl.when(has_up)(lambda: down_copy(p, m - 2, slot(downs, p, m - 2)).wait_recv())
        where = fins[seg].at[at] if k == 0 else away_v[seg].at[at, i]

        def put(*extra):
            value = chunk(away_v, part, i)[...].astype(F32)
            for e in extra:
                value = value + e[...].astype(F32)
            where[...] = value.astype(BF)

        u, d = slot(ups, p, m - 2), slot(downs, p, m - 2)
        pl.when(has_up & has_down)(lambda: put(u, d))
        pl.when(has_up & (i == 0))(lambda: put(d))
        pl.when(has_down & (i == m - 1))(lambda: put(u))
        if k != 0:
            peer_copy(p).start()

    def gup_copy(p, t, j, src):
        return remote(src, out(mines, parts[p], j), gup_s.at[p, t], gup_r.at[p, t], above)

    def gdown_copy(p, t, j, src):
        return remote(src, out(mines, parts[p], j), gdown_s.at[p, t], gdown_r.at[p, t], below)

    def sib_copy(p, j, src):
        return remote(src, out(others, parts[p], j), sib_s.at[p, j], sib_r.at[p, j], sibling)

    def gather_step(p, t):
        part = parts[p]
        if t == 0:
            seg, at, k = part
            if k != 0:
                peer_copy(p).wait_recv()
            fin = fins[seg].at[at]
            pl.when(has_up)(lambda: gup_copy(p, 0, i, fin).start())
            pl.when(has_down)(lambda: gdown_copy(p, 0, i, fin).start())
            sib_copy(p, i, fin).start()
            pltpu.make_async_copy(fin, out(mines, part, i), own_sem.at[p]).start()
            return

        @pl.when(i - t >= 0)
        def _():
            here = out(mines, part, i - t)
            gup_copy(p, t - 1, i - t, here).wait_recv()
            if t < m - 1:
                pl.when(has_up)(lambda: gup_copy(p, t, i - t, here).start())
            sib_copy(p, i - t, here).start()

        @pl.when(i + t < m)
        def _():
            here = out(mines, part, i + t)
            gdown_copy(p, t - 1, i + t, here).wait_recv()
            if t < m - 1:
                pl.when(has_down)(lambda: gdown_copy(p, t, i + t, here).start())
            sib_copy(p, i + t, here).start()

    def gain_copies(level):
        if level == 0:
            return [remote(gain_ref, gain_pair, gain_s.at[0], gain_r.at[0], sibling)]
        if level == 1:
            return [
                remote(
                    gain_group.at[shard], gain_group.at[shard], gain_s.at[k], gain_r.at[k], peers[k]
                )
                for k in range(1, n)
            ]
        return [
            remote(
                gain_line.at[i], gain_line.at[i], gain_s.at[n - 1 + d], gain_r.at[n - 1 + d], line[d]
            )
            for d in range(1, m)
        ]

    def gains(level):
        if level > 0:
            for copy in gain_copies(level - 1):
                copy.wait_recv()
        if level == 1:
            gain_group[shard] = gain_ref[...] + gain_pair[...]
        elif level == 2:
            value = gain_group[0]
            for k in range(1, n):
                value = value + gain_group[k]
            gain_line[i] = value
        elif level == 3:
            value = gain_line[0]
            for k in range(1, m):
                value = value + gain_line[k]
            gain_out[...] = value
        if level < 3:
            for copy in gain_copies(level):
                copy.start()

    def tiles(cols):
        step = min(cols, 512)
        return [slice(c, c + step) for c in range(0, cols, step)]

    def first(p):
        seg, at, k = parts[p]
        away = away_v[seg]
        pair_copy(p).wait_recv()
        if seg < 2:
            load_copy(p).wait()
            for j in range(m):
                for c in tiles(away.shape[3]):
                    away[at, j, :, c] = (
                        stage[p % 2, j, :, c].astype(F32) + away[at, j, :, c].astype(F32)
                    ).astype(BF)
            if p + 2 < len(parts) and parts[p + 2][0] < 2:
                load_copy(p + 2).start()
        else:
            shape = away.shape[1:3]
            for c in tiles(away.shape[3]):
                if seg == 2:
                    size = o.shape[1] // 2
                    left = o[:, pl.ds(pl.multiple_of(core * size, size), size)]
                    right = dz_all[:, :, c].reshape(n * rows, -1)
                else:
                    left, right = normed[:, k * half : (k + 1) * half], dqkv[:, c]
                value = dot_first(left, right)
                away[at, :, :, c] = (
                    value.reshape(shape + value.shape[1:]) + away[at, :, :, c].astype(F32)
                ).astype(BF)
        scatter_step(p, 0)

    loads = [
        pltpu.make_async_copy(src, dst, in_sem.at[f])
        for f, (src, dst) in enumerate(
            [
                (dhn_hbm.at[0], part_own), (x_hbm, x_v), (dy_hbm, dy_v), (hidden_hbm, hidden),
                (wo_hbm, wo), (qkv_hbm, qkv), (qr_hbm, qr), (kr_hbm, kr), (vb_hbm, vb),
                (o_hbm, o), (normed_hbm, normed),
            ]
        )
    ]

    def dhn_copy(k):
        return remote(dhn_hbm.at[k], part_r.at[k - 1], dhn_s.at[k], dhn_r.at[k], peers[k])

    def dz_copy(k):
        return remote(dz_all.at[0], dz_all.at[k], dz_s.at[k], dz_r.at[k], peers[k])

    def dn_copy(k):
        return remote(part_s.at[k], part_r.at[k - 1], dn_s.at[k], dn_r.at[k], peers[k])

    strip = min(rows, 32)

    def strips(body):
        pl.loop(0, rows // strip)(
            lambda b: body(pl.ds(pl.multiple_of(b * strip, strip), strip))
        )

    def add_gain(at, value):
        for b in range(value.shape[1] // HD):
            gain_ref[at + b : at + b + 1, :] += value[:, b * HD : (b + 1) * HD]

    def norm_back(values, gain, at, own_part, result):
        def body(r):
            v = values[r, :].astype(F32)
            scaled = v * lax.rsqrt(jnp.mean(v * v, -1, keepdims=True) + EPSILON)
            rstat = lax.rsqrt(jnp.mean(v * v, -1, keepdims=True) + EPSILON)
            grad = own_part[r, :].astype(F32)
            for k in range(1, n):
                grad = grad + part_r[k - 1, r, :].astype(F32)
            add_gain(at, jnp.sum(grad * scaled, 0, keepdims=True))
            weighted = grad * gain[...]
            result(
                r, rstat * (weighted - scaled * jnp.mean(weighted * scaled, -1, keepdims=True))
            )

        strips(body)

    def hook_hidden():
        for copy in loads[:4]:
            copy.wait()
        for k in range(1, n):
            dhn_copy(k).wait_recv()
        gain_ref[...] = jnp.zeros_like(gain_ref)

        def result(r, value):
            value = dy_v[r, :].astype(F32) + value
            grad_in[r, :] = value
            dz_all[0, r, :] = value.astype(BF)

        norm_back(hidden, mg, width // HD, part_own, result)
        for k in range(1, n):
            dz_copy(k).start()

    def hook_do():
        for copy in loads[4:]:
            copy.wait()
        for k in range(n):
            if k > 0:
                dz_copy(k).wait_recv()
            do[k * rows : (k + 1) * rows, :] = dot_last(dz_all[k], wo[...]).astype(BF)

    def hook_send_out():
        size = o.shape[1] // 2
        left = pl.ds(pl.multiple_of((1 - core) * size, size), size)
        for c in tiles(width):
            value = dot_first(o[:, left], dz_all[:, :, c].reshape(n * rows, -1))
            for a in range(send_out.shape[0]):
                send_out[a, :, :, c] = value.astype(BF).reshape((m, -1) + value.shape[1:])

    def hook_head(j):
        gq, gk = attend_back_pair(
            j, nq, nk, qkv, qr, kr, vb, do, dqkv, qg, kg, cos2, sin2, trow, tcol, scale
        )
        add_gain(2 * width // HD, gq)
        add_gain(2 * width // HD + 1, gk)

    def tile_copy(b):
        src = (wm_hbm if b < n else wx_hbm).at[b % n]
        return pltpu.make_async_copy(src, wtile.at[b % 2], wt_sem.at[b % 2])

    def hook_normed():
        tile_copy(0).start()
        for b in range(2 * n):
            tile_copy(b).wait()
            if b + 1 < 2 * n:
                tile_copy(b + 1).start()
            h, kk = b // n, b % n
            at = pl.ds(
                pl.multiple_of((shard ^ kk) * own + (core if h == 0 else 1 - core) * half, half),
                half,
            )
            w = wtile[b % 2].reshape(half, dqkv.shape[1])
            for k in range(n):
                part_s[k, :, at] = dot_last(dqkv[k * rows : (k + 1) * rows, :], w).astype(BF)
        for k in range(1, n):
            dn_copy(k).start()

    def hook_send_qkv():
        for k in range(n):
            value = dot_first(normed[:, (n + k) * half : (n + k + 1) * half], dqkv[...])
            send_qkv[k] = value.astype(BF).reshape((m, -1) + value.shape[1:])

    def hook_pairs(seg):
        for p in range(len(parts)):
            if parts[p][0] == seg:
                pair_copy(p).start()

    def hook_input():
        for k in range(1, n):
            dn_copy(k).wait_recv()

        def result(r, value):
            grad_in[r, :] = grad_in[r, :] + value

        norm_back(x_v, ag, 0, part_s.at[0], result)

    hooks = [hook_hidden, hook_do, hook_send_out, lambda: hook_pairs(2)]
    hooks += [partial(hook_head, j) for j in range(nk)]
    hooks += [
        hook_send_qkv, lambda: hook_pairs(3), hook_normed, hook_input,
    ] + [partial(gains, level) for level in range(4)]
    at_tick = {}
    last_free = sum(1 for part in parts if part[0] < 2)
    schedule = HOOK_TICKS if nk == 2 else None
    for f, hook in enumerate(hooks):
        tick = schedule[f] if schedule else min(f, last_free - 1 if f < 2 + nk + 5 else f)
        at_tick.setdefault(tick, []).append(hook)

    for k in range(1, n):
        dhn_copy(k).start()

    stages = [first] + [lambda p, t=t: scatter_step(p, t) for t in range(1, m - 1)]
    stages += [total] + [lambda p, t=t: gather_step(p, t) for t in range(m)]

    load_copy(0).start()
    load_copy(1).start()
    hook_pairs(0)
    for copy in loads:
        copy.start()
    hook_pairs(1)
    ticks = len(parts) + len(stages) - 1
    for tick in range(max(ticks, max(at_tick) + 1)):
        for st in range(len(stages) - 1, -1, -1):
            p = tick - st
            if 0 <= p < len(parts):
                stages[st](p)
        for hook in at_tick.get(tick, []):
            hook()

    for k in range(1, n):
        dhn_copy(k).wait_send()
        dz_copy(k).wait_send()
        dn_copy(k).wait_send()
    for level in range(3):
        for copy in gain_copies(level):
            copy.wait_send()
    for p in range(len(parts)):
        part = parts[p]
        seg, at, k = part
        pair_copy(p).wait_send()
        if k != 0:
            peer_copy(p).wait_send()
        pltpu.make_async_copy(fins[seg].at[at], out(mines, part, i), own_sem.at[p]).wait()
        for t in range(m - 1):
            pl.when((i <= t) & has_up)(lambda: up_copy(p, t, slot(ups, p, t)).wait_send())
            pl.when((i >= m - 1 - t) & has_down)(
                lambda: down_copy(p, t, slot(downs, p, t)).wait_send()
            )
            pl.when((i - t >= 0) & has_up)(
                lambda: gup_copy(p, t, i, fins[seg].at[at]).wait_send()
            )
            pl.when((i + t < m) & has_down)(
                lambda: gdown_copy(p, t, i, fins[seg].at[at]).wait_send()
            )
        for j in range(m):
            copy = sib_copy(p, j, fins[seg].at[at])
            copy.wait_send()
            copy.wait_recv()


def back(n, m, nq, nk, parts, dhn, x, dy, hidden, wo, w_qkv, qkv, heads, o, normed, gains, tables,
         sends, keeps):
    total = len(parts)
    rows, width = x.shape
    length = n * rows
    q, cols = w_qkv[0].shape[2:]
    dma = pltpu.SemaphoreType.DMA
    sd = jax.ShapeDtypeStruct
    hbm, vmem = pl.BlockSpec(memory_space=pl.ANY), pl.BlockSpec(memory_space=pltpu.VMEM)
    places = nq * HD // 2 // (m * q)
    segments = [v.shape for v in keeps] + [(places, m, q, width), (n, m, q, cols)]
    count = 2 * width // HD + 2
    gain_shape = (count + -count % 8, HD)

    def slots(extra):
        return [pltpu.VMEM((v[0],) + extra + v[2:], BF) for v in segments]

    outs = [sd((m, v[0]) + v[2:], BF) for v in segments]
    like = lambda v: pltpu.VMEM(v.shape, v.dtype)
    operands = [dhn, x, dy, hidden, wo, *w_qkv, qkv, *heads, o, normed]
    return pl.pallas_call(
        partial(back_kernel, n, m, nq, nk, 1.0 / math.sqrt(HD), parts),
        out_shape=tuple([sd((rows, width), F32), sd(gain_shape, F32)] + outs + outs),
        in_specs=[hbm] * len(operands) + [vmem] * 8 + [hbm] * 4,
        out_specs=tuple([vmem, vmem] + [hbm] * 8),
        scratch_shapes=[pltpu.VMEM(v, BF) for v in segments]
        + [slots((m - 1,)), slots((m - 1,)), slots(())]
        + [pltpu.VMEM((2, m, max(v[2] for v in segments[:2]), max(v[3] for v in segments[:2])), BF)]
        + [pltpu.VMEM(v, BF) for v in segments[2:]]
        + [like(v) for v in (x, dy, hidden, wo, qkv, *heads, o, normed)]
        + [
            pltpu.VMEM((rows, width), BF), pltpu.VMEM((n - 1, rows, width), BF),
            pltpu.VMEM((n, rows, width), BF), pltpu.VMEM((n, rows, width), BF),
            pltpu.VMEM((length, nq * HD), BF), pltpu.VMEM((length, cols), BF),
            pltpu.VMEM((2, m, q, cols), BF), pltpu.VMEM(gain_shape, F32),
            dma((total,)), dma((total,)), dma((total,)),
            dma((total, m - 1)), dma((total, m - 1)), dma((total, m - 1)), dma((total, m - 1)),
            dma((total,)), dma((total,)),
            dma((total, m - 1)), dma((total, m - 1)), dma((total, m - 1)), dma((total, m - 1)),
            dma((total, m)), dma((total, m)), dma((total,)),
            pltpu.VMEM(gain_shape, F32), pltpu.VMEM((n,) + gain_shape, F32),
            pltpu.VMEM((m,) + gain_shape, F32), dma((n + m,)), dma((n + m,)),
            dma((11,)), dma((2,)), dma((n,)), dma((n,)), dma((n,)), dma((n,)), dma((n,)), dma((n,)),
        ],
        compiler_params=pltpu.CompilerParams(
            collective_id=3, has_side_effects=True, vmem_limit_bytes=67043328
        ),
        name="back",
    )(*operands, *gains, *tables, *sends, *keeps)


def front_kernel(
    n, m, nq, nk, scale,
    x_hbm, dy_hbm, wq, wk, wv, wg, wu, wo_hbm,
    ag, qg, kg, mg, cos2, sin2, trow, tcol,
    normed, qkv, qr, kr, vb, o, hidden, hn, qkv_mine, qkv_other, mlp_mine, mlp_other, dy_all,
    x_all, wo, bounce, dy_v, hn_all, part_own, part_s, part_r,
    x_ss, x_rs, w_ss, w_rs, up_ss, up_rs, down_ss, down_rs, sib_ss, sib_rs,
    own_sem, back_sem, load_sem, part_ss, part_rs, hn_ss, hn_rs, dy_ss, dy_rs
):
    shard, rep = lax.axis_index("shard"), lax.axis_index("rep")
    i = rep // 2
    core = lax.rem(rep, 2)
    sibling = {"rep": 2 * i + 1 - core}
    above, below = {"rep": rep + 2}, {"rep": rep - 2}
    peers = [None] + [{"shard": shard ^ k} for k in range(1, n)]
    has_up, has_down = i < m - 1, i > 0
    rows, width = x_all.shape[1], x_all.shape[2]
    own = width // n
    half = own // 2

    barrier = pltpu.get_barrier_semaphore()

    def greet(dev):
        pl.semaphore_signal(barrier, inc=1, device_id=dev, device_id_type=MESH_ID)

    greet(sibling)
    for k in range(1, n):
        greet(peers[k])
    for d in range(1, m):
        greet({"rep": 2 * lax.rem(i + d, m) + core})
    pl.semaphore_wait(barrier, n + m - 1)

    def remote(src, dst, ssem, rsem, dev):
        return pltpu.make_async_remote_copy(
            src_ref=src, dst_ref=dst, send_sem=ssem, recv_sem=rsem,
            device_id=dev, device_id_type=MESH_ID,
        )

    groups = [
        ([wq, wk, wv], qkv_mine, qkv_other),
        ([wg, wu], mlp_mine, mlp_other),
    ]

    def fields(weights):
        at = 0
        for w in weights:
            size = w.shape[3] // n
            yield w, at, size
            at += size

    def cols_of(k, size):
        return pl.ds(pl.multiple_of((shard ^ k) * size, size), size)

    def piece_copies(g, k):
        weights, mine, _ = groups[g]
        return [
            remote(
                w.at[core, i, :, cols_of(k, size)],
                mine.at[k, i, :, pl.ds(at, size)],
                w_ss.at[g, k, f], w_rs.at[g, k, f], peers[k],
            )
            for f, (w, at, size) in enumerate(fields(weights))
        ]

    def own_copies(g):
        weights, mine, other = groups[g]
        out = []
        for h, dst in enumerate((mine, other)):
            for f, (w, at, size) in enumerate(fields(weights)):
                to = dst.at[0, :, :, pl.ds(at, size)] if g == 0 else bounce.at[h, :, :, pl.ds(at, size)]
                src = w.at[core if h == 0 else 1 - core, :, :, cols_of(0, size)]
                out.append(pltpu.make_async_copy(src, to, own_sem.at[g, h, f]))
        return out

    def back_copies():
        return [
            pltpu.make_async_copy(bounce.at[h], dst.at[0], back_sem.at[h])
            for h, dst in enumerate((mlp_mine, mlp_other))
        ]

    def region(ref, j):
        return ref.at[pl.ds(1, n - 1), j]

    def up_copy(g, t, j):
        r = region(groups[g][1], j)
        return remote(r, r, up_ss.at[g, t], up_rs.at[g, t], above)

    def down_copy(g, t, j):
        r = region(groups[g][1], j)
        return remote(r, r, down_ss.at[g, t], down_rs.at[g, t], below)

    def sib_copy(g, j):
        _, mine, other = groups[g]
        return remote(region(mine, j), region(other, j), sib_ss.at[g, j], sib_rs.at[g, j], sibling)

    def gather_weights(g, t):
        if t == 0:
            for k in range(1, n):
                for copy in piece_copies(g, k):
                    copy.wait_recv()
            pl.when(has_up)(lambda: up_copy(g, 0, i).start())
            pl.when(has_down)(lambda: down_copy(g, 0, i).start())
            sib_copy(g, i).start()
            return

        @pl.when(i - t >= 0)
        def _():
            up_copy(g, t - 1, i - t).wait_recv()
            if t < m - 1:
                pl.when(has_up)(lambda: up_copy(g, t, i - t).start())
            sib_copy(g, i - t).start()

        @pl.when(i + t < m)
        def _():
            down_copy(g, t - 1, i + t).wait_recv()
            if t < m - 1:
                pl.when(has_down)(lambda: down_copy(g, t, i + t).start())
            sib_copy(g, i + t).start()

    def x_copy(k):
        return remote(x_hbm, x_all.at[k], x_ss.at[k], x_rs.at[k], peers[k])

    def dy_copy(k):
        return remote(dy_hbm, dy_all.at[k], dy_ss.at[k], dy_rs.at[k], peers[k])

    def hn_copy(k):
        return remote(hn_all.at[0], hn_all.at[k], hn_ss.at[k], hn_rs.at[k], peers[k])

    def part_copy(k):
        return remote(part_s.at[k], part_r.at[k], part_ss.at[k], part_rs.at[k], peers[k])

    load_x = pltpu.make_async_copy(x_hbm, x_all.at[0], load_sem.at[0])
    load_wo = pltpu.make_async_copy(wo_hbm, wo, load_sem.at[1])
    load_dy = pltpu.make_async_copy(dy_hbm, dy_v, load_sem.at[2])
    keep_dy = pltpu.make_async_copy(dy_v, dy_all.at[0], load_sem.at[3])

    load_x.start()
    for k in range(1, n):
        for copy in piece_copies(0, k):
            copy.start()
    for k in range(1, n):
        x_copy(k).start()
    for copy in own_copies(0):
        copy.start()
    for k in range(1, n):
        for copy in piece_copies(1, k):
            copy.start()
    for copy in own_copies(1):
        copy.start()
    load_wo.start()
    load_dy.start()

    def place(k, h, kk):
        return pl.ds(
            pl.multiple_of((shard ^ kk) * own + (core if h == 0 else 1 - core) * half, half), half
        )

    gather_weights(0, 0)
    for k in range(n):
        if k == 0:
            load_x.wait()
        else:
            x_copy(k).wait_recv()
        v = x_all[k].astype(F32)
        r = lax.rsqrt(jnp.mean(v * v, -1, keepdims=True) + EPSILON)
        for h in range(2):
            for kk in range(n):
                at = place(k, h, kk)
                normed[k * rows : (k + 1) * rows, (h * n + kk) * half : (h * n + kk + 1) * half] = (
                    x_all[k, :, at].astype(F32) * r * ag[:, at]
                ).astype(BF)
    for t in range(1, m - 1):
        gather_weights(0, t)
    gather_weights(1, 0)
    gather_weights(0, m - 1)
    for copy in own_copies(0):
        copy.wait()
    for j in range(m):
        sib_copy(0, j).wait_recv()

    cols = qkv.shape[1]
    step = min(cols, 256)

    @pl.loop(0, cols // step)
    def _(b):
        at = pl.ds(pl.multiple_of(b * step, step), step)
        both = n * half
        qkv[:, at] = dot(
            normed[:, :both], qkv_mine[:, :, :, at].reshape(both, step)
        ) + dot(normed[:, both:], qkv_other[:, :, :, at].reshape(both, step))

    hop = 1
    for copy in own_copies(1):
        copy.wait()
    for copy in back_copies():
        copy.start()
    load_dy.wait()
    keep_dy.start()
    for j in range(nk):
        attend_pair(qkv, j, nq, nk, qg, kg, cos2, sin2, trow, tcol, o, qr, kr, vb, scale)
        if j == 0 and hop < m - 1:
            gather_weights(1, hop)
            hop += 1

    load_wo.wait()
    step = min(width, 512)

    @pl.loop(0, width // step)
    def _(b):
        at = pl.ds(pl.multiple_of(b * step, step), step)
        for k in range(n):
            value = dot(o[k * rows : (k + 1) * rows, :], wo[:, at])
            if k == 0:
                part_own[:, at] = value
            else:
                part_s[k, :, at] = value.astype(BF)

    for k in range(1, n):
        part_copy(k).start()
    if hop < m - 1:
        gather_weights(1, hop)
        hop += 1
    total = x_all[0].astype(F32) + part_own[...]
    for k in range(1, n):
        part_copy(k).wait_recv()
        total = total + part_r[k].astype(F32)
    hidden[...] = total
    r = lax.rsqrt(jnp.mean(total * total, -1, keepdims=True) + EPSILON)
    hn_all[0] = (total * r * mg[...]).astype(BF)
    for k in range(1, n):
        hn_copy(k).start()
    for k in range(1, n):
        dy_copy(k).start()
    while hop < m - 1:
        gather_weights(1, hop)
        hop += 1
    for k in range(n):
        if k > 0:
            hn_copy(k).wait_recv()
        for h in range(2):
            for kk in range(n):
                hn[k * rows : (k + 1) * rows, (h * n + kk) * half : (h * n + kk + 1) * half] = (
                    hn_all[k, :, place(k, h, kk)]
                )
    gather_weights(1, m - 1)

    for copy in back_copies():
        copy.wait()
    keep_dy.wait()
    for k in range(1, n):
        for g in range(2):
            for copy in piece_copies(g, k):
                copy.wait_send()
        x_copy(k).wait_send()
        part_copy(k).wait_send()
        hn_copy(k).wait_send()
        dy_copy(k).wait_send()
        dy_copy(k).wait_recv()
    for g in range(2):
        for j in range(m):
            sib_copy(g, j).wait_send()
            if g == 1:
                sib_copy(g, j).wait_recv()
        for t in range(m - 1):
            pl.when((i - t >= 0) & has_up)(lambda: up_copy(g, t, i).wait_send())
            pl.when((i + t < m) & has_down)(lambda: down_copy(g, t, i).wait_send())


def front(n, m, nq, nk, x, dy, weights, wo, gains, tables):
    rows, width = x.shape
    length = n * rows
    q = weights[0].shape[2]
    cols = [sum(w.shape[3] // n for w in ws) for ws in (weights[:3], weights[3:])]
    vmem, hbm = pl.BlockSpec(memory_space=pltpu.VMEM), pl.BlockSpec(memory_space=pl.ANY)
    dma = pltpu.SemaphoreType.DMA
    sd = jax.ShapeDtypeStruct
    outs = [
        (sd((length, width), BF), vmem),
        (sd((length, cols[0]), F32), vmem),
        (sd((length, nq * HD), BF), vmem),
        (sd((length, nk * HD), BF), vmem),
        (sd((length, nk * HD), BF), vmem),
        (sd((length, nq * HD), BF), vmem),
        (sd((rows, width), F32), vmem),
        (sd((length, width), BF), vmem),
        (sd((n, m, q, cols[0]), BF), vmem),
        (sd((n, m, q, cols[0]), BF), vmem),
        (sd((n, m, q, cols[1]), BF), hbm),
        (sd((n, m, q, cols[1]), BF), hbm),
        (sd((n, rows, width), BF), hbm),
    ]
    return pl.pallas_call(
        partial(front_kernel, n, m, nq, nk, 1.0 / math.sqrt(HD)),
        out_shape=tuple(v[0] for v in outs),
        in_specs=[hbm] * 8 + [vmem] * 8,
        out_specs=tuple(v[1] for v in outs),
        scratch_shapes=[
            pltpu.VMEM((n, rows, width), BF),
            pltpu.VMEM(wo.shape, BF),
            pltpu.VMEM((2, m, q, cols[1]), BF),
            pltpu.VMEM((rows, width), BF),
            pltpu.VMEM((n, rows, width), BF),
            pltpu.VMEM((rows, width), F32),
            pltpu.VMEM((n, rows, width), BF),
            pltpu.VMEM((n, rows, width), BF),
            dma((n,)), dma((n,)),
            dma((2, n, 3)), dma((2, n, 3)),
            dma((2, m)), dma((2, m)), dma((2, m)), dma((2, m)), dma((2, m)), dma((2, m)),
            dma((2, 2, 3)), dma((2,)), dma((4,)),
            dma((n,)), dma((n,)), dma((n,)), dma((n,)), dma((n,)), dma((n,)),
        ],
        compiler_params=pltpu.CompilerParams(
            collective_id=1, has_side_effects=True, vmem_limit_bytes=60 << 20
        ),
        name="front",
    )(x, dy, *weights, wo, *gains, *tables)


def build(n, reps):
    m = reps // 2

    def pairs(move):
        out = []
        for s in range(n):
            for r in range(reps):
                to = move(s, r)
                if to is not None:
                    out.append((s * reps + r, to[0] * reps + to[1]))
        return out

    peer_pairs = [pairs(lambda s, r, k=k: (s ^ k, r)) for k in range(n)]

    def to_peer(v, k):
        return lax.ppermute(v, AXES, peer_pairs[k])

    def gather(v):
        return jnp.concatenate([v] + [to_peer(v, k) for k in range(1, n)], 0)

    def scatter_sum(v):
        total = v[0].astype(F32)
        for k in range(1, n):
            total = total + to_peer(v[k].astype(BF), k).astype(F32)
        return total

    def per_device(
        activations, segments, attn_gain, query_weight, key_weight, value_weight,
        query_gain, key_gain, out_weight, mlp_gain, gate_weight, up_weight, down_weight,
        cotangent,
    ):
        rows, width = activations.shape[1], activations.shape[2]
        length = segments.shape[1]
        shard = lax.axis_index("shard")
        core = lax.axis_index("rep") % 2
        own = width // n
        half = own // 2
        nq, nk = HQ // n, HK // n
        ffl = FF // n
        owner = [shard ^ k for k in range(n)]

        def cut(v, start, size, axis):
            return lax.dynamic_slice_in_dim(v, start, size, axis)

        def reorder(v):
            return jnp.concatenate(
                [
                    cut(v, owner[k] * own + (core ^ h) * half, half, 1)
                    for h in range(2)
                    for k in range(n)
                ],
                1,
            )

        def restore(v):
            return jnp.concatenate(
                [
                    cut(v, ((core ^ h) * n + owner[b]) * half, half, 1)
                    for b in range(n)
                    for h in range(2)
                ],
                1,
            )

        def times(v, w):
            both = v.shape[1] // 2
            return dot(v[:, :both], w[0]) + dot(v[:, both:], w[1])

        def times_back(v, w):
            return jnp.concatenate(
                [dot_last(v, w[0]).astype(BF), dot_last(v, w[1]).astype(BF)], 1
            )

        def pair_parts(left, right, places, q):
            both = left.shape[1] // 2
            return [
                dot_first(v, right).astype(BF).reshape(places, m, q, right.shape[1])
                for v in (left[:, both:], left[:, :both])
            ]

        def rows_parts(left, right):
            q = half // m
            both = left.shape[1] // 2
            out = []
            for h in (1, 0):
                v = left[:, h * both : (h + 1) * both]
                g = dot_first(v, right).astype(BF)
                out.append(g.reshape(both // (m * q), m, q, right.shape[1]))
            return out

        def halves(v):
            both = v.shape[1] // 2
            return jnp.concatenate(
                [cut(v, core * both, both, 1), cut(v, (1 - core) * both, both, 1)], 1
            )

        seg_ids = segments[0]
        pos = positions(seg_ids)
        tokens = jnp.arange(length, dtype=jnp.int32)
        shuffle = lambda v: jnp.concatenate([cut(v, owner[k] * rows, rows, 0) for k in range(n)])
        index, seg_ids, pos = shuffle(tokens), shuffle(seg_ids), shuffle(pos)
        inv_freq = 1.0 / ROPE_BASE ** (jnp.arange(HD // 2, dtype=F32) * (2.0 / HD))
        angles = pos[:, None] * inv_freq[None, :]
        cosine, sine = jnp.cos(angles), jnp.sin(angles)
        cos2 = jnp.concatenate([cosine, cosine], 1)
        sin2 = jnp.concatenate([-sine, sine], 1)
        tcol = jnp.stack([index, seg_ids], 0)
        trow = jnp.stack([index, seg_ids], 1)
        qg, kg = query_gain[None], key_gain[None]

        cut_rows = lambda w: w.reshape(2, m, half // m, w.shape[1])
        (
            normed, qkv, qr, kr, vb, attn_out, hidden, normed_mlp,
            qkv_mine, qkv_other, mlp_mine, mlp_other, all_grads,
        ) = front(
            n, m, nq, nk, activations[0], cotangent[0],
            [cut_rows(w) for w in (query_weight, key_weight, value_weight, gate_weight, up_weight)],
            out_weight,
            [attn_gain[None], qg, kg, mlp_gain[None]],
            [cos2, sin2, trow, tcol],
        )
        w_qkv = [v.reshape(n * half, -1) for v in (qkv_mine, qkv_other)]
        w_mlp = [v.reshape(n * half, -1) for v in (mlp_mine, mlp_other)]
        all_grads = all_grads.reshape(length, width)
        pre = times(normed_mlp, w_mlp)
        gate_pre, up_pre = pre[:, :ffl], pre[:, ffl:]
        sig = jax.nn.sigmoid(gate_pre)
        activated = (gate_pre * sig * up_pre).astype(BF)
        down_pair = rows_parts(halves(activated), all_grads)
        grad_act = dot_last(all_grads, down_weight)
        grad_gate = (grad_act * up_pre * sig * (1.0 + gate_pre * (1.0 - sig))).astype(BF)
        grad_up = (grad_act * gate_pre * sig).astype(BF)
        grad_pre = jnp.concatenate([grad_gate, grad_up], 1)
        mlp_pair = pair_parts(normed_mlp, grad_pre, n, half // m)
        dhn = restore(times_back(grad_pre, w_mlp)).reshape(n, rows, width)
        output = (
            hidden + scatter_sum(dot(activated, down_weight).reshape(n, rows, width))
        ).astype(BF)[None]

        segments_of = [down_pair, mlp_pair]
        parts = [(0, a, 0) for a in range(down_pair[0].shape[0])] + [(1, k, k) for k in range(n)]
        parts += [(2, a, 0) for a in range(nq * HD // 2 // half)] + [(3, k, k) for k in range(n)]
        grad_input, gains, *summed = back(
            n, m, nq, nk, parts, dhn, activations[0], cotangent[0], hidden, out_weight,
            [qkv_mine, qkv_other], qkv, [qr, kr, vb], attn_out, normed,
            [attn_gain[None], mlp_gain[None], qg, kg], [cos2, sin2, trow, tcol],
            [v[0] for v in segments_of], [v[1] for v in segments_of],
        )
        grad_input = grad_input[None]
        mines, others = summed[:4], summed[4:]

        pick = lambda seg, at=None, width=None: (
            (mines[seg], others[seg]) if at is None else (mines[seg], others[seg], at, width)
        )
        (
            grad_down, grad_out_weight, grad_gate_weight, grad_up_weight,
            grad_query_weight, grad_key_weight, grad_value_weight,
        ) = assemble(
            [pick(0), pick(2)],
            [
                pick(1, 0, ffl), pick(1, 1, ffl), pick(3, 0, nq * HD),
                pick(3, nq // nk, nk * HD), pick(3, nq // nk + 1, nk * HD),
            ],
            core,
            owner,
        )
        gains = gains.reshape(-1)
        grad_attn_gain, grad_mlp_gain = gains[:width], gains[width : 2 * width]
        grad_query_gain = gains[2 * width : 2 * width + HD]
        grad_key_gain = gains[2 * width + HD : 2 * width + 2 * HD]
        return (
            output,
            grad_input,
            grad_attn_gain,
            grad_query_weight,
            grad_key_weight,
            grad_value_weight,
            grad_query_gain,
            grad_key_gain,
            grad_out_weight,
            grad_mlp_gain,
            grad_gate_weight,
            grad_up_weight,
            grad_down,
        )

    return per_device


def solution(mesh):
    tok = P("rep", "shard", None)
    row = P("shard", None)
    return jax.shard_map(
        build(mesh.shape["shard"], mesh.shape["rep"]),
        mesh=mesh,
        in_specs=(
            tok, P("rep", None), P(), row, row, row, P(), P(), row, P(), row, row, row, tok,
        ),
        out_specs=(tok, tok, P(), row, row, row, P(), P(), row, P(), row, row, row),
        check_vma=False,
    )
```

```python
from functools import partial
import math

import jax
import jax.numpy as jnp
from jax import lax
from jax.experimental import pallas as pl
from jax.experimental.pallas import tpu as pltpu
from jax.sharding import PartitionSpec as P

HQ = 16
HK = 8
HD = 128
FF = 6144
GROUPS = HQ // HK

EPSILON = 1e-06
ROPE_BASE = 1000000.0
MASKED = -1e30
BF = jnp.bfloat16
F32 = jnp.float32

HOOK_TICKS = (0, 4, 6, 7, 8, 9, 11, 12, 13, 14, 15, 16, 18)


def dot(a, b):
    return jnp.dot(a, b, preferred_element_type=F32)


def dot_last(a, b):
    return lax.dot_general(a, b, (((1,), (1,)), ((), ())), preferred_element_type=F32)


def dot_first(a, b):
    return lax.dot_general(a, b, (((0,), (0,)), ((), ())), preferred_element_type=F32)


def positions(seg_ids):
    token_index = jnp.arange(seg_ids.shape[0], dtype=jnp.int32)
    before = jnp.concatenate([jnp.full((1,), -1, jnp.int32), seg_ids[:-1]])
    starts = lax.cummax(
        jnp.where(seg_ids != before, token_index, jnp.zeros_like(token_index)), axis=0
    )
    return (token_index - starts).astype(F32)


def head_rope(raw, gain, cos2, sin2):
    rstat = lax.rsqrt(jnp.mean(raw * raw, -1, keepdims=True) + EPSILON)
    scaled = raw * rstat * gain
    return scaled * cos2 + pltpu.roll(scaled, HD // 2, 1) * sin2


def attend_pair(qkv, j, nq, nk, qg, kg, cos2, sin2, trow, tcol, o_ref, qr_ref, kr_ref, vb_ref, scale):
    length = qkv.shape[0]
    block = min(length, 512)
    own = slice(j * HD, (j + 1) * HD)
    at = (nq + j) * HD
    kr = head_rope(qkv[:, at : at + HD], kg[...], cos2[...], sin2[...]).astype(BF)
    at = (nq + nk + j) * HD
    vb = qkv[:, at : at + HD].astype(BF)
    kr_ref[:, own] = kr
    vb_ref[:, own] = vb
    for g in range(GROUPS):
        cols = slice((j * GROUPS + g) * HD, (j * GROUPS + g + 1) * HD)
        qr_ref[:, cols] = head_rope(qkv[:, cols], qg[...], cos2[...], sin2[...]).astype(BF)
        for b in range(length // block):
            rows = slice(b * block, (b + 1) * block)
            s = dot_last(qr_ref[rows, cols], kr) * scale
            seen = (tcol[0:1, :] <= trow[rows, 0:1]) & (tcol[1:2, :] == trow[rows, 1:2])
            s = jnp.where(seen, s, MASKED)
            e = jnp.exp(s - jnp.max(s, -1, keepdims=True))
            p = (e / jnp.sum(e, -1, keepdims=True)).astype(BF)
            o_ref[rows, cols] = dot(p, vb).astype(BF)


def head_back(grad_rot, raw, gain, cos2, sin2):
    back = grad_rot * cos2 - pltpu.roll(grad_rot, HD // 2, 1) * sin2
    rstat = lax.rsqrt(jnp.mean(raw * raw, -1, keepdims=True) + EPSILON)
    scaled = raw * rstat
    gain_part = jnp.sum(back * scaled, 0, keepdims=True)
    b = back * gain
    return rstat * (b - scaled * jnp.mean(b * scaled, -1, keepdims=True)), gain_part


def attend_back_pair(
    j, nq, nk, qkv, qr_ref, kr_ref, vb_ref, do_ref, dqkv, qg, kg, cos_ref, sin_ref, trow, tcol, scale
):
    cos2, sin2 = cos_ref[...], sin_ref[...]
    own = slice(j * HD, (j + 1) * HD)
    length = qkv.shape[0]
    block = min(length, 256)
    kr, vb = kr_ref[:, own], vb_ref[:, own]
    dkr = jnp.zeros((length, HD), F32)
    dv = jnp.zeros((length, HD), F32)
    gq = jnp.zeros((1, HD), F32)
    for g in range(GROUPS):
        cols = slice((j * GROUPS + g) * HD, (j * GROUPS + g + 1) * HD)
        dqr = []
        for b in range(length // block):
            rows = slice(b * block, (b + 1) * block)
            qr, do = qr_ref[rows, cols], do_ref[rows, cols]
            s = dot_last(qr, kr) * scale
            seen = (tcol[0:1, :] <= trow[rows, 0:1]) & (tcol[1:2, :] == trow[rows, 1:2])
            s = jnp.where(seen, s, MASKED)
            e = jnp.exp(s - jnp.max(s, -1, keepdims=True))
            p = e / jnp.sum(e, -1, keepdims=True)
            dp = dot_last(do, vb)
            ds = (p * (dp - jnp.sum(p * dp, -1, keepdims=True))).astype(BF)
            dqr.append(dot(ds, kr) * scale)
            dkr += dot_first(ds, qr)
            dv += dot_first(p.astype(BF), do)
        dqr = dqr[0] if len(dqr) == 1 else jnp.concatenate(dqr, 0)
        dq, part = head_back(dqr, qkv[:, cols], qg[...], cos2, sin2)
        dqkv[:, cols] = dq.astype(BF)
        gq += part
    at = (nq + j) * HD
    dk, gk = head_back(dkr * scale, qkv[:, at : at + HD], kg[...], cos2, sin2)
    dqkv[:, at : at + HD] = dk.astype(BF)
    at = (nq + nk + j) * HD
    dqkv[:, at : at + HD] = dv.astype(BF)
    return gq, gk


def assemble_kernel(counts, order_ref, *refs):
    n_rows, n_cols = counts
    total = n_rows + n_cols
    mine, other, outs = refs[:total], refs[total : 2 * total], refs[2 * total :]

    def fill(sources):
        for src, out in zip(sources, outs):
            m, places, q, width = src.shape
            for a in range(places):
                out[a * m * q : (a + 1) * m * q, :] = (
                    src[:, a].reshape(m * q, width).astype(F32)
                )

    pl.when(pl.program_id(0) == 0)(lambda: fill(mine))
    pl.when(pl.program_id(0) == 1)(lambda: fill(other))


def assemble(rows, cols, core, owner):
    n = len(owner)
    order = jnp.stack(list(owner) + [core]).astype(jnp.int32)
    in_specs, out_specs, shapes, operands = [[], []], [], [], [[], []]
    size = 0
    for mine, other in rows:
        m, places, q, width = mine.shape
        block = (m, places, q, width // n)
        in_specs[0].append(
            pl.BlockSpec(block, lambda g, b, o: (0, 0, 0, jnp.where(g == 0, b, n - 1)))
        )
        in_specs[1].append(
            pl.BlockSpec(block, lambda g, b, o: (0, 0, 0, jnp.where(g == 0, 0, b)))
        )
        out_specs.append(
            pl.BlockSpec((places * m * q, width // n), lambda g, b, o: (g ^ o[n], b))
        )
        shapes.append(jax.ShapeDtypeStruct((2 * places * m * q, width), F32))
        operands[0].append(mine)
        operands[1].append(other)
        size += mine.size
    for mine, other, at, width in cols:
        m, _, q, _ = mine.shape
        block = (m, 1, q, width)
        in_specs[0].append(
            pl.BlockSpec(block, lambda g, b, o, at=at: (0, o[jnp.where(g == 0, b, n - 1)], 0, at))
        )
        in_specs[1].append(
            pl.BlockSpec(block, lambda g, b, o, at=at: (0, o[jnp.where(g == 0, 0, b)], 0, at))
        )
        out_specs.append(pl.BlockSpec((m * q, width), lambda g, b, o: (g ^ o[n], b)))
        shapes.append(jax.ShapeDtypeStruct((2 * m * q, n * width), F32))
        operands[0].append(mine)
        operands[1].append(other)
        size += m * n * q * width
    return pl.pallas_call(
        partial(assemble_kernel, (len(rows), len(cols))),
        out_shape=tuple(shapes),
        grid_spec=pltpu.PrefetchScalarGridSpec(
            num_scalar_prefetch=1,
            grid=(2, n),
            in_specs=in_specs[0] + in_specs[1],
            out_specs=tuple(out_specs),
        ),
        compiler_params=pltpu.CompilerParams(vmem_limit_bytes=56 << 20),
        cost_estimate=pl.CostEstimate(flops=0, bytes_accessed=12 * size, transcendentals=0),
        name="assemble",
    )(order, *operands[0], *operands[1])


MESH_ID = pl.DeviceIdType.MESH


def back_kernel(n, m, nq, nk, scale, parts, *refs):
    (x_hbm, hidden_hbm, wo_hbm, wd_hbm, qkv_mine, qkv_other, mlp_mine, mlp_other,
     qkv_hbm, qr_hbm, kr_hbm, vb_hbm, o_hbm, normed_hbm, hn_hbm, act_hbm, dy_hbm, dpre_hbm,
     ag, mg, qg, kg, cos2, sin2, trow, tcol,
     output, grad_in, gain_out) = refs[:29]
    mines, others, away_v, fins, refs = refs[29:33], refs[33:37], refs[37:41], refs[41:45], refs[45:]
    (ups, downs, send_v,
     x_v, hidden, wo, qkv, qr, kr, vb, o, normed, hn, act, dy_all, dpre,
     part_s, part_r, out_r, dz_all, do, dqkv, wtile, dtile, gain_ref,
     pair_s, pair_r, up_s, up_r, down_s, down_r,
     peer_s, peer_r, gup_s, gup_r, gdown_s, gdown_r, sib_s, sib_r, own_sem, gain_pair, gain_group,
     gain_line, gain_s, gain_r, in_sem, wt_sem, dhn_s, dhn_r, dz_s, dz_r, dn_s, dn_r, out_ss,
     out_rs) = refs
    rows, width = x_v.shape
    own = width // n
    half = own // 2
    ring = ups.shape[0]
    shard, rep = lax.axis_index("shard"), lax.axis_index("rep")
    i = rep // 2
    core = lax.rem(rep, 2)
    sibling = {"rep": 2 * i + 1 - core}
    above, below = {"rep": rep + 2}, {"rep": rep - 2}
    peers = [None] + [{"shard": shard ^ k} for k in range(1, n)]
    has_up, has_down = i < m - 1, i > 0

    barrier = pltpu.get_barrier_semaphore()

    def greet(dev):
        pl.semaphore_signal(barrier, inc=1, device_id=dev, device_id_type=MESH_ID)

    greet(sibling)
    for k in range(1, n):
        greet(peers[k])
    line = [None] + [{"rep": 2 * lax.rem(i + d, m) + core} for d in range(1, m)]
    for d in range(1, m):
        greet(line[d])

    loads = [
        pltpu.make_async_copy(src, dst, in_sem.at[f])
        for f, (src, dst) in enumerate(
            [
                (act_hbm, act), (dy_hbm, dy_all), (dpre_hbm, dpre), (hn_hbm, hn),
                (hidden_hbm, hidden), (wo_hbm, wo), (qkv_hbm, qkv), (qr_hbm, qr), (kr_hbm, kr),
                (vb_hbm, vb), (o_hbm, o), (normed_hbm, normed), (x_hbm, x_v),
            ]
        )
    ]
    for copy in loads:
        copy.start()
    pl.semaphore_wait(barrier, n + m - 1)

    def remote(src, dst, ssem, rsem, dev):
        return pltpu.make_async_remote_copy(
            src_ref=src, dst_ref=dst, send_sem=ssem, recv_sem=rsem,
            device_id=dev, device_id_type=MESH_ID,
        )

    def cols_of(p):
        return pl.ds(parts[p][3], parts[p][4])

    def chunk(p, j):
        seg, at = parts[p][:2]
        return away_v[seg].at[at, j, :, cols_of(p)]

    def fin(p):
        seg, at = parts[p][:2]
        return fins[seg].at[at, :, cols_of(p)]

    def out(refs, p, j):
        seg, at = parts[p][:2]
        return refs[seg].at[j, at, :, cols_of(p)]

    def pair_copy(p):
        seg, at = parts[p][:2]
        return remote(
            send_v.at[p % 3, :, :, pl.ds(0, parts[p][4])], away_v[seg].at[at, :, :, cols_of(p)],
            pair_s.at[p], pair_r.at[p], sibling,
        )

    def slot(ref, p, t):
        return ref.at[p % ring, t, :, pl.ds(0, parts[p][4])]

    def up_copy(p, t, src):
        return remote(src, slot(ups, p, t), up_s.at[p, t], up_r.at[p, t], above)

    def down_copy(p, t, src):
        return remote(src, slot(downs, p, t), down_s.at[p, t], down_r.at[p, t], below)

    def add_into(ref, other):
        ref[...] = (ref[...].astype(F32) + other[...].astype(F32)).astype(BF)

    def scatter_step(p, t):
        if t > 0:

            @pl.when((i > 0) & (i <= t) & has_up)
            def _():
                up_copy(p, t - 1, slot(ups, p, t - 1)).wait_recv()
                add_into(slot(ups, p, t - 1), chunk(p, m - 1 - t + i))

            @pl.when((i < m - 1) & (i >= m - 1 - t) & has_down)
            def _():
                down_copy(p, t - 1, slot(downs, p, t - 1)).wait_recv()
                add_into(slot(downs, p, t - 1), chunk(p, i - (m - 1 - t)))

            pl.when((i > 0) & (i <= t) & has_up)(
                lambda: up_copy(p, t, slot(ups, p, t - 1)).start()
            )
            pl.when((i < m - 1) & (i >= m - 1 - t) & has_down)(
                lambda: down_copy(p, t, slot(downs, p, t - 1)).start()
            )
        pl.when(i == 0)(lambda: up_copy(p, t, chunk(p, m - 1 - t)).start())
        pl.when(i == m - 1)(lambda: down_copy(p, t, chunk(p, t)).start())

    def peer_copy(p):
        return remote(chunk(p, i), fin(p), peer_s.at[p], peer_r.at[p], peers[parts[p][2]])

    def total(p):
        pl.when(has_down)(lambda: up_copy(p, m - 2, slot(ups, p, m - 2)).wait_recv())
        pl.when(has_up)(lambda: down_copy(p, m - 2, slot(downs, p, m - 2)).wait_recv())
        where = fin(p) if parts[p][2] == 0 else chunk(p, i)

        def put(*extra):
            value = chunk(p, i)[...].astype(F32)
            for e in extra:
                value = value + e[...].astype(F32)
            where[...] = value.astype(BF)

        u, d = slot(ups, p, m - 2), slot(downs, p, m - 2)
        pl.when(has_up & has_down)(lambda: put(u, d))
        pl.when(has_up & (i == 0))(lambda: put(d))
        pl.when(has_down & (i == m - 1))(lambda: put(u))
        if parts[p][2] != 0:
            peer_copy(p).start()

    def gup_copy(p, t, j, src):
        return remote(src, out(mines, p, j), gup_s.at[p, t], gup_r.at[p, t], above)

    def gdown_copy(p, t, j, src):
        return remote(src, out(mines, p, j), gdown_s.at[p, t], gdown_r.at[p, t], below)

    def sib_copy(p, j, src):
        return remote(src, out(others, p, j), sib_s.at[p, j], sib_r.at[p, j], sibling)

    def own_copy(p):
        return pltpu.make_async_copy(fin(p), out(mines, p, i), own_sem.at[p])

    def gather_step(p, t):
        if t == 0:
            for u in range(m - 1):
                pl.when((i <= u) & has_up)(lambda: up_copy(p, u, slot(ups, p, u)).wait_send())
                pl.when((i >= m - 1 - u) & has_down)(
                    lambda: down_copy(p, u, slot(downs, p, u)).wait_send()
                )
            if parts[p][2] != 0:
                peer_copy(p).wait_recv()
            pl.when(has_up)(lambda: gup_copy(p, 0, i, fin(p)).start())
            pl.when(has_down)(lambda: gdown_copy(p, 0, i, fin(p)).start())
            sib_copy(p, i, fin(p)).start()
            own_copy(p).start()
            return

        @pl.when(i - t >= 0)
        def _():
            here = out(mines, p, i - t)
            gup_copy(p, t - 1, i - t, here).wait_recv()
            if t < m - 1:
                pl.when(has_up)(lambda: gup_copy(p, t, i - t, here).start())
            sib_copy(p, i - t, here).start()

        @pl.when(i + t < m)
        def _():
            here = out(mines, p, i + t)
            gdown_copy(p, t - 1, i + t, here).wait_recv()
            if t < m - 1:
                pl.when(has_down)(lambda: gdown_copy(p, t, i + t, here).start())
            sib_copy(p, i + t, here).start()

    def gain_copies(level):
        if level == 0:
            return [remote(gain_ref, gain_pair, gain_s.at[0], gain_r.at[0], sibling)]
        if level == 1:
            return [
                remote(
                    gain_group.at[shard], gain_group.at[shard], gain_s.at[k], gain_r.at[k], peers[k]
                )
                for k in range(1, n)
            ]
        return [
            remote(
                gain_line.at[i], gain_line.at[i], gain_s.at[n - 1 + d], gain_r.at[n - 1 + d], line[d]
            )
            for d in range(1, m)
        ]

    def gains(level):
        if level > 0:
            for copy in gain_copies(level - 1):
                copy.wait_recv()
        if level == 1:
            gain_group[shard] = gain_ref[...] + gain_pair[...]
        elif level == 2:
            value = gain_group[0]
            for k in range(1, n):
                value = value + gain_group[k]
            gain_line[i] = value
        elif level == 3:
            value = gain_line[0]
            for k in range(1, m):
                value = value + gain_line[k]
            gain_out[...] = value
        if level < 3:
            for copy in gain_copies(level):
                copy.start()

    def tiles(cols, first=0):
        step = max(v for v in range(HD, 513, HD) if cols % v == 0)
        return [(c, pl.ds(first + c, step), pl.ds(c, step)) for c in range(0, cols, step)]

    def product(p, h, at):
        seg, place, k = parts[p][:3]
        if seg in (0, 2):
            ref = act if seg == 0 else o
            both = ref.shape[1] // 2
            start = (core if h == 0 else 1 - core) * both + place * half
            left = ref[:, pl.ds(pl.multiple_of(start, half), half)]
            right = (dy_all if seg == 0 else dz_all)[:, :, at].reshape(n * rows, at.size)
        else:
            left = (hn if seg == 1 else normed)[:, (h * n + k) * half : (h * n + k + 1) * half]
            right = (dpre if seg == 1 else dqkv)[:, at]
        return dot_first(left, right).reshape(m, half // m, at.size)

    def send(p):
        if p >= 3:
            pair_copy(p - 3).wait_send()
        for _, at, to in tiles(parts[p][4], parts[p][3]):
            send_v[p % 3, :, :, to] = product(p, 1, at).astype(BF)
        pair_copy(p).start()

    def first(p):
        seg, place = parts[p][:2]
        pair_copy(p).wait_recv()
        for _, at, _ in tiles(parts[p][4], parts[p][3]):
            away_v[seg][place, :, :, at] = (
                product(p, 0, at) + away_v[seg][place, :, :, at].astype(F32)
            ).astype(BF)
        scatter_step(p, 0)

    def dhn_copy(k):
        return remote(part_s.at[k], part_r.at[k - 1], dhn_s.at[k], dhn_r.at[k], peers[k])

    def dn_copy(k):
        return remote(part_s.at[k], part_r.at[k - 1], dn_s.at[k], dn_r.at[k], peers[k])

    def out_copy(k):
        return remote(part_s.at[k], out_r.at[k - 1], out_ss.at[k], out_rs.at[k], peers[k])

    def dz_copy(k):
        return remote(dz_all.at[0], dz_all.at[k], dz_s.at[k], dz_r.at[k], peers[k])

    strip = min(rows, 32)

    def strips(body):
        pl.loop(0, rows // strip)(
            lambda b: body(pl.ds(pl.multiple_of(b * strip, strip), strip))
        )

    def add_gain(at, value):
        for b in range(value.shape[1] // HD):
            gain_ref[at + b : at + b + 1, :] += value[:, b * HD : (b + 1) * HD]

    def norm_back(values, gain, at, result):
        def body(r):
            v = values[r, :].astype(F32)
            rstat = lax.rsqrt(jnp.mean(v * v, -1, keepdims=True) + EPSILON)
            scaled = v * rstat
            grad = part_s[0, r, :].astype(F32)
            for k in range(1, n):
                grad = grad + part_r[k - 1, r, :].astype(F32)
            add_gain(at, jnp.sum(grad * scaled, 0, keepdims=True))
            weighted = grad * gain[...]
            result(
                r, rstat * (weighted - scaled * jnp.mean(weighted * scaled, -1, keepdims=True))
            )

        strips(body)

    def partial_rows(grads, mine, other):
        cols = grads.shape[1]

        def tile_copy(b):
            src = (mine if b < n else other).at[b % n]
            return pltpu.make_async_copy(
                src, wtile.at[b % 2, :, :, pl.ds(0, cols)], wt_sem.at[b % 2]
            )

        tile_copy(0).start()
        for b in range(2 * n):
            tile_copy(b).wait()
            if b + 1 < 2 * n:
                tile_copy(b + 1).start()
            h, kk = b // n, b % n
            at = pl.ds(
                pl.multiple_of((shard ^ kk) * own + (core if h == 0 else 1 - core) * half, half),
                half,
            )
            w = wtile[b % 2, :, :, :cols].reshape(half, cols)
            for k in range(n):
                part_s[k, :, at] = dot_last(grads[k * rows : (k + 1) * rows, :], w).astype(BF)

    def hook_dhn():
        loads[2].wait()
        partial_rows(dpre, mlp_mine, mlp_other)
        for k in range(1, n):
            dhn_copy(k).start()

    def hook_hidden():
        loads[4].wait()
        for k in range(1, n):
            dhn_copy(k).wait_recv()
        gain_ref[...] = jnp.zeros_like(gain_ref)

        def result(r, value):
            value = dy_all[0, r, :].astype(F32) + value
            grad_in[r, :] = value
            dz_all[0, r, :] = value.astype(BF)

        norm_back(hidden, mg, width // HD, result)
        for k in range(1, n):
            dz_copy(k).start()

    def hook_do():
        for copy in loads[5:]:
            copy.wait()
        for k in range(n):
            if k > 0:
                dz_copy(k).wait_recv()
            do[k * rows : (k + 1) * rows, :] = dot_last(dz_all[k], wo[...]).astype(BF)

    def hook_head(j):
        gq, gk = attend_back_pair(
            j, nq, nk, qkv, qr, kr, vb, do, dqkv, qg, kg, cos2, sin2, trow, tcol, scale
        )
        add_gain(2 * width // HD, gq)
        add_gain(2 * width // HD + 1, gk)

    def hook_normed():
        for k in range(1, n):
            dhn_copy(k).wait_send()
        partial_rows(dqkv, qkv_mine, qkv_other)
        for k in range(1, n):
            dn_copy(k).start()

    def hook_input():
        for k in range(1, n):
            dn_copy(k).wait_recv()

        def result(r, value):
            grad_in[r, :] = grad_in[r, :] + value

        norm_back(x_v, ag, 0, result)

    def hook_down():
        for k in range(1, n):
            dn_copy(k).wait_send()
        step = dtile.shape[2]

        def tile_copy(b):
            return pltpu.make_async_copy(
                wd_hbm.at[:, pl.ds(b * step, step)], dtile.at[b % 2], wt_sem.at[b % 2]
            )

        tile_copy(0).start()
        for b in range(width // step):
            tile_copy(b).wait()
            if b + 1 < width // step:
                tile_copy(b + 1).start()
            for k in range(n):
                part_s[k, :, b * step : (b + 1) * step] = dot(
                    act[k * rows : (k + 1) * rows, :], dtile[b % 2]
                ).astype(BF)
        for k in range(1, n):
            out_copy(k).start()

    def hook_output():
        for k in range(1, n):
            out_copy(k).wait_recv()

        def body(r):
            value = hidden[r, :] + part_s[0, r, :].astype(F32)
            for k in range(1, n):
                value = value + out_r[k - 1, r, :].astype(F32)
            output[r, :] = value.astype(BF)

        strips(body)

    at_tick = {}
    hooks = [hook_dhn, hook_hidden, hook_do] + [partial(hook_head, j) for j in range(nk)]
    hooks += [hook_normed, hook_input] + [partial(gains, level) for level in range(4)]
    hooks += [hook_down, hook_output]
    for hook, tick in zip(hooks, HOOK_TICKS[:3] + HOOK_TICKS[3 : 3 + nk] + HOOK_TICKS[-8:]):
        at_tick.setdefault(tick, []).append(hook)

    stages = [first] + [lambda p, t=t: scatter_step(p, t) for t in range(1, m - 1)]
    stages += [total] + [lambda p, t=t: gather_step(p, t) for t in range(m)]

    loads[0].wait()
    loads[1].wait()
    send(0)
    send(1)
    ticks = len(parts) + len(stages) - 1
    for tick in range(max(ticks, max(at_tick) + 1)):
        if tick == 0:
            loads[3].wait()
        for st in range(len(stages) - 1, -1, -1):
            p = tick - st
            if 0 <= p < len(parts):
                stages[st](p)
        for hook in at_tick.get(tick, []):
            hook()
        if tick + 2 < len(parts):
            send(tick + 2)

    for k in range(1, n):
        dz_copy(k).wait_send()
        out_copy(k).wait_send()
    for level in range(3):
        for copy in gain_copies(level):
            copy.wait_send()
    for p in range(len(parts)):
        if p >= len(parts) - 3:
            pair_copy(p).wait_send()
        if parts[p][2] != 0:
            peer_copy(p).wait_send()
        own_copy(p).wait()
        for t in range(m - 1):
            pl.when((i - t >= 0) & has_up)(lambda: gup_copy(p, t, i, fin(p)).wait_send())
            pl.when((i + t < m) & has_down)(lambda: gdown_copy(p, t, i, fin(p)).wait_send())
        for j in range(m):
            copy = sib_copy(p, j, fin(p))
            copy.wait_send()
            copy.wait_recv()


def back(n, m, nq, nk, x, hidden, wo, wd, weights, qkv, heads, o, normed, hn, act, dy_all, dpre,
         gains, tables):
    rows, width = x.shape
    length = n * rows
    q, cols = weights[0].shape[2:]
    wide = dpre.shape[1]
    half = m * q
    dma = pltpu.SemaphoreType.DMA
    sd = jax.ShapeDtypeStruct
    hbm, vmem = pl.BlockSpec(memory_space=pl.ANY), pl.BlockSpec(memory_space=pltpu.VMEM)
    segments = [
        (act.shape[1] // 2 // half, m, q, width), (n, m, q, wide),
        (nq * HD // 2 // half, m, q, width), (n, m, q, cols),
    ]

    def cut(seg, at, k, sizes):
        out, c = [], 0
        for size in sizes:
            out.append((seg, at, k, c, size))
            c += size
        return out

    parts = cut(0, 0, 0, [width // 4, width // 4, width // 2])
    for a in range(1, segments[0][0]):
        parts += cut(0, a, 0, [width // 2] * 2)
    for k in range(n):
        parts += cut(1, k, k, [wide // 2] * 2)
    for a in range(segments[2][0]):
        parts += cut(2, a, 0, [width // 2] * 2)
    for k in range(n):
        parts += cut(3, k, k, [cols] if k < n - 1 else [cols // 2] * 2)
    total = len(parts)
    most = max(part[4] for part in parts)
    ring = m + 2
    count = 2 * width // HD + 2
    gain_shape = (count + -count % 8, HD)
    outs = [sd((m, v[0]) + v[2:], BF) for v in segments]
    like = lambda v: pltpu.VMEM(v.shape, v.dtype)
    operands = [x, hidden, wo, wd, *weights, qkv, *heads, o, normed, hn, act, dy_all, dpre]
    return pl.pallas_call(
        partial(back_kernel, n, m, nq, nk, 1.0 / math.sqrt(HD), parts),
        out_shape=tuple(
            [sd((rows, width), BF), sd((rows, width), F32), sd(gain_shape, F32)] + outs + outs
        ),
        in_specs=[hbm] * len(operands) + [vmem] * 8,
        out_specs=tuple([vmem] * 3 + [hbm] * 8),
        scratch_shapes=[pltpu.VMEM(v, BF) for v in segments]
        + [pltpu.VMEM(v[:1] + v[2:], BF) for v in segments]
        + [pltpu.VMEM((ring, m - 1, q, most), BF)] * 2
        + [pltpu.VMEM((3, m, q, most), BF)]
        + [like(v) for v in (x, hidden, wo, qkv, *heads, o, normed, hn, act, dy_all, dpre)]
        + [
            pltpu.VMEM((n, rows, width), BF), pltpu.VMEM((n - 1, rows, width), BF),
            pltpu.VMEM((n - 1, rows, width), BF), pltpu.VMEM((n, rows, width), BF),
            pltpu.VMEM((length, nq * HD), BF), pltpu.VMEM((length, cols), BF),
            pltpu.VMEM((2, m, q, wide), BF), pltpu.VMEM((2, wd.shape[0], 256), BF),
            pltpu.VMEM(gain_shape, F32),
            dma((total,)), dma((total,)),
            dma((total, m - 1)), dma((total, m - 1)), dma((total, m - 1)), dma((total, m - 1)),
            dma((total,)), dma((total,)),
            dma((total, m - 1)), dma((total, m - 1)), dma((total, m - 1)), dma((total, m - 1)),
            dma((total, m)), dma((total, m)), dma((total,)),
            pltpu.VMEM(gain_shape, F32), pltpu.VMEM((n,) + gain_shape, F32),
            pltpu.VMEM((m,) + gain_shape, F32), dma((n + m,)), dma((n + m,)),
            dma((13,)), dma((2,)),
        ]
        + [dma((n,))] * 8,
        compiler_params=pltpu.CompilerParams(
            collective_id=3, has_side_effects=True, vmem_limit_bytes=67043328
        ),
        name="back",
    )(*operands, *gains, *tables)


def front_kernel(
    n, m, nq, nk, scale,
    x_hbm, dy_hbm, wq, wk, wv, wg, wu, wo_hbm,
    ag, qg, kg, mg, cos2, sin2, trow, tcol,
    normed, qkv, qr, kr, vb, o, hidden, hn, qkv_mine, qkv_other, mlp_mine, mlp_other, dy_all,
    x_all, wo, bounce, dy_v, hn_all, part_own, part_s, part_r,
    x_ss, x_rs, w_ss, w_rs, up_ss, up_rs, down_ss, down_rs, sib_ss, sib_rs,
    own_sem, back_sem, load_sem, part_ss, part_rs, hn_ss, hn_rs, dy_ss, dy_rs
):
    shard, rep = lax.axis_index("shard"), lax.axis_index("rep")
    i = rep // 2
    core = lax.rem(rep, 2)
    sibling = {"rep": 2 * i + 1 - core}
    above, below = {"rep": rep + 2}, {"rep": rep - 2}
    peers = [None] + [{"shard": shard ^ k} for k in range(1, n)]
    has_up, has_down = i < m - 1, i > 0
    rows, width = x_all.shape[1], x_all.shape[2]
    own = width // n
    half = own // 2

    barrier = pltpu.get_barrier_semaphore()

    def greet(dev):
        pl.semaphore_signal(barrier, inc=1, device_id=dev, device_id_type=MESH_ID)

    greet(sibling)
    for k in range(1, n):
        greet(peers[k])
    for d in range(1, m):
        greet({"rep": 2 * lax.rem(i + d, m) + core})
    pl.semaphore_wait(barrier, n + m - 1)

    def remote(src, dst, ssem, rsem, dev):
        return pltpu.make_async_remote_copy(
            src_ref=src, dst_ref=dst, send_sem=ssem, recv_sem=rsem,
            device_id=dev, device_id_type=MESH_ID,
        )

    groups = [
        ([wq, wk, wv], qkv_mine, qkv_other),
        ([wg, wu], mlp_mine, mlp_other),
    ]

    def fields(weights):
        at = 0
        for w in weights:
            size = w.shape[3] // n
            yield w, at, size
            at += size

    def cols_of(k, size):
        return pl.ds(pl.multiple_of((shard ^ k) * size, size), size)

    def piece_copies(g, k):
        weights, mine, _ = groups[g]
        return [
            remote(
                w.at[core, i, :, cols_of(k, size)],
                mine.at[k, i, :, pl.ds(at, size)],
                w_ss.at[g, k, f], w_rs.at[g, k, f], peers[k],
            )
            for f, (w, at, size) in enumerate(fields(weights))
        ]

    def own_copies(g):
        weights, mine, other = groups[g]
        out = []
        for h, dst in enumerate((mine, other)):
            for f, (w, at, size) in enumerate(fields(weights)):
                to = dst.at[0, :, :, pl.ds(at, size)] if g == 0 else bounce.at[h, :, :, pl.ds(at, size)]
                src = w.at[core if h == 0 else 1 - core, :, :, cols_of(0, size)]
                out.append(pltpu.make_async_copy(src, to, own_sem.at[g, h, f]))
        return out

    def back_copies():
        return [
            pltpu.make_async_copy(bounce.at[h], dst.at[0], back_sem.at[h])
            for h, dst in enumerate((mlp_mine, mlp_other))
        ]

    def region(ref, j):
        return ref.at[pl.ds(1, n - 1), j]

    def up_copy(g, t, j):
        r = region(groups[g][1], j)
        return remote(r, r, up_ss.at[g, t], up_rs.at[g, t], above)

    def down_copy(g, t, j):
        r = region(groups[g][1], j)
        return remote(r, r, down_ss.at[g, t], down_rs.at[g, t], below)

    def sib_copy(g, j):
        _, mine, other = groups[g]
        return remote(region(mine, j), region(other, j), sib_ss.at[g, j], sib_rs.at[g, j], sibling)

    def gather_weights(g, t):
        if t == 0:
            for k in range(1, n):
                for copy in piece_copies(g, k):
                    copy.wait_recv()
            pl.when(has_up)(lambda: up_copy(g, 0, i).start())
            pl.when(has_down)(lambda: down_copy(g, 0, i).start())
            sib_copy(g, i).start()
            return

        @pl.when(i - t >= 0)
        def _():
            up_copy(g, t - 1, i - t).wait_recv()
            if t < m - 1:
                pl.when(has_up)(lambda: up_copy(g, t, i - t).start())
            sib_copy(g, i - t).start()

        @pl.when(i + t < m)
        def _():
            down_copy(g, t - 1, i + t).wait_recv()
            if t < m - 1:
                pl.when(has_down)(lambda: down_copy(g, t, i + t).start())
            sib_copy(g, i + t).start()

    def x_copy(k):
        return remote(x_hbm, x_all.at[k], x_ss.at[k], x_rs.at[k], peers[k])

    def dy_copy(k):
        return remote(dy_hbm, dy_all.at[k], dy_ss.at[k], dy_rs.at[k], peers[k])

    def hn_copy(k):
        return remote(hn_all.at[0], hn_all.at[k], hn_ss.at[k], hn_rs.at[k], peers[k])

    def part_copy(k):
        return remote(part_s.at[k], part_r.at[k], part_ss.at[k], part_rs.at[k], peers[k])

    load_x = pltpu.make_async_copy(x_hbm, x_all.at[0], load_sem.at[0])
    load_wo = pltpu.make_async_copy(wo_hbm, wo, load_sem.at[1])
    load_dy = pltpu.make_async_copy(dy_hbm, dy_v, load_sem.at[2])
    keep_dy = pltpu.make_async_copy(dy_v, dy_all.at[0], load_sem.at[3])

    load_x.start()
    for k in range(1, n):
        for copy in piece_copies(0, k):
            copy.start()
    for k in range(1, n):
        x_copy(k).start()
    for copy in own_copies(0):
        copy.start()
    for k in range(1, n):
        for copy in piece_copies(1, k):
            copy.start()
    for copy in own_copies(1):
        copy.start()
    load_wo.start()
    load_dy.start()

    def place(k, h, kk):
        return pl.ds(
            pl.multiple_of((shard ^ kk) * own + (core if h == 0 else 1 - core) * half, half), half
        )

    gather_weights(0, 0)
    for k in range(n):
        if k == 0:
            load_x.wait()
        else:
            x_copy(k).wait_recv()
        v = x_all[k].astype(F32)
        r = lax.rsqrt(jnp.mean(v * v, -1, keepdims=True) + EPSILON)
        for h in range(2):
            for kk in range(n):
                at = place(k, h, kk)
                normed[k * rows : (k + 1) * rows, (h * n + kk) * half : (h * n + kk + 1) * half] = (
                    x_all[k, :, at].astype(F32) * r * ag[:, at]
                ).astype(BF)
    for t in range(1, m - 1):
        gather_weights(0, t)
    gather_weights(1, 0)
    gather_weights(0, m - 1)
    for copy in own_copies(0):
        copy.wait()
    for j in range(m):
        sib_copy(0, j).wait_recv()

    cols = qkv.shape[1]
    step = min(cols, 256)

    @pl.loop(0, cols // step)
    def _(b):
        at = pl.ds(pl.multiple_of(b * step, step), step)
        both = n * half
        qkv[:, at] = dot(
            normed[:, :both], qkv_mine[:, :, :, at].reshape(both, step)
        ) + dot(normed[:, both:], qkv_other[:, :, :, at].reshape(both, step))

    hop = 1
    for copy in own_copies(1):
        copy.wait()
    for copy in back_copies():
        copy.start()
    load_dy.wait()
    keep_dy.start()
    for j in range(nk):
        attend_pair(qkv, j, nq, nk, qg, kg, cos2, sin2, trow, tcol, o, qr, kr, vb, scale)
        if j == 0 and hop < m - 1:
            gather_weights(1, hop)
            hop += 1

    load_wo.wait()
    step = min(width, 512)

    @pl.loop(0, width // step)
    def _(b):
        at = pl.ds(pl.multiple_of(b * step, step), step)
        for k in range(n):
            value = dot(o[k * rows : (k + 1) * rows, :], wo[:, at])
            if k == 0:
                part_own[:, at] = value
            else:
                part_s[k, :, at] = value.astype(BF)

    for k in range(1, n):
        part_copy(k).start()
    if hop < m - 1:
        gather_weights(1, hop)
        hop += 1
    total = x_all[0].astype(F32) + part_own[...]
    for k in range(1, n):
        part_copy(k).wait_recv()
        total = total + part_r[k].astype(F32)
    hidden[...] = total
    r = lax.rsqrt(jnp.mean(total * total, -1, keepdims=True) + EPSILON)
    hn_all[0] = (total * r * mg[...]).astype(BF)
    for k in range(1, n):
        hn_copy(k).start()
    for k in range(1, n):
        dy_copy(k).start()
    while hop < m - 1:
        gather_weights(1, hop)
        hop += 1
    for k in range(n):
        if k > 0:
            hn_copy(k).wait_recv()
        for h in range(2):
            for kk in range(n):
                hn[k * rows : (k + 1) * rows, (h * n + kk) * half : (h * n + kk + 1) * half] = (
                    hn_all[k, :, place(k, h, kk)]
                )
    gather_weights(1, m - 1)

    for copy in back_copies():
        copy.wait()
    keep_dy.wait()
    for k in range(1, n):
        for g in range(2):
            for copy in piece_copies(g, k):
                copy.wait_send()
        x_copy(k).wait_send()
        part_copy(k).wait_send()
        hn_copy(k).wait_send()
        dy_copy(k).wait_send()
        dy_copy(k).wait_recv()
    for g in range(2):
        for j in range(m):
            sib_copy(g, j).wait_send()
            if g == 1:
                sib_copy(g, j).wait_recv()
        for t in range(m - 1):
            pl.when((i - t >= 0) & has_up)(lambda: up_copy(g, t, i).wait_send())
            pl.when((i + t < m) & has_down)(lambda: down_copy(g, t, i).wait_send())


def front(n, m, nq, nk, x, dy, weights, wo, gains, tables):
    rows, width = x.shape
    length = n * rows
    q = weights[0].shape[2]
    cols = [sum(w.shape[3] // n for w in ws) for ws in (weights[:3], weights[3:])]
    vmem, hbm = pl.BlockSpec(memory_space=pltpu.VMEM), pl.BlockSpec(memory_space=pl.ANY)
    dma = pltpu.SemaphoreType.DMA
    sd = jax.ShapeDtypeStruct
    outs = [
        (sd((length, width), BF), vmem),
        (sd((length, cols[0]), F32), vmem),
        (sd((length, nq * HD), BF), vmem),
        (sd((length, nk * HD), BF), vmem),
        (sd((length, nk * HD), BF), vmem),
        (sd((length, nq * HD), BF), vmem),
        (sd((rows, width), F32), vmem),
        (sd((length, width), BF), vmem),
        (sd((n, m, q, cols[0]), BF), vmem),
        (sd((n, m, q, cols[0]), BF), vmem),
        (sd((n, m, q, cols[1]), BF), hbm),
        (sd((n, m, q, cols[1]), BF), hbm),
        (sd((n, rows, width), BF), hbm),
    ]
    return pl.pallas_call(
        partial(front_kernel, n, m, nq, nk, 1.0 / math.sqrt(HD)),
        out_shape=tuple(v[0] for v in outs),
        in_specs=[hbm] * 8 + [vmem] * 8,
        out_specs=tuple(v[1] for v in outs),
        scratch_shapes=[
            pltpu.VMEM((n, rows, width), BF),
            pltpu.VMEM(wo.shape, BF),
            pltpu.VMEM((2, m, q, cols[1]), BF),
            pltpu.VMEM((rows, width), BF),
            pltpu.VMEM((n, rows, width), BF),
            pltpu.VMEM((rows, width), F32),
            pltpu.VMEM((n, rows, width), BF),
            pltpu.VMEM((n, rows, width), BF),
            dma((n,)), dma((n,)),
            dma((2, n, 3)), dma((2, n, 3)),
            dma((2, m)), dma((2, m)), dma((2, m)), dma((2, m)), dma((2, m)), dma((2, m)),
            dma((2, 2, 3)), dma((2,)), dma((4,)),
            dma((n,)), dma((n,)), dma((n,)), dma((n,)), dma((n,)), dma((n,)),
        ],
        compiler_params=pltpu.CompilerParams(
            collective_id=1, has_side_effects=True, vmem_limit_bytes=60 << 20
        ),
        name="front",
    )(x, dy, *weights, wo, *gains, *tables)


def build(n, reps):
    m = reps // 2

    def per_device(
        activations, segments, attn_gain, query_weight, key_weight, value_weight,
        query_gain, key_gain, out_weight, mlp_gain, gate_weight, up_weight, down_weight,
        cotangent,
    ):
        rows, width = activations.shape[1], activations.shape[2]
        length = segments.shape[1]
        shard = lax.axis_index("shard")
        core = lax.axis_index("rep") % 2
        own = width // n
        half = own // 2
        nq, nk = HQ // n, HK // n
        ffl = FF // n
        owner = [shard ^ k for k in range(n)]

        def cut(v, start, size, axis):
            return lax.dynamic_slice_in_dim(v, start, size, axis)

        def times(v, w):
            both = v.shape[1] // 2
            return dot(v[:, :both], w[0]) + dot(v[:, both:], w[1])

        seg_ids = segments[0]
        pos = positions(seg_ids)
        tokens = jnp.arange(length, dtype=jnp.int32)
        shuffle = lambda v: jnp.concatenate([cut(v, owner[k] * rows, rows, 0) for k in range(n)])
        index, seg_ids, pos = shuffle(tokens), shuffle(seg_ids), shuffle(pos)
        inv_freq = 1.0 / ROPE_BASE ** (jnp.arange(HD // 2, dtype=F32) * (2.0 / HD))
        angles = pos[:, None] * inv_freq[None, :]
        cosine, sine = jnp.cos(angles), jnp.sin(angles)
        cos2 = jnp.concatenate([cosine, cosine], 1)
        sin2 = jnp.concatenate([-sine, sine], 1)
        tcol = jnp.stack([index, seg_ids], 0)
        trow = jnp.stack([index, seg_ids], 1)
        qg, kg = query_gain[None], key_gain[None]

        cut_rows = lambda w: w.reshape(2, m, half // m, w.shape[1])
        (
            normed, qkv, qr, kr, vb, attn_out, hidden, normed_mlp,
            qkv_mine, qkv_other, mlp_mine, mlp_other, all_grads,
        ) = front(
            n, m, nq, nk, activations[0], cotangent[0],
            [cut_rows(w) for w in (query_weight, key_weight, value_weight, gate_weight, up_weight)],
            out_weight,
            [attn_gain[None], qg, kg, mlp_gain[None]],
            [cos2, sin2, trow, tcol],
        )
        w_mlp = [v.reshape(n * half, -1) for v in (mlp_mine, mlp_other)]
        flat_grads = all_grads.reshape(length, width)
        pre = times(normed_mlp, w_mlp)
        gate_pre, up_pre = pre[:, :ffl], pre[:, ffl:]
        sig = jax.nn.sigmoid(gate_pre)
        activated = (gate_pre * sig * up_pre).astype(BF)
        grad_act = dot_last(flat_grads, down_weight)
        grad_gate = (grad_act * up_pre * sig * (1.0 + gate_pre * (1.0 - sig))).astype(BF)
        grad_up = (grad_act * gate_pre * sig).astype(BF)
        grad_pre = jnp.concatenate([grad_gate, grad_up], 1)
        output, grad_input, gains, *summed = back(
            n, m, nq, nk, activations[0], hidden, out_weight, down_weight,
            [qkv_mine, qkv_other, mlp_mine, mlp_other], qkv, [qr, kr, vb], attn_out, normed,
            normed_mlp, activated, all_grads, grad_pre,
            [attn_gain[None], mlp_gain[None], qg, kg], [cos2, sin2, trow, tcol],
        )
        output, grad_input = output[None], grad_input[None]
        mines, others = summed[:4], summed[4:]

        pick = lambda seg, at=None, width=None: (
            (mines[seg], others[seg]) if at is None else (mines[seg], others[seg], at, width)
        )
        (
            grad_down, grad_out_weight, grad_gate_weight, grad_up_weight,
            grad_query_weight, grad_key_weight, grad_value_weight,
        ) = assemble(
            [pick(0), pick(2)],
            [
                pick(1, 0, ffl), pick(1, 1, ffl), pick(3, 0, nq * HD),
                pick(3, nq // nk, nk * HD), pick(3, nq // nk + 1, nk * HD),
            ],
            core,
            owner,
        )
        gains = gains.reshape(-1)
        grad_attn_gain, grad_mlp_gain = gains[:width], gains[width : 2 * width]
        grad_query_gain = gains[2 * width : 2 * width + HD]
        grad_key_gain = gains[2 * width + HD : 2 * width + 2 * HD]
        return (
            output,
            grad_input,
            grad_attn_gain,
            grad_query_weight,
            grad_key_weight,
            grad_value_weight,
            grad_query_gain,
            grad_key_gain,
            grad_out_weight,
            grad_mlp_gain,
            grad_gate_weight,
            grad_up_weight,
            grad_down,
        )

    return per_device


def solution(mesh):
    tok = P("rep", "shard", None)
    row = P("shard", None)
    return jax.shard_map(
        build(mesh.shape["shard"], mesh.shape["rep"]),
        mesh=mesh,
        in_specs=(
            tok, P("rep", None), P(), row, row, row, P(), P(), row, P(), row, row, row, tok,
        ),
        out_specs=(tok, tok, P(), row, row, row, P(), P(), row, P(), row, row, row),
        check_vma=False,
    )
```

```python
from functools import partial
import math

import jax
import jax.numpy as jnp
from jax import lax
from jax.experimental import pallas as pl
from jax.experimental.pallas import tpu as pltpu
from jax.sharding import PartitionSpec as P

HQ = 16
HK = 8
HD = 128
FF = 6144
GROUPS = HQ // HK

EPSILON = 1e-06
ROPE_BASE = 1000000.0
MASKED = -1e30
BF = jnp.bfloat16
F32 = jnp.float32

DHN_TICK = 1


def dot(a, b):
    return jnp.dot(a, b, preferred_element_type=F32)


def dot_last(a, b):
    return lax.dot_general(a, b, (((1,), (1,)), ((), ())), preferred_element_type=F32)


def dot_first(a, b):
    return lax.dot_general(a, b, (((0,), (0,)), ((), ())), preferred_element_type=F32)


def positions(seg_ids):
    token_index = jnp.arange(seg_ids.shape[0], dtype=jnp.int32)
    before = jnp.concatenate([jnp.full((1,), -1, jnp.int32), seg_ids[:-1]])
    starts = lax.cummax(
        jnp.where(seg_ids != before, token_index, jnp.zeros_like(token_index)), axis=0
    )
    return (token_index - starts).astype(F32)


def head_rope(raw, gain, cos2, sin2):
    rstat = lax.rsqrt(jnp.mean(raw * raw, -1, keepdims=True) + EPSILON)
    scaled = raw * rstat * gain
    return scaled * cos2 + pltpu.roll(scaled, HD // 2, 1) * sin2


def attend_pair(qkv, j, nq, nk, qg, kg, cos2, sin2, trow, tcol, o_ref, qr_ref, kr_ref, vb_ref, scale):
    length = qkv.shape[0]
    block = min(length, 512)
    own = slice(j * HD, (j + 1) * HD)
    at = (nq + j) * HD
    kr = head_rope(qkv[:, at : at + HD], kg[...], cos2[...], sin2[...]).astype(BF)
    at = (nq + nk + j) * HD
    vb = qkv[:, at : at + HD].astype(BF)
    kr_ref[:, own] = kr
    vb_ref[:, own] = vb
    for g in range(GROUPS):
        cols = slice((j * GROUPS + g) * HD, (j * GROUPS + g + 1) * HD)
        qr_ref[:, cols] = head_rope(qkv[:, cols], qg[...], cos2[...], sin2[...]).astype(BF)
        for b in range(length // block):
            rows = slice(b * block, (b + 1) * block)
            s = dot_last(qr_ref[rows, cols], kr) * scale
            seen = (tcol[0:1, :] <= trow[rows, 0:1]) & (tcol[1:2, :] == trow[rows, 1:2])
            s = jnp.where(seen, s, MASKED)
            e = jnp.exp(s - jnp.max(s, -1, keepdims=True))
            p = (e * (1.0 / jnp.sum(e, -1, keepdims=True))).astype(BF)
            o_ref[rows, cols] = dot(p, vb).astype(BF)


def head_back(grad_rot, raw, gain, cos2, sin2):
    back = grad_rot * cos2 - pltpu.roll(grad_rot, HD // 2, 1) * sin2
    rstat = lax.rsqrt(jnp.mean(raw * raw, -1, keepdims=True) + EPSILON)
    scaled = raw * rstat
    gain_part = jnp.sum(back * scaled, 0, keepdims=True)
    b = back * gain
    return rstat * (b - scaled * jnp.mean(b * scaled, -1, keepdims=True)), gain_part


def attend_back_pair(
    j, nq, nk, qkv, qr_ref, kr_ref, vb_ref, do_ref, dqkv, qg, kg, cos_ref, sin_ref, trow, tcol, scale
):
    cos2, sin2 = cos_ref[...], sin_ref[...]
    own = slice(j * HD, (j + 1) * HD)
    length = qkv.shape[0]
    block = min(length, 256)
    kr, vb = kr_ref[:, own], vb_ref[:, own]
    dkr = jnp.zeros((length, HD), F32)
    dv = jnp.zeros((length, HD), F32)
    gq = jnp.zeros((1, HD), F32)
    for g in range(GROUPS):
        cols = slice((j * GROUPS + g) * HD, (j * GROUPS + g + 1) * HD)
        dqr = []
        for b in range(length // block):
            rows = slice(b * block, (b + 1) * block)
            qr, do = qr_ref[rows, cols], do_ref[rows, cols]
            s = dot_last(qr, kr) * scale
            seen = (tcol[0:1, :] <= trow[rows, 0:1]) & (tcol[1:2, :] == trow[rows, 1:2])
            s = jnp.where(seen, s, MASKED)
            e = jnp.exp(s - jnp.max(s, -1, keepdims=True))
            p = e * (1.0 / jnp.sum(e, -1, keepdims=True))
            dp = dot_last(do, vb)
            ds = (p * (dp - jnp.sum(p * dp, -1, keepdims=True))).astype(BF)
            dqr.append(dot(ds, kr) * scale)
            dkr += dot_first(ds, qr)
            dv += dot_first(p.astype(BF), do)
        dqr = dqr[0] if len(dqr) == 1 else jnp.concatenate(dqr, 0)
        dq, part = head_back(dqr, qkv[:, cols], qg[...], cos2, sin2)
        dqkv[:, cols] = dq.astype(BF)
        gq += part
    at = (nq + j) * HD
    dk, gk = head_back(dkr * scale, qkv[:, at : at + HD], kg[...], cos2, sin2)
    dqkv[:, at : at + HD] = dk.astype(BF)
    at = (nq + nk + j) * HD
    dqkv[:, at : at + HD] = dv.astype(BF)
    return gq, gk


def assemble_kernel(counts, order_ref, *refs):
    n_rows, n_cols = counts
    total = n_rows + n_cols
    mine, other, outs = refs[:total], refs[total : 2 * total], refs[2 * total :]

    def fill(sources):
        for src, out in zip(sources, outs):
            m, places, q, width = src.shape
            for a in range(places):
                out[a * m * q : (a + 1) * m * q, :] = (
                    src[:, a].reshape(m * q, width).astype(F32)
                )

    pl.when(pl.program_id(0) == 0)(lambda: fill(mine))
    pl.when(pl.program_id(0) == 1)(lambda: fill(other))


def assemble(rows, cols, core, owner):
    n = len(owner)
    order = jnp.stack(list(owner) + [core]).astype(jnp.int32)
    in_specs, out_specs, shapes, operands = [[], []], [], [], [[], []]
    size = 0
    for mine, other in rows:
        m, places, q, width = mine.shape
        block = (m, places, q, width // n)
        in_specs[0].append(
            pl.BlockSpec(block, lambda g, b, o: (0, 0, 0, jnp.where(g == 0, b, n - 1)))
        )
        in_specs[1].append(
            pl.BlockSpec(block, lambda g, b, o: (0, 0, 0, jnp.where(g == 0, 0, b)))
        )
        out_specs.append(
            pl.BlockSpec((places * m * q, width // n), lambda g, b, o: (g ^ o[n], b))
        )
        shapes.append(jax.ShapeDtypeStruct((2 * places * m * q, width), F32))
        operands[0].append(mine)
        operands[1].append(other)
        size += mine.size
    for mine, other, at, width in cols:
        m, _, q, _ = mine.shape
        block = (m, 1, q, width)
        in_specs[0].append(
            pl.BlockSpec(block, lambda g, b, o, at=at: (0, o[jnp.where(g == 0, b, n - 1)], 0, at))
        )
        in_specs[1].append(
            pl.BlockSpec(block, lambda g, b, o, at=at: (0, o[jnp.where(g == 0, 0, b)], 0, at))
        )
        out_specs.append(pl.BlockSpec((m * q, width), lambda g, b, o: (g ^ o[n], b)))
        shapes.append(jax.ShapeDtypeStruct((2 * m * q, n * width), F32))
        operands[0].append(mine)
        operands[1].append(other)
        size += m * n * q * width
    return pl.pallas_call(
        partial(assemble_kernel, (len(rows), len(cols))),
        out_shape=tuple(shapes),
        grid_spec=pltpu.PrefetchScalarGridSpec(
            num_scalar_prefetch=1,
            grid=(2, n),
            in_specs=in_specs[0] + in_specs[1],
            out_specs=tuple(out_specs),
        ),
        compiler_params=pltpu.CompilerParams(vmem_limit_bytes=56 << 20),
        cost_estimate=pl.CostEstimate(flops=0, bytes_accessed=12 * size, transcendentals=0),
        name="assemble",
    )(order, *operands[0], *operands[1])


MESH_ID = pl.DeviceIdType.MESH


def back_kernel(n, m, nq, nk, scale, parts, *refs):
    (x_hbm, hidden_hbm, wo_hbm, wd_hbm, qkv_mine, qkv_other, mlp_mine, mlp_other,
     qkv_hbm, qr_hbm, kr_hbm, vb_hbm, o_hbm, normed_hbm, hn_hbm, act_hbm, dy_hbm, dpre_hbm,
     ag, mg, qg, kg, cos2, sin2, trow, tcol,
     output, grad_in, gain_out) = refs[:29]
    mines, others, away_v, fins, refs = refs[29:33], refs[33:37], refs[37:41], refs[41:45], refs[45:]
    (ups, downs, send_v,
     x_v, hidden, wo, qkv, qr, kr, vb, o, normed, hn, act, dy_all, dpre,
     part_s, part_r, out_r, dz_all, do, dqkv, wtile, dtile, gain_ref,
     pair_s, pair_r, up_s, up_r, down_s, down_r,
     peer_s, peer_r, gup_s, gup_r, gdown_s, gdown_r, sib_s, sib_r, own_sem, gain_pair, gain_group,
     gain_line, gain_s, gain_r, in_sem, wt_sem, dhn_s, dhn_r, dz_s, dz_r, dn_s, dn_r, out_ss,
     out_rs) = refs
    rows, width = x_v.shape
    own = width // n
    half = own // 2
    ring = ups.shape[0]
    shard, rep = lax.axis_index("shard"), lax.axis_index("rep")
    i = rep // 2
    core = lax.rem(rep, 2)
    sibling = {"rep": 2 * i + 1 - core}
    above, below = {"rep": rep + 2}, {"rep": rep - 2}
    peers = [None] + [{"shard": shard ^ k} for k in range(1, n)]
    has_up, has_down = i < m - 1, i > 0

    barrier = pltpu.get_barrier_semaphore()

    def greet(dev):
        pl.semaphore_signal(barrier, inc=1, device_id=dev, device_id_type=MESH_ID)

    greet(sibling)
    for k in range(1, n):
        greet(peers[k])
    line = [None] + [{"rep": 2 * lax.rem(i + d, m) + core} for d in range(1, m)]
    for d in range(1, m):
        greet(line[d])

    loads = [
        pltpu.make_async_copy(src, dst, in_sem.at[f])
        for f, (src, dst) in enumerate(
            [
                (act_hbm, act), (dy_hbm, dy_all), (dpre_hbm, dpre), (hn_hbm, hn),
                (hidden_hbm, hidden), (wo_hbm, wo), (qkv_hbm, qkv), (qr_hbm, qr), (kr_hbm, kr),
                (vb_hbm, vb), (o_hbm, o), (normed_hbm, normed), (x_hbm, x_v),
            ]
        )
    ]
    for copy in loads:
        copy.start()
    pl.semaphore_wait(barrier, n + m - 1)

    def remote(src, dst, ssem, rsem, dev):
        return pltpu.make_async_remote_copy(
            src_ref=src, dst_ref=dst, send_sem=ssem, recv_sem=rsem,
            device_id=dev, device_id_type=MESH_ID,
        )

    def cols_of(p):
        return pl.ds(parts[p][3], parts[p][4])

    def chunk(p, j):
        seg, at = parts[p][:2]
        return away_v[seg].at[at, j, :, cols_of(p)]

    def fin(p):
        seg, at = parts[p][:2]
        return fins[seg].at[at, :, cols_of(p)]

    def out(refs, p, j):
        seg, at = parts[p][:2]
        return refs[seg].at[j, at, :, cols_of(p)]

    def pair_copy(p):
        seg, at = parts[p][:2]
        return remote(
            send_v.at[p % 3, :, :, pl.ds(0, parts[p][4])], away_v[seg].at[at, :, :, cols_of(p)],
            pair_s.at[p], pair_r.at[p], sibling,
        )

    def slot(ref, p, t):
        return ref.at[p % ring, t, :, pl.ds(0, parts[p][4])]

    def up_copy(p, t, src):
        return remote(src, slot(ups, p, t), up_s.at[p, t], up_r.at[p, t], above)

    def down_copy(p, t, src):
        return remote(src, slot(downs, p, t), down_s.at[p, t], down_r.at[p, t], below)

    def add_into(ref, other):
        ref[...] = (ref[...].astype(F32) + other[...].astype(F32)).astype(BF)

    def scatter_step(p, t):
        if t > 0:

            @pl.when((i > 0) & (i <= t) & has_up)
            def _():
                up_copy(p, t - 1, slot(ups, p, t - 1)).wait_recv()
                add_into(slot(ups, p, t - 1), chunk(p, m - 1 - t + i))

            @pl.when((i < m - 1) & (i >= m - 1 - t) & has_down)
            def _():
                down_copy(p, t - 1, slot(downs, p, t - 1)).wait_recv()
                add_into(slot(downs, p, t - 1), chunk(p, i - (m - 1 - t)))

            pl.when((i > 0) & (i <= t) & has_up)(
                lambda: up_copy(p, t, slot(ups, p, t - 1)).start()
            )
            pl.when((i < m - 1) & (i >= m - 1 - t) & has_down)(
                lambda: down_copy(p, t, slot(downs, p, t - 1)).start()
            )
        pl.when(i == 0)(lambda: up_copy(p, t, chunk(p, m - 1 - t)).start())
        pl.when(i == m - 1)(lambda: down_copy(p, t, chunk(p, t)).start())

    def peer_copy(p):
        return remote(chunk(p, i), fin(p), peer_s.at[p], peer_r.at[p], peers[parts[p][2]])

    def total(p):
        pl.when(has_down)(lambda: up_copy(p, m - 2, slot(ups, p, m - 2)).wait_recv())
        pl.when(has_up)(lambda: down_copy(p, m - 2, slot(downs, p, m - 2)).wait_recv())
        where = fin(p) if parts[p][2] == 0 else chunk(p, i)

        def put(*extra):
            value = chunk(p, i)[...].astype(F32)
            for e in extra:
                value = value + e[...].astype(F32)
            where[...] = value.astype(BF)

        u, d = slot(ups, p, m - 2), slot(downs, p, m - 2)
        pl.when(has_up & has_down)(lambda: put(u, d))
        pl.when(has_up & (i == 0))(lambda: put(d))
        pl.when(has_down & (i == m - 1))(lambda: put(u))
        if parts[p][2] != 0:
            peer_copy(p).start()

    def gup_copy(p, t, j, src):
        return remote(src, out(mines, p, j), gup_s.at[p, t], gup_r.at[p, t], above)

    def gdown_copy(p, t, j, src):
        return remote(src, out(mines, p, j), gdown_s.at[p, t], gdown_r.at[p, t], below)

    def sib_copy(p, j, src):
        return remote(src, out(others, p, j), sib_s.at[p, j], sib_r.at[p, j], sibling)

    def own_copy(p):
        return pltpu.make_async_copy(fin(p), out(mines, p, i), own_sem.at[p])

    def gather_step(p, t):
        if t == 0:
            for u in range(m - 1):
                pl.when((i <= u) & has_up)(lambda: up_copy(p, u, slot(ups, p, u)).wait_send())
                pl.when((i >= m - 1 - u) & has_down)(
                    lambda: down_copy(p, u, slot(downs, p, u)).wait_send()
                )
            if parts[p][2] != 0:
                peer_copy(p).wait_recv()
            pl.when(has_up)(lambda: gup_copy(p, 0, i, fin(p)).start())
            pl.when(has_down)(lambda: gdown_copy(p, 0, i, fin(p)).start())
            sib_copy(p, i, fin(p)).start()
            own_copy(p).start()
            return

        @pl.when(i - t >= 0)
        def _():
            here = out(mines, p, i - t)
            gup_copy(p, t - 1, i - t, here).wait_recv()
            if t < m - 1:
                pl.when(has_up)(lambda: gup_copy(p, t, i - t, here).start())
            sib_copy(p, i - t, here).start()

        @pl.when(i + t < m)
        def _():
            here = out(mines, p, i + t)
            gdown_copy(p, t - 1, i + t, here).wait_recv()
            if t < m - 1:
                pl.when(has_down)(lambda: gdown_copy(p, t, i + t, here).start())
            sib_copy(p, i + t, here).start()

    def gain_copies(level):
        if level == 0:
            return [remote(gain_ref, gain_pair, gain_s.at[0], gain_r.at[0], sibling)]
        if level == 1:
            return [
                remote(
                    gain_group.at[shard], gain_group.at[shard], gain_s.at[k], gain_r.at[k], peers[k]
                )
                for k in range(1, n)
            ]
        return [
            remote(
                gain_line.at[i], gain_line.at[i], gain_s.at[n - 1 + d], gain_r.at[n - 1 + d], line[d]
            )
            for d in range(1, m)
        ]

    def gains(level):
        if level > 0:
            for copy in gain_copies(level - 1):
                copy.wait_recv()
        if level == 1:
            gain_group[shard] = gain_ref[...] + gain_pair[...]
        elif level == 2:
            value = gain_group[0]
            for k in range(1, n):
                value = value + gain_group[k]
            gain_line[i] = value
        elif level == 3:
            value = gain_line[0]
            for k in range(1, m):
                value = value + gain_line[k]
            gain_out[...] = value
        if level < 3:
            for copy in gain_copies(level):
                copy.start()

    def tiles(cols, first=0):
        step = max(v for v in range(HD, 513, HD) if cols % v == 0)
        return [(c, pl.ds(first + c, step), pl.ds(c, step)) for c in range(0, cols, step)]

    def product(p, h, at):
        seg, place, k = parts[p][:3]
        if seg in (0, 2):
            ref = act if seg == 0 else o
            both = ref.shape[1] // 2
            start = (core if h == 0 else 1 - core) * both + place * half
            left = ref[:, pl.ds(pl.multiple_of(start, half), half)]
            right = (dy_all if seg == 0 else dz_all)[:, :, at].reshape(n * rows, at.size)
        else:
            left = (hn if seg == 1 else normed)[:, (h * n + k) * half : (h * n + k + 1) * half]
            right = (dpre if seg == 1 else dqkv)[:, at]
        return dot_first(left, right).reshape(m, half // m, at.size)

    def send(p):
        if p >= 3:
            pair_copy(p - 3).wait_send()
        for _, at, to in tiles(parts[p][4], parts[p][3]):
            send_v[p % 3, :, :, to] = product(p, 1, at).astype(BF)
        pair_copy(p).start()

    def first(p):
        seg, place = parts[p][:2]
        pair_copy(p).wait_recv()
        for _, at, _ in tiles(parts[p][4], parts[p][3]):
            away_v[seg][place, :, :, at] = (
                product(p, 0, at) + away_v[seg][place, :, :, at].astype(F32)
            ).astype(BF)
        scatter_step(p, 0)

    def dhn_copy(k):
        return remote(part_s.at[k], part_r.at[k - 1], dhn_s.at[k], dhn_r.at[k], peers[k])

    def dn_copy(k):
        return remote(part_s.at[k], part_r.at[k - 1], dn_s.at[k], dn_r.at[k], peers[k])

    def out_copy(k):
        return remote(part_s.at[k], out_r.at[k - 1], out_ss.at[k], out_rs.at[k], peers[k])

    def dz_copy(k):
        return remote(dz_all.at[0], dz_all.at[k], dz_s.at[k], dz_r.at[k], peers[k])

    strip = min(rows, 32)

    def strips(body):
        pl.loop(0, rows // strip)(
            lambda b: body(pl.ds(pl.multiple_of(b * strip, strip), strip))
        )

    def add_gain(at, value):
        for b in range(value.shape[1] // HD):
            gain_ref[at + b : at + b + 1, :] += value[:, b * HD : (b + 1) * HD]

    def norm_back(values, gain, at, result):
        def body(r):
            v = values[r, :].astype(F32)
            rstat = lax.rsqrt(jnp.mean(v * v, -1, keepdims=True) + EPSILON)
            scaled = v * rstat
            grad = part_s[0, r, :].astype(F32)
            for k in range(1, n):
                grad = grad + part_r[k - 1, r, :].astype(F32)
            add_gain(at, jnp.sum(grad * scaled, 0, keepdims=True))
            weighted = grad * gain[...]
            result(
                r, rstat * (weighted - scaled * jnp.mean(weighted * scaled, -1, keepdims=True))
            )

        strips(body)

    def partial_rows(grads, mine, other, turn):
        cols = grads.shape[1]

        def tile_copy(b):
            src = (mine if b < n else other).at[b % n]
            return pltpu.make_async_copy(
                src, wtile.at[b % 2, :, :, pl.ds(0, cols)], wt_sem.at[b % 2]
            )

        if turn == 0:
            tile_copy(0).start()
        for b in (2 * turn, 2 * turn + 1):
            tile_copy(b).wait()
            if b + 1 < 2 * n:
                tile_copy(b + 1).start()
            h, kk = b // n, b % n
            at = pl.ds(
                pl.multiple_of((shard ^ kk) * own + (core if h == 0 else 1 - core) * half, half),
                half,
            )
            w = wtile[b % 2, :, :, :cols].reshape(half, cols)
            for k in range(n):
                part_s[k, :, at] = dot_last(grads[k * rows : (k + 1) * rows, :], w).astype(BF)

    def hook_dhn(turn):
        if turn == 0:
            loads[2].wait()
        partial_rows(dpre, mlp_mine, mlp_other, turn)
        if turn == n - 1:
            for k in range(1, n):
                dhn_copy(k).start()

    def hook_hidden():
        loads[4].wait()
        for k in range(1, n):
            dhn_copy(k).wait_recv()
        gain_ref[...] = jnp.zeros_like(gain_ref)

        def result(r, value):
            value = dy_all[0, r, :].astype(F32) + value
            grad_in[r, :] = value
            dz_all[0, r, :] = value.astype(BF)

        norm_back(hidden, mg, width // HD, result)
        for k in range(1, n):
            dz_copy(k).start()

    def hook_do():
        for copy in loads[5:]:
            copy.wait()
        for k in range(n):
            if k > 0:
                dz_copy(k).wait_recv()
            do[k * rows : (k + 1) * rows, :] = dot_last(dz_all[k], wo[...]).astype(BF)

    def hook_head(j):
        gq, gk = attend_back_pair(
            j, nq, nk, qkv, qr, kr, vb, do, dqkv, qg, kg, cos2, sin2, trow, tcol, scale
        )
        add_gain(2 * width // HD, gq)
        add_gain(2 * width // HD + 1, gk)

    def hook_normed(turn):
        if turn == 0:
            for k in range(1, n):
                out_copy(k).wait_send()
        partial_rows(dqkv, qkv_mine, qkv_other, turn)
        if turn == n - 1:
            for k in range(1, n):
                dn_copy(k).start()

    def hook_input():
        for k in range(1, n):
            dn_copy(k).wait_recv()

        def result(r, value):
            grad_in[r, :] = grad_in[r, :] + value

        norm_back(x_v, ag, 0, result)

    def hook_down(turn):
        if turn == 0:
            for k in range(1, n):
                dhn_copy(k).wait_send()
        step = dtile.shape[2]

        def tile_copy(b):
            return pltpu.make_async_copy(
                wd_hbm.at[:, pl.ds(b * step, step)], dtile.at[b % 2], wt_sem.at[b % 2]
            )

        count = width // step
        if turn == 0:
            tile_copy(0).start()
        for b in range(turn * count // 2, (turn + 1) * count // 2):
            tile_copy(b).wait()
            if b + 1 < count:
                tile_copy(b + 1).start()
            for k in range(n):
                part_s[k, :, b * step : (b + 1) * step] = dot(
                    act[k * rows : (k + 1) * rows, :], dtile[b % 2]
                ).astype(BF)
        if turn == 1:
            for k in range(1, n):
                out_copy(k).start()

    def hook_output():
        for k in range(1, n):
            out_copy(k).wait_recv()

        def body(r):
            value = hidden[r, :] + part_s[0, r, :].astype(F32)
            for k in range(1, n):
                value = value + out_r[k - 1, r, :].astype(F32)
            output[r, :] = value.astype(BF)

        strips(body)

    at_tick = {}
    def plan(tick, *pieces):
        for f, piece in enumerate(pieces):
            at_tick.setdefault(tick + f, []).append(piece)

    plan(DHN_TICK, *[partial(hook_dhn, turn) for turn in range(n)])
    tick = DHN_TICK + n + 2
    plan(tick, hook_hidden, partial(hook_down, 0), partial(hook_down, 1), hook_do)
    tick += 4
    plan(tick, *[partial(hook_head, j) for j in range(nk)])
    plan(tick + nk, hook_output, *[partial(hook_normed, turn) for turn in range(n)])
    tick += nk + n + 3
    plan(tick, hook_input, *[partial(gains, level) for level in range(4)])

    stages = [first] + [lambda p, t=t: scatter_step(p, t) for t in range(1, m - 1)]
    stages += [total] + [lambda p, t=t: gather_step(p, t) for t in range(m)]

    loads[0].wait()
    loads[1].wait()
    send(0)
    send(1)
    ticks = len(parts) + len(stages) - 1
    for tick in range(max(ticks, max(at_tick) + 1)):
        if tick == 0:
            loads[3].wait()
        for st in range(len(stages) - 1, -1, -1):
            p = tick - st
            if 0 <= p < len(parts):
                stages[st](p)
        for hook in at_tick.get(tick, []):
            hook()
        if tick + 2 < len(parts):
            send(tick + 2)

    for k in range(1, n):
        dz_copy(k).wait_send()
        dn_copy(k).wait_send()
    for level in range(3):
        for copy in gain_copies(level):
            copy.wait_send()
    for p in range(len(parts)):
        if p >= len(parts) - 3:
            pair_copy(p).wait_send()
        if parts[p][2] != 0:
            peer_copy(p).wait_send()
        own_copy(p).wait()
        for t in range(m - 1):
            pl.when((i - t >= 0) & has_up)(lambda: gup_copy(p, t, i, fin(p)).wait_send())
            pl.when((i + t < m) & has_down)(lambda: gdown_copy(p, t, i, fin(p)).wait_send())
        for j in range(m):
            copy = sib_copy(p, j, fin(p))
            copy.wait_send()
            copy.wait_recv()


def back(n, m, nq, nk, x, hidden, wo, wd, weights, qkv, heads, o, normed, hn, act, dy_all, dpre,
         gains, tables):
    rows, width = x.shape
    length = n * rows
    q, cols = weights[0].shape[2:]
    wide = dpre.shape[1]
    half = m * q
    dma = pltpu.SemaphoreType.DMA
    sd = jax.ShapeDtypeStruct
    hbm, vmem = pl.BlockSpec(memory_space=pl.ANY), pl.BlockSpec(memory_space=pltpu.VMEM)
    segments = [
        (act.shape[1] // 2 // half, m, q, width), (n, m, q, wide),
        (nq * HD // 2 // half, m, q, width), (n, m, q, cols),
    ]

    def cut(seg, at, k, sizes):
        out, c = [], 0
        for size in sizes:
            out.append((seg, at, k, c, size))
            c += size
        return out

    parts = cut(0, 0, 0, [width // 4, width // 4, width // 2])
    for a in range(1, segments[0][0]):
        parts += cut(0, a, 0, [width // 2] * 2)
    for k in range(n):
        parts += cut(1, k, k, [wide // 2] * 2)
    for a in range(segments[2][0]):
        parts += cut(2, a, 0, [width // 2] * 2)
    for k in range(n):
        parts += cut(3, k, k, [cols] if k < n - 1 else [cols // 2] * 2)
    total = len(parts)
    most = max(part[4] for part in parts)
    ring = m + 2
    count = 2 * width // HD + 2
    gain_shape = (count + -count % 8, HD)
    outs = [sd((m, v[0]) + v[2:], BF) for v in segments]
    like = lambda v: pltpu.VMEM(v.shape, v.dtype)
    operands = [x, hidden, wo, wd, *weights, qkv, *heads, o, normed, hn, act, dy_all, dpre]
    return pl.pallas_call(
        partial(back_kernel, n, m, nq, nk, 1.0 / math.sqrt(HD), parts),
        out_shape=tuple(
            [sd((rows, width), BF), sd((rows, width), F32), sd(gain_shape, F32)] + outs + outs
        ),
        in_specs=[hbm] * len(operands) + [vmem] * 8,
        out_specs=tuple([vmem] * 3 + [hbm] * 8),
        scratch_shapes=[pltpu.VMEM(v, BF) for v in segments]
        + [pltpu.VMEM(v[:1] + v[2:], BF) for v in segments]
        + [pltpu.VMEM((ring, m - 1, q, most), BF)] * 2
        + [pltpu.VMEM((3, m, q, most), BF)]
        + [like(v) for v in (x, hidden, wo, qkv, *heads, o, normed, hn, act, dy_all, dpre)]
        + [
            pltpu.VMEM((n, rows, width), BF), pltpu.VMEM((n - 1, rows, width), BF),
            pltpu.VMEM((n - 1, rows, width), BF), pltpu.VMEM((n, rows, width), BF),
            pltpu.VMEM((length, nq * HD), BF), pltpu.VMEM((length, cols), BF),
            pltpu.VMEM((2, m, q, wide), BF), pltpu.VMEM((2, wd.shape[0], 256), BF),
            pltpu.VMEM(gain_shape, F32),
            dma((total,)), dma((total,)),
            dma((total, m - 1)), dma((total, m - 1)), dma((total, m - 1)), dma((total, m - 1)),
            dma((total,)), dma((total,)),
            dma((total, m - 1)), dma((total, m - 1)), dma((total, m - 1)), dma((total, m - 1)),
            dma((total, m)), dma((total, m)), dma((total,)),
            pltpu.VMEM(gain_shape, F32), pltpu.VMEM((n,) + gain_shape, F32),
            pltpu.VMEM((m,) + gain_shape, F32), dma((n + m,)), dma((n + m,)),
            dma((13,)), dma((2,)),
        ]
        + [dma((n,))] * 8,
        compiler_params=pltpu.CompilerParams(
            collective_id=3, has_side_effects=True, vmem_limit_bytes=67043328
        ),
        name="back",
    )(*operands, *gains, *tables)


def front_kernel(
    n, m, nq, nk, scale,
    x_hbm, dy_hbm, wq, wk, wv, wg, wu, wo_hbm,
    ag, qg, kg, mg, cos2, sin2, trow, tcol,
    normed_hbm, qkv_hbm, qr_hbm, kr_hbm, vb_hbm, o_hbm, hidden_hbm, hn_hbm,
    qkv_mine_hbm, qkv_other_hbm, mlp_mine, mlp_other, dy_all,
    normed, qkv, qr, kr, vb, o, hidden, hn, qkv_mine, qkv_other,
    x_all, wo, bounce, dy_v, hn_all, part_own, part_s, part_r,
    x_ss, x_rs, w_ss, w_rs, up_ss, up_rs, down_ss, down_rs, sib_ss, sib_rs,
    own_sem, back_sem, load_sem, part_ss, part_rs, hn_ss, hn_rs, dy_ss, dy_rs, store_sem
):
    shard, rep = lax.axis_index("shard"), lax.axis_index("rep")
    i = rep // 2
    core = lax.rem(rep, 2)
    sibling = {"rep": 2 * i + 1 - core}
    above, below = {"rep": rep + 2}, {"rep": rep - 2}
    peers = [None] + [{"shard": shard ^ k} for k in range(1, n)]
    has_up, has_down = i < m - 1, i > 0
    rows, width = x_all.shape[1], x_all.shape[2]
    own = width // n
    half = own // 2

    barrier = pltpu.get_barrier_semaphore()

    def greet(dev):
        pl.semaphore_signal(barrier, inc=1, device_id=dev, device_id_type=MESH_ID)

    greet(sibling)
    for k in range(1, n):
        greet(peers[k])
    for d in range(1, m):
        greet({"rep": 2 * lax.rem(i + d, m) + core})
    pl.semaphore_wait(barrier, n + m - 1)

    def remote(src, dst, ssem, rsem, dev):
        return pltpu.make_async_remote_copy(
            src_ref=src, dst_ref=dst, send_sem=ssem, recv_sem=rsem,
            device_id=dev, device_id_type=MESH_ID,
        )

    results = [
        (normed, normed_hbm), (qkv_mine, qkv_mine_hbm), (qkv_other, qkv_other_hbm),
        (qkv, qkv_hbm), (qr, qr_hbm), (kr, kr_hbm), (vb, vb_hbm), (o, o_hbm), (hidden, hidden_hbm),
    ] + [(hn.at[pl.ds(k * rows, rows)], hn_hbm.at[pl.ds(k * rows, rows)]) for k in range(n)]
    stores = [
        pltpu.make_async_copy(src, dst, store_sem.at[f]) for f, (src, dst) in enumerate(results)
    ]

    ffl = wg.shape[3] // n
    groups = [
        ([wq, wk, wv], qkv_mine, qkv_other, 0, qkv.shape[1]),
        ([wg], mlp_mine, mlp_other, 0, ffl),
        ([wu], mlp_mine, mlp_other, ffl, ffl),
    ]

    def fields(g):
        weights, _, _, at, _ = groups[g]
        for w in weights:
            size = w.shape[3] // n
            yield w, at, size
            at += size

    def cols_of(k, size):
        return pl.ds(pl.multiple_of((shard ^ k) * size, size), size)

    def piece_copies(g, k):
        mine = groups[g][1]
        return [
            remote(
                w.at[core, i, :, cols_of(k, size)],
                mine.at[k, i, :, pl.ds(at, size)],
                w_ss.at[g, k, f], w_rs.at[g, k, f], peers[k],
            )
            for f, (w, at, size) in enumerate(fields(g))
        ]

    def own_copies(g):
        mine, other = groups[g][1:3]
        out = []
        for h, dst in enumerate((mine, other)):
            for f, (w, at, size) in enumerate(fields(g)):
                to = dst.at[0, :, :, pl.ds(at, size)] if g == 0 else bounce.at[h, :, :, pl.ds(at, size)]
                src = w.at[core if h == 0 else 1 - core, :, :, cols_of(0, size)]
                out.append(pltpu.make_async_copy(src, to, own_sem.at[g, h, f]))
        return out

    def back_copies():
        return [
            pltpu.make_async_copy(bounce.at[h], dst.at[0], back_sem.at[h])
            for h, dst in enumerate((mlp_mine, mlp_other))
        ]

    def region(g, ref, j):
        at, size = groups[g][3:]
        return ref.at[pl.ds(1, n - 1), j, :, pl.ds(at, size)]

    def up_copy(g, t, j):
        r = region(g, groups[g][1], j)
        return remote(r, r, up_ss.at[g, t], up_rs.at[g, t], above)

    def down_copy(g, t, j):
        r = region(g, groups[g][1], j)
        return remote(r, r, down_ss.at[g, t], down_rs.at[g, t], below)

    def sib_copy(g, j):
        mine, other = groups[g][1:3]
        return remote(region(g, mine, j), region(g, other, j), sib_ss.at[g, j], sib_rs.at[g, j], sibling)

    def gather_weights(g, t):
        if t == 0:
            for k in range(1, n):
                for copy in piece_copies(g, k):
                    copy.wait_recv()
            pl.when(has_up)(lambda: up_copy(g, 0, i).start())
            pl.when(has_down)(lambda: down_copy(g, 0, i).start())
            sib_copy(g, i).start()
            return

        @pl.when(i - t >= 0)
        def _():
            up_copy(g, t - 1, i - t).wait_recv()
            if t < m - 1:
                pl.when(has_up)(lambda: up_copy(g, t, i - t).start())
            sib_copy(g, i - t).start()

        @pl.when(i + t < m)
        def _():
            down_copy(g, t - 1, i + t).wait_recv()
            if t < m - 1:
                pl.when(has_down)(lambda: down_copy(g, t, i + t).start())
            sib_copy(g, i + t).start()

    def x_copy(k):
        return remote(x_hbm, x_all.at[k], x_ss.at[k], x_rs.at[k], peers[k])

    def dy_copy(k):
        return remote(dy_hbm, dy_all.at[k], dy_ss.at[k], dy_rs.at[k], peers[k])

    def hn_copy(k):
        return remote(hn_all.at[0], hn_all.at[k], hn_ss.at[k], hn_rs.at[k], peers[k])

    def part_copy(k):
        return remote(part_s.at[k], part_r.at[k], part_ss.at[k], part_rs.at[k], peers[k])

    load_x = pltpu.make_async_copy(x_hbm, x_all.at[0], load_sem.at[0])
    load_wo = pltpu.make_async_copy(wo_hbm, wo, load_sem.at[1])
    load_dy = pltpu.make_async_copy(dy_hbm, dy_v, load_sem.at[2])
    keep_dy = pltpu.make_async_copy(dy_v, dy_all.at[0], load_sem.at[3])

    def start_pieces(g):
        for k in range(1, n):
            for copy in piece_copies(g, k):
                copy.start()

    load_x.start()
    start_pieces(0)
    start_pieces(1)
    for k in range(1, n):
        x_copy(k).start()
    for copy in own_copies(0):
        copy.start()
    start_pieces(2)
    for k in range(1, n):
        dy_copy(k).start()
    load_wo.start()
    for g in (1, 2):
        for copy in own_copies(g):
            copy.start()
    load_dy.start()

    def place(k, h, kk):
        return pl.ds(
            pl.multiple_of((shard ^ kk) * own + (core if h == 0 else 1 - core) * half, half), half
        )

    hops = [(1, t) for t in range(1, m)] + [(2, t) for t in range(m)]
    hops.sort(key=lambda v: 2 * v[1] + v[0])

    def next_hops(count):
        for _ in range(min(count, len(hops))):
            gather_weights(*hops.pop(0))

    gather_weights(0, 0)
    for k in range(n):
        if k == 0:
            load_x.wait()
        else:
            x_copy(k).wait_recv()
        v = x_all[k].astype(F32)
        r = lax.rsqrt(jnp.mean(v * v, -1, keepdims=True) + EPSILON)
        for h in range(2):
            for kk in range(n):
                at = place(k, h, kk)
                normed[k * rows : (k + 1) * rows, (h * n + kk) * half : (h * n + kk + 1) * half] = (
                    x_all[k, :, at].astype(F32) * r * ag[:, at]
                ).astype(BF)
        if k + 1 < m - 1:
            gather_weights(0, k + 1)
        if k == min(n, m - 1) - 1:
            gather_weights(1, 0)
    for t in range(n + 1, m - 1):
        gather_weights(0, t)
    stores[0].start()
    gather_weights(0, m - 1)
    for copy in own_copies(0):
        copy.wait()
    for j in range(m):
        sib_copy(0, j).wait_recv()
    stores[1].start()
    stores[2].start()

    cols = qkv.shape[1]
    step = min(cols, 256)

    @pl.loop(0, cols // step)
    def _(b):
        at = pl.ds(pl.multiple_of(b * step, step), step)
        both = n * half
        qkv[:, at] = dot(
            normed[:, :both], qkv_mine[:, :, :, at].reshape(both, step)
        ) + dot(normed[:, both:], qkv_other[:, :, :, at].reshape(both, step))

    stores[3].start()
    for g in (1, 2):
        for copy in own_copies(g):
            copy.wait()
    for copy in back_copies():
        copy.start()
    load_dy.wait()
    keep_dy.start()
    for j in range(nk):
        attend_pair(qkv, j, nq, nk, qg, kg, cos2, sin2, trow, tcol, o, qr, kr, vb, scale)
        if j == 0:
            next_hops(2)
    for f in range(4, 8):
        stores[f].start()

    load_wo.wait()
    step = min(width, 512)

    @pl.loop(0, width // step)
    def _(b):
        at = pl.ds(pl.multiple_of(b * step, step), step)
        for k in range(n):
            value = dot(o[k * rows : (k + 1) * rows, :], wo[:, at])
            if k == 0:
                part_own[:, at] = value
            else:
                part_s[k, :, at] = value.astype(BF)

    for k in range(1, n):
        part_copy(k).start()
    next_hops(2)
    total = x_all[0].astype(F32) + part_own[...]
    for k in range(1, n):
        part_copy(k).wait_recv()
        total = total + part_r[k].astype(F32)
    hidden[...] = total
    stores[8].start()
    r = lax.rsqrt(jnp.mean(total * total, -1, keepdims=True) + EPSILON)
    hn_all[0] = (total * r * mg[...]).astype(BF)
    for k in range(1, n):
        hn_copy(k).start()
    next_hops(len(hops) - 1)
    for k in range(n):
        if k > 0:
            hn_copy(k).wait_recv()
        for h in range(2):
            for kk in range(n):
                hn[k * rows : (k + 1) * rows, (h * n + kk) * half : (h * n + kk + 1) * half] = (
                    hn_all[k, :, place(k, h, kk)]
                )
        stores[9 + k].start()
    next_hops(len(hops))

    for copy in back_copies() + stores:
        copy.wait()
    keep_dy.wait()
    for k in range(1, n):
        for g in range(3):
            for copy in piece_copies(g, k):
                copy.wait_send()
        x_copy(k).wait_send()
        part_copy(k).wait_send()
        hn_copy(k).wait_send()
        dy_copy(k).wait_send()
        dy_copy(k).wait_recv()
    for g in range(3):
        for j in range(m):
            sib_copy(g, j).wait_send()
            if g > 0:
                sib_copy(g, j).wait_recv()
        for t in range(m - 1):
            pl.when((i - t >= 0) & has_up)(lambda: up_copy(g, t, i).wait_send())
            pl.when((i + t < m) & has_down)(lambda: down_copy(g, t, i).wait_send())


def front(n, m, nq, nk, x, dy, weights, wo, gains, tables):
    rows, width = x.shape
    length = n * rows
    q = weights[0].shape[2]
    cols = [sum(w.shape[3] // n for w in ws) for ws in (weights[:3], weights[3:])]
    vmem, hbm = pl.BlockSpec(memory_space=pltpu.VMEM), pl.BlockSpec(memory_space=pl.ANY)
    dma = pltpu.SemaphoreType.DMA
    sd = jax.ShapeDtypeStruct
    outs = [
        sd((length, width), BF),
        sd((length, cols[0]), F32),
        sd((length, nq * HD), BF),
        sd((length, nk * HD), BF),
        sd((length, nk * HD), BF),
        sd((length, nq * HD), BF),
        sd((rows, width), F32),
        sd((length, width), BF),
        sd((n, m, q, cols[0]), BF),
        sd((n, m, q, cols[0]), BF),
        sd((n, m, q, cols[1]), BF),
        sd((n, m, q, cols[1]), BF),
        sd((n, rows, width), BF),
    ]
    return pl.pallas_call(
        partial(front_kernel, n, m, nq, nk, 1.0 / math.sqrt(HD)),
        out_shape=tuple(outs),
        in_specs=[hbm] * 8 + [vmem] * 8,
        out_specs=tuple([hbm] * len(outs)),
        scratch_shapes=[pltpu.VMEM(v.shape, v.dtype) for v in outs[:10]]
        + [
            pltpu.VMEM((n, rows, width), BF),
            pltpu.VMEM(wo.shape, BF),
            pltpu.VMEM((2, m, q, cols[1]), BF),
            pltpu.VMEM((rows, width), BF),
            pltpu.VMEM((n, rows, width), BF),
            pltpu.VMEM((rows, width), F32),
            pltpu.VMEM((n, rows, width), BF),
            pltpu.VMEM((n, rows, width), BF),
            dma((n,)), dma((n,)),
            dma((3, n, 3)), dma((3, n, 3)),
            dma((3, m)), dma((3, m)), dma((3, m)), dma((3, m)), dma((3, m)), dma((3, m)),
            dma((3, 2, 3)), dma((2,)), dma((4,)),
            dma((n,)), dma((n,)), dma((n,)), dma((n,)), dma((n,)), dma((n,)), dma((9 + n,)),
        ],
        compiler_params=pltpu.CompilerParams(
            collective_id=1, has_side_effects=True, vmem_limit_bytes=60 << 20
        ),
        name="front",
    )(x, dy, *weights, wo, *gains, *tables)


def build(n, reps):
    m = reps // 2

    def per_device(
        activations, segments, attn_gain, query_weight, key_weight, value_weight,
        query_gain, key_gain, out_weight, mlp_gain, gate_weight, up_weight, down_weight,
        cotangent,
    ):
        rows, width = activations.shape[1], activations.shape[2]
        length = segments.shape[1]
        shard = lax.axis_index("shard")
        core = lax.axis_index("rep") % 2
        own = width // n
        half = own // 2
        nq, nk = HQ // n, HK // n
        ffl = FF // n
        owner = [shard ^ k for k in range(n)]

        def cut(v, start, size, axis):
            return lax.dynamic_slice_in_dim(v, start, size, axis)

        def times(v, w):
            both = v.shape[1] // 2
            return dot(v[:, :both], w[0]) + dot(v[:, both:], w[1])

        seg_ids = segments[0]
        pos = positions(seg_ids)
        tokens = jnp.arange(length, dtype=jnp.int32)
        shuffle = lambda v: jnp.concatenate([cut(v, owner[k] * rows, rows, 0) for k in range(n)])
        index, seg_ids, pos = shuffle(tokens), shuffle(seg_ids), shuffle(pos)
        inv_freq = 1.0 / ROPE_BASE ** (jnp.arange(HD // 2, dtype=F32) * (2.0 / HD))
        angles = pos[:, None] * inv_freq[None, :]
        cosine, sine = jnp.cos(angles), jnp.sin(angles)
        cos2 = jnp.concatenate([cosine, cosine], 1)
        sin2 = jnp.concatenate([-sine, sine], 1)
        tcol = jnp.stack([index, seg_ids], 0)
        trow = jnp.stack([index, seg_ids], 1)
        qg, kg = query_gain[None], key_gain[None]

        cut_rows = lambda w: w.reshape(2, m, half // m, w.shape[1])
        (
            normed, qkv, qr, kr, vb, attn_out, hidden, normed_mlp,
            qkv_mine, qkv_other, mlp_mine, mlp_other, all_grads,
        ) = front(
            n, m, nq, nk, activations[0], cotangent[0],
            [cut_rows(w) for w in (query_weight, key_weight, value_weight, gate_weight, up_weight)],
            out_weight,
            [attn_gain[None], qg, kg, mlp_gain[None]],
            [cos2, sin2, trow, tcol],
        )
        w_mlp = [v.reshape(n * half, -1) for v in (mlp_mine, mlp_other)]
        flat_grads = all_grads.reshape(length, width)
        pre = times(normed_mlp, w_mlp)
        gate_pre, up_pre = pre[:, :ffl], pre[:, ffl:]
        sig = jax.nn.sigmoid(gate_pre)
        activated = (gate_pre * sig * up_pre).astype(BF)
        grad_act = dot_last(flat_grads, down_weight)
        grad_gate = (grad_act * up_pre * sig * (1.0 + gate_pre * (1.0 - sig))).astype(BF)
        grad_up = (grad_act * gate_pre * sig).astype(BF)
        grad_pre = jnp.concatenate([grad_gate, grad_up], 1)
        output, grad_input, gains, *summed = back(
            n, m, nq, nk, activations[0], hidden, out_weight, down_weight,
            [qkv_mine, qkv_other, mlp_mine, mlp_other], qkv, [qr, kr, vb], attn_out, normed,
            normed_mlp, activated, all_grads, grad_pre,
            [attn_gain[None], mlp_gain[None], qg, kg], [cos2, sin2, trow, tcol],
        )
        output, grad_input = output[None], grad_input[None]
        mines, others = summed[:4], summed[4:]

        pick = lambda seg, at=None, width=None: (
            (mines[seg], others[seg]) if at is None else (mines[seg], others[seg], at, width)
        )
        (
            grad_down, grad_out_weight, grad_gate_weight, grad_up_weight,
            grad_query_weight, grad_key_weight, grad_value_weight,
        ) = assemble(
            [pick(0), pick(2)],
            [
                pick(1, 0, ffl), pick(1, 1, ffl), pick(3, 0, nq * HD),
                pick(3, nq // nk, nk * HD), pick(3, nq // nk + 1, nk * HD),
            ],
            core,
            owner,
        )
        gains = gains.reshape(-1)
        grad_attn_gain, grad_mlp_gain = gains[:width], gains[width : 2 * width]
        grad_query_gain = gains[2 * width : 2 * width + HD]
        grad_key_gain = gains[2 * width + HD : 2 * width + 2 * HD]
        return (
            output,
            grad_input,
            grad_attn_gain,
            grad_query_weight,
            grad_key_weight,
            grad_value_weight,
            grad_query_gain,
            grad_key_gain,
            grad_out_weight,
            grad_mlp_gain,
            grad_gate_weight,
            grad_up_weight,
            grad_down,
        )

    return per_device


def solution(mesh):
    tok = P("rep", "shard", None)
    row = P("shard", None)
    return jax.shard_map(
        build(mesh.shape["shard"], mesh.shape["rep"]),
        mesh=mesh,
        in_specs=(
            tok, P("rep", None), P(), row, row, row, P(), P(), row, P(), row, row, row, tok,
        ),
        out_specs=(tok, tok, P(), row, row, row, P(), P(), row, P(), row, row, row),
        check_vma=False,
    )
```

```python
from functools import partial
import math

import jax
import jax.numpy as jnp
from jax import lax
from jax.experimental import pallas as pl
from jax.experimental.pallas import tpu as pltpu
from jax.sharding import PartitionSpec as P

HQ = 16
HK = 8
HD = 128
FF = 6144
GROUPS = HQ // HK

EPSILON = 1e-06
ROPE_BASE = 1000000.0
MASKED = -1e30
BF = jnp.bfloat16
F32 = jnp.float32

DHN_TICK = 2


def dot(a, b):
    return jnp.dot(a, b, preferred_element_type=F32)


def dot_last(a, b):
    return lax.dot_general(a, b, (((1,), (1,)), ((), ())), preferred_element_type=F32)


def dot_first(a, b):
    return lax.dot_general(a, b, (((0,), (0,)), ((), ())), preferred_element_type=F32)


def positions(seg_ids):
    token_index = jnp.arange(seg_ids.shape[0], dtype=jnp.int32)
    before = jnp.concatenate([jnp.full((1,), -1, jnp.int32), seg_ids[:-1]])
    starts = lax.cummax(
        jnp.where(seg_ids != before, token_index, jnp.zeros_like(token_index)), axis=0
    )
    return (token_index - starts).astype(F32)


def head_rope(raw, gain, cos2, sin2):
    rstat = lax.rsqrt(jnp.mean(raw * raw, -1, keepdims=True) + EPSILON)
    scaled = raw * rstat * gain
    return scaled * cos2 + pltpu.roll(scaled, HD // 2, 1) * sin2


def attend_pair(qkv, j, nq, nk, qg, kg, cos2, sin2, trow, tcol, o_ref, qr_ref, kr_ref, vb_ref, scale):
    length = qkv.shape[0]
    block = min(length, 256)
    own = slice(j * HD, (j + 1) * HD)
    at = (nq + j) * HD
    kr = head_rope(qkv[:, at : at + HD], kg[...], cos2[...], sin2[...]).astype(BF)
    at = (nq + nk + j) * HD
    vb = qkv[:, at : at + HD].astype(BF)
    kr_ref[:, own] = kr
    vb_ref[:, own] = vb

    @pl.loop(0, GROUPS)
    def _(g):
        cols = pl.ds(pl.multiple_of((j * GROUPS + g) * HD, HD), HD)
        qr_ref[:, cols] = head_rope(qkv[:, cols], qg[...], cos2[...], sin2[...]).astype(BF)

        @pl.loop(0, length // block)
        def _(b):
            rows = pl.ds(pl.multiple_of(b * block, block), block)
            s = dot_last(qr_ref[rows, cols], kr_ref[:, own]) * scale
            at = trow[rows, :]
            seen = (tcol[0:1, :] <= at[:, 0:1]) & (tcol[1:2, :] == at[:, 1:2])
            s = jnp.where(seen, s, MASKED)
            e = jnp.exp(s - jnp.max(s, -1, keepdims=True))
            p = (e * (1.0 / jnp.sum(e, -1, keepdims=True))).astype(BF)
            o_ref[rows, cols] = dot(p, vb_ref[:, own]).astype(BF)


def head_back(grad_rot, raw, gain, cos2, sin2):
    back = grad_rot * cos2 - pltpu.roll(grad_rot, HD // 2, 1) * sin2
    rstat = lax.rsqrt(jnp.mean(raw * raw, -1, keepdims=True) + EPSILON)
    scaled = raw * rstat
    gain_part = jnp.sum(back * scaled, 0, keepdims=True)
    b = back * gain
    return rstat * (b - scaled * jnp.mean(b * scaled, -1, keepdims=True)), gain_part


def attend_back_pair(
    j, nq, nk, qkv, qr_ref, kr_ref, vb_ref, do_ref, dqkv, qg, kg, cos_ref, sin_ref, trow, tcol, scale,
    sums, add_gain
):
    own = slice(j * HD, (j + 1) * HD)
    length = qkv.shape[0]
    block = min(length, 256)
    sums[1] = jnp.zeros((length, HD), F32)
    sums[2] = jnp.zeros((length, HD), F32)

    @pl.loop(0, GROUPS)
    def _(g):
        cols = pl.ds(pl.multiple_of((j * GROUPS + g) * HD, HD), HD)

        @pl.loop(0, length // block)
        def _(b):
            rows = pl.ds(pl.multiple_of(b * block, block), block)
            kr = kr_ref[:, own]
            qr, do = qr_ref[rows, cols], do_ref[rows, cols]
            s = dot_last(qr, kr) * scale
            at = trow[rows, :]
            seen = (tcol[0:1, :] <= at[:, 0:1]) & (tcol[1:2, :] == at[:, 1:2])
            s = jnp.where(seen, s, MASKED)
            e = jnp.exp(s - jnp.max(s, -1, keepdims=True))
            p = e * (1.0 / jnp.sum(e, -1, keepdims=True))
            dp = dot_last(do, vb_ref[:, own])
            ds = (p * (dp - jnp.sum(p * dp, -1, keepdims=True))).astype(BF)
            sums[0, rows, :] = dot(ds, kr) * scale
            sums[1] += dot_first(ds, qr)
            sums[2] += dot_first(p.astype(BF), do)

        dq, part = head_back(sums[0], qkv[:, cols], qg[...], cos_ref[...], sin_ref[...])
        dqkv[:, cols] = dq.astype(BF)
        add_gain(0, part)

    at = (nq + j) * HD
    dk, part = head_back(
        sums[1] * scale, qkv[:, at : at + HD], kg[...], cos_ref[...], sin_ref[...]
    )
    dqkv[:, at : at + HD] = dk.astype(BF)
    add_gain(1, part)
    at = (nq + nk + j) * HD
    dqkv[:, at : at + HD] = sums[2].astype(BF)


def assemble_kernel(counts, order_ref, *refs):
    n_rows, n_cols = counts
    total = n_rows + n_cols
    mine, other, outs = refs[:total], refs[total : 2 * total], refs[2 * total :]

    def fill(sources):
        for src, out in zip(sources, outs):
            m, places, q, width = src.shape
            for a in range(places):
                out[a * m * q : (a + 1) * m * q, :] = (
                    src[:, a].reshape(m * q, width).astype(F32)
                )

    pl.when(pl.program_id(0) == 0)(lambda: fill(mine))
    pl.when(pl.program_id(0) == 1)(lambda: fill(other))


def assemble(rows, cols, core, owner):
    n = len(owner)
    order = jnp.stack(list(owner) + [core]).astype(jnp.int32)
    in_specs, out_specs, shapes, operands = [[], []], [], [], [[], []]
    size = 0
    for mine, other in rows:
        m, places, q, width = mine.shape
        block = (m, places, q, width // n)
        in_specs[0].append(
            pl.BlockSpec(block, lambda g, b, o: (0, 0, 0, jnp.where(g == 0, b, n - 1)))
        )
        in_specs[1].append(
            pl.BlockSpec(block, lambda g, b, o: (0, 0, 0, jnp.where(g == 0, 0, b)))
        )
        out_specs.append(
            pl.BlockSpec((places * m * q, width // n), lambda g, b, o: (g ^ o[n], b))
        )
        shapes.append(jax.ShapeDtypeStruct((2 * places * m * q, width), F32))
        operands[0].append(mine)
        operands[1].append(other)
        size += mine.size
    for mine, other, at, width in cols:
        m, _, q, _ = mine.shape
        block = (m, 1, q, width)
        in_specs[0].append(
            pl.BlockSpec(block, lambda g, b, o, at=at: (0, o[jnp.where(g == 0, b, n - 1)], 0, at))
        )
        in_specs[1].append(
            pl.BlockSpec(block, lambda g, b, o, at=at: (0, o[jnp.where(g == 0, 0, b)], 0, at))
        )
        out_specs.append(pl.BlockSpec((m * q, width), lambda g, b, o: (g ^ o[n], b)))
        shapes.append(jax.ShapeDtypeStruct((2 * m * q, n * width), F32))
        operands[0].append(mine)
        operands[1].append(other)
        size += m * n * q * width
    return pl.pallas_call(
        partial(assemble_kernel, (len(rows), len(cols))),
        out_shape=tuple(shapes),
        grid_spec=pltpu.PrefetchScalarGridSpec(
            num_scalar_prefetch=1,
            grid=(2, n),
            in_specs=in_specs[0] + in_specs[1],
            out_specs=tuple(out_specs),
        ),
        compiler_params=pltpu.CompilerParams(vmem_limit_bytes=56 << 20),
        cost_estimate=pl.CostEstimate(flops=0, bytes_accessed=12 * size, transcendentals=0),
        name="assemble",
    )(order, *operands[0], *operands[1])


MESH_ID = pl.DeviceIdType.MESH


def back_kernel(n, m, nq, nk, scale, parts, *refs):
    (x_hbm, hidden_hbm, wo_hbm, wd_hbm, qkv_mine, qkv_other, mlp_mine, mlp_other,
     qkv_hbm, qr_hbm, kr_hbm, vb_hbm, o_hbm, normed_hbm, hn_hbm, act_hbm, dy_hbm, dpre_hbm,
     ag, mg, qg, kg, cos2, sin2, trow, tcol,
     output, grad_in, gain_out) = refs[:29]
    mines, others, away_v, fins, refs = refs[29:33], refs[33:37], refs[37:41], refs[41:45], refs[45:]
    (ups, downs, send_v,
     x_v, hidden, wo, qkv, qr, kr, vb, o, normed, hn, act, dy_all, dpre,
     part_s, part_r, out_r, dz_all, do, dqkv, wtile, dtile, gain_ref, sums,
     pair_s, pair_r, up_s, up_r, down_s, down_r,
     peer_s, peer_r, gup_s, gup_r, gdown_s, gdown_r, sib_s, sib_r, own_sem, gain_pair, gain_group,
     gain_line, gain_s, gain_r, in_sem, wt_sem, dhn_s, dhn_r, dz_s, dz_r, dn_s, dn_r, out_ss,
     out_rs) = refs
    rows, width = x_v.shape
    own = width // n
    half = own // 2
    ring = ups.shape[0]
    shard, rep = lax.axis_index("shard"), lax.axis_index("rep")
    i = rep // 2
    core = lax.rem(rep, 2)
    sibling = {"rep": 2 * i + 1 - core}
    above, below = {"rep": rep + 2}, {"rep": rep - 2}
    peers = [None] + [{"shard": shard ^ k} for k in range(1, n)]
    has_up, has_down = i < m - 1, i > 0

    barrier = pltpu.get_barrier_semaphore()

    def greet(dev):
        pl.semaphore_signal(barrier, inc=1, device_id=dev, device_id_type=MESH_ID)

    greet(sibling)
    for k in range(1, n):
        greet(peers[k])
    line = [None] + [{"rep": 2 * lax.rem(i + d, m) + core} for d in range(1, m)]
    for d in range(1, m):
        greet(line[d])

    loads = [
        pltpu.make_async_copy(src, dst, in_sem.at[f])
        for f, (src, dst) in enumerate(
            [
                (act_hbm, act), (dy_hbm, dy_all), (dpre_hbm, dpre), (hn_hbm, hn),
                (hidden_hbm, hidden), (wo_hbm, wo), (qkv_hbm, qkv), (qr_hbm, qr), (kr_hbm, kr),
                (vb_hbm, vb), (o_hbm, o), (normed_hbm, normed), (x_hbm, x_v),
            ]
        )
    ]
    for copy in loads:
        copy.start()
    pl.semaphore_wait(barrier, n + m - 1)

    def remote(src, dst, ssem, rsem, dev):
        return pltpu.make_async_remote_copy(
            src_ref=src, dst_ref=dst, send_sem=ssem, recv_sem=rsem,
            device_id=dev, device_id_type=MESH_ID,
        )

    def cols_of(p):
        return pl.ds(parts[p][3], parts[p][4])

    def chunk(p, j):
        seg, at = parts[p][:2]
        return away_v[seg].at[at, j, :, cols_of(p)]

    def fin(p):
        seg, at = parts[p][:2]
        return fins[seg].at[at, :, cols_of(p)]

    def out(refs, p, j):
        seg, at = parts[p][:2]
        return refs[seg].at[j, at, :, cols_of(p)]

    def pair_copy(p):
        seg, at = parts[p][:2]
        return remote(
            send_v.at[p % 3, :, :, pl.ds(0, parts[p][4])], away_v[seg].at[at, :, :, cols_of(p)],
            pair_s.at[p], pair_r.at[p], sibling,
        )

    def slot(ref, p, t):
        return ref.at[p % ring, t, :, pl.ds(0, parts[p][4])]

    def up_copy(p, t, src):
        return remote(src, slot(ups, p, t), up_s.at[p, t], up_r.at[p, t], above)

    def down_copy(p, t, src):
        return remote(src, slot(downs, p, t), down_s.at[p, t], down_r.at[p, t], below)

    def by_strips(size, body):
        step = 16
        pl.loop(0, size // step)(
            lambda b: body(pl.ds(pl.multiple_of(b * step, step), step))
        )

    def add_into(ref, other):
        def body(r):
            ref[r, :] = (ref[r, :].astype(F32) + other[r, :].astype(F32)).astype(BF)

        by_strips(ref.shape[0], body)

    def scatter_step(p, t):
        if t > 0:

            @pl.when((i > 0) & (i <= t) & has_up)
            def _():
                up_copy(p, t - 1, slot(ups, p, t - 1)).wait_recv()
                add_into(slot(ups, p, t - 1), chunk(p, m - 1 - t + i))

            @pl.when((i < m - 1) & (i >= m - 1 - t) & has_down)
            def _():
                down_copy(p, t - 1, slot(downs, p, t - 1)).wait_recv()
                add_into(slot(downs, p, t - 1), chunk(p, i - (m - 1 - t)))

            pl.when((i > 0) & (i <= t) & has_up)(
                lambda: up_copy(p, t, slot(ups, p, t - 1)).start()
            )
            pl.when((i < m - 1) & (i >= m - 1 - t) & has_down)(
                lambda: down_copy(p, t, slot(downs, p, t - 1)).start()
            )
        pl.when(i == 0)(lambda: up_copy(p, t, chunk(p, m - 1 - t)).start())
        pl.when(i == m - 1)(lambda: down_copy(p, t, chunk(p, t)).start())

    def peer_copy(p):
        return remote(chunk(p, i), fin(p), peer_s.at[p], peer_r.at[p], peers[parts[p][2]])

    def total(p):
        pl.when(has_down)(lambda: up_copy(p, m - 2, slot(ups, p, m - 2)).wait_recv())
        pl.when(has_up)(lambda: down_copy(p, m - 2, slot(downs, p, m - 2)).wait_recv())
        where = fin(p) if parts[p][2] == 0 else chunk(p, i)

        mine = chunk(p, i)

        def put(*extra):
            def body(r):
                value = mine[r, :].astype(F32)
                for e in extra:
                    value = value + e[r, :].astype(F32)
                where[r, :] = value.astype(BF)

            by_strips(mine.shape[0], body)

        u, d = slot(ups, p, m - 2), slot(downs, p, m - 2)
        pl.when(has_up & has_down)(lambda: put(u, d))
        pl.when(has_up & (i == 0))(lambda: put(d))
        pl.when(has_down & (i == m - 1))(lambda: put(u))
        if parts[p][2] != 0:
            peer_copy(p).start()

    def gup_copy(p, t, j, src):
        return remote(src, out(mines, p, j), gup_s.at[p, t], gup_r.at[p, t], above)

    def gdown_copy(p, t, j, src):
        return remote(src, out(mines, p, j), gdown_s.at[p, t], gdown_r.at[p, t], below)

    def sib_copy(p):
        seg, at = parts[p][:2]
        src = mines[seg].at[:, at, :, cols_of(p)]
        return remote(src, others[seg].at[:, at, :, cols_of(p)], sib_s.at[p], sib_r.at[p], sibling)

    def own_copy(p):
        return pltpu.make_async_copy(fin(p), out(mines, p, i), own_sem.at[p])

    def gather_step(p, t):
        if t == 0:
            for u in range(m - 1):
                pl.when((i <= u) & has_up)(lambda: up_copy(p, u, slot(ups, p, u)).wait_send())
                pl.when((i >= m - 1 - u) & has_down)(
                    lambda: down_copy(p, u, slot(downs, p, u)).wait_send()
                )
            if parts[p][2] != 0:
                peer_copy(p).wait_recv()
            pl.when(has_up)(lambda: gup_copy(p, 0, i, fin(p)).start())
            pl.when(has_down)(lambda: gdown_copy(p, 0, i, fin(p)).start())
            own_copy(p).start()
            return

        @pl.when(i - t >= 0)
        def _():
            here = out(mines, p, i - t)
            gup_copy(p, t - 1, i - t, here).wait_recv()
            if t < m - 1:
                pl.when(has_up)(lambda: gup_copy(p, t, i - t, here).start())

        @pl.when(i + t < m)
        def _():
            here = out(mines, p, i + t)
            gdown_copy(p, t - 1, i + t, here).wait_recv()
            if t < m - 1:
                pl.when(has_down)(lambda: gdown_copy(p, t, i + t, here).start())

        if t == m - 1:
            own_copy(p).wait()
            sib_copy(p).start()

    def gain_copies(level):
        if level == 0:
            return [remote(gain_ref, gain_pair, gain_s.at[0], gain_r.at[0], sibling)]
        if level == 1:
            return [
                remote(
                    gain_group.at[shard], gain_group.at[shard], gain_s.at[k], gain_r.at[k], peers[k]
                )
                for k in range(1, n)
            ]
        return [
            remote(
                gain_line.at[i], gain_line.at[i], gain_s.at[n - 1 + d], gain_r.at[n - 1 + d], line[d]
            )
            for d in range(1, m)
        ]

    def gains(level):
        if level > 0:
            for copy in gain_copies(level - 1):
                copy.wait_recv()
        if level == 1:
            gain_group[shard] = gain_ref[...] + gain_pair[...]
        elif level == 2:
            value = gain_group[0]
            for k in range(1, n):
                value = value + gain_group[k]
            gain_line[i] = value
        elif level == 3:
            value = gain_line[0]
            for k in range(1, m):
                value = value + gain_line[k]
            gain_out[...] = value
        if level < 3:
            for copy in gain_copies(level):
                copy.start()

    def over_tiles(p, body):
        start, cols = parts[p][3:]
        step = max(v for v in range(HD, 513, HD) if cols % v == 0)

        @pl.loop(0, cols // step)
        def _(b):
            to = pl.multiple_of(b * step, HD)
            body(pl.ds(pl.multiple_of(start + b * step, HD), step), pl.ds(to, step))

    def product(p, h, at):
        seg, place, k = parts[p][:3]
        if seg in (0, 2):
            ref = act if seg == 0 else o
            both = ref.shape[1] // 2
            start = (core if h == 0 else 1 - core) * both + place * half
            left = ref[:, pl.ds(pl.multiple_of(start, half), half)]
            right = (dy_all if seg == 0 else dz_all)[:, :, at].reshape(n * rows, at.size)
        else:
            left = (hn if seg == 1 else normed)[:, (h * n + k) * half : (h * n + k + 1) * half]
            right = (dpre if seg == 1 else dqkv)[:, at]
        return dot_first(left, right).reshape(m, half // m, at.size)

    def send(p):
        if p >= 3:
            pair_copy(p - 3).wait_send()

        def body(at, to):
            send_v[p % 3, :, :, to] = product(p, 1, at).astype(BF)

        over_tiles(p, body)
        pair_copy(p).start()

    def first(p):
        seg, place = parts[p][:2]
        pair_copy(p).wait_recv()

        def body(at, to):
            away_v[seg][place, :, :, at] = (
                product(p, 0, at) + away_v[seg][place, :, :, at].astype(F32)
            ).astype(BF)

        over_tiles(p, body)
        scatter_step(p, 0)

    def dhn_copy(k):
        return remote(part_s.at[k], part_r.at[k - 1], dhn_s.at[k], dhn_r.at[k], peers[k])

    def dn_copy(k):
        return remote(part_s.at[k], part_r.at[k - 1], dn_s.at[k], dn_r.at[k], peers[k])

    def out_copy(k):
        return remote(part_s.at[k], out_r.at[k - 1], out_ss.at[k], out_rs.at[k], peers[k])

    def dz_copy(k):
        return remote(dz_all.at[0], dz_all.at[k], dz_s.at[k], dz_r.at[k], peers[k])

    strip = min(rows, 32)

    def strips(body):
        pl.loop(0, rows // strip)(
            lambda b: body(pl.ds(pl.multiple_of(b * strip, strip), strip))
        )

    def add_gain(at, value):
        for b in range(value.shape[1] // HD):
            gain_ref[at + b : at + b + 1, :] += value[:, b * HD : (b + 1) * HD]

    def norm_back(values, gain, at, result):
        def body(r):
            v = values[r, :].astype(F32)
            rstat = lax.rsqrt(jnp.mean(v * v, -1, keepdims=True) + EPSILON)
            scaled = v * rstat
            grad = part_s[0, r, :].astype(F32)
            for k in range(1, n):
                grad = grad + part_r[k - 1, r, :].astype(F32)
            add_gain(at, jnp.sum(grad * scaled, 0, keepdims=True))
            weighted = grad * gain[...]
            result(
                r, rstat * (weighted - scaled * jnp.mean(weighted * scaled, -1, keepdims=True))
            )

        strips(body)

    def partial_rows(grads, mine, other, turn):
        cols = grads.shape[1]

        def tile_copy(b):
            src = (mine if b < n else other).at[b % n]
            return pltpu.make_async_copy(
                src, wtile.at[b % 2, :, :, pl.ds(0, cols)], wt_sem.at[b % 2]
            )

        if turn == 0:
            tile_copy(0).start()
            tile_copy(1).start()
        tile_copy(2 * turn).wait()
        tile_copy(2 * turn + 1).wait()
        h, first_k = 2 * turn // n, 2 * turn % n

        @pl.loop(0, 2 * n)
        def _(f):
            b, k = f // n, lax.rem(f, n)
            at = (shard ^ (first_k + b)) * own + (core if h == 0 else 1 - core) * half
            at = pl.ds(pl.multiple_of(at, half), half)
            tokens = pl.ds(pl.multiple_of(k * rows, rows), rows)
            w = wtile[b, :, :, :cols].reshape(half, cols)
            part_s[k, :, at] = dot_last(grads[tokens, :], w).astype(BF)

        if turn < n - 1:
            tile_copy(2 * turn + 2).start()
            tile_copy(2 * turn + 3).start()

    def hook_dhn(turn):
        if turn == 0:
            loads[2].wait()
        partial_rows(dpre, mlp_mine, mlp_other, turn)
        if turn == n - 1:
            for k in range(1, n):
                dhn_copy(k).start()

    def hook_hidden():
        loads[4].wait()
        for k in range(1, n):
            dhn_copy(k).wait_recv()
        gain_ref[...] = jnp.zeros_like(gain_ref)

        def result(r, value):
            value = dy_all[0, r, :].astype(F32) + value
            grad_in[r, :] = value
            dz_all[0, r, :] = value.astype(BF)

        norm_back(hidden, mg, width // HD, result)
        for k in range(1, n):
            dz_copy(k).start()

    def hook_do():
        for copy in loads[5:]:
            copy.wait()
        for k in range(1, n):
            dz_copy(k).wait_recv()

        @pl.loop(0, n)
        def _(k):
            tokens = pl.ds(pl.multiple_of(k * rows, rows), rows)
            do[tokens, :] = dot_last(dz_all[k], wo[...]).astype(BF)

    def hook_head(j):
        attend_back_pair(
            j, nq, nk, qkv, qr, kr, vb, do, dqkv, qg, kg, cos2, sin2, trow, tcol, scale, sums,
            lambda f, value: add_gain(2 * width // HD + f, value),
        )

    def hook_normed(turn):
        if turn == 0:
            for k in range(1, n):
                out_copy(k).wait_send()
        partial_rows(dqkv, qkv_mine, qkv_other, turn)
        if turn == n - 1:
            for k in range(1, n):
                dn_copy(k).start()

    def hook_input():
        for k in range(1, n):
            dn_copy(k).wait_recv()

        def result(r, value):
            grad_in[r, :] = grad_in[r, :] + value

        norm_back(x_v, ag, 0, result)

    def hook_down(turn):
        if turn == 0:
            for k in range(1, n):
                dhn_copy(k).wait_send()
        step = dtile.shape[2]

        def tile_copy(b):
            return pltpu.make_async_copy(
                wd_hbm.at[:, pl.ds(b * step, step)], dtile.at[b % 2], wt_sem.at[b % 2]
            )

        count = width // step
        if turn == 0:
            tile_copy(0).start()
        for b in range(turn * count // 2, (turn + 1) * count // 2):
            tile_copy(b).wait()
            if b + 1 < count:
                tile_copy(b + 1).start()

            @pl.loop(0, n)
            def _(k):
                tokens = pl.ds(pl.multiple_of(k * rows, rows), rows)
                part_s[k, :, b * step : (b + 1) * step] = dot(
                    act[tokens, :], dtile[b % 2]
                ).astype(BF)

        if turn == 1:
            for k in range(1, n):
                out_copy(k).start()

    def hook_output():
        for k in range(1, n):
            out_copy(k).wait_recv()

        def body(r):
            value = hidden[r, :] + part_s[0, r, :].astype(F32)
            for k in range(1, n):
                value = value + out_r[k - 1, r, :].astype(F32)
            output[r, :] = value.astype(BF)

        strips(body)

    at_tick = {}
    def plan(tick, *pieces):
        for f, piece in enumerate(pieces):
            at_tick.setdefault(tick + f, []).append(piece)

    plan(DHN_TICK, *[partial(hook_dhn, turn) for turn in range(n)])
    tick = DHN_TICK + n + 2
    plan(tick, hook_hidden, partial(hook_down, 0), partial(hook_down, 1), hook_do)
    tick += 4
    plan(tick, *[partial(hook_head, j) for j in range(nk)])
    plan(tick + nk, hook_output, *[partial(hook_normed, turn) for turn in range(n)])
    tick += nk + n + 3
    plan(tick, hook_input, *[partial(gains, level) for level in range(4)])

    stages = [first] + [lambda p, t=t: scatter_step(p, t) for t in range(1, m - 1)]
    stages += [total] + [lambda p, t=t: gather_step(p, t) for t in range(m)]

    loads[0].wait()
    loads[1].wait()
    send(0)
    send(1)
    ticks = len(parts) + len(stages) - 1
    for tick in range(max(ticks, max(at_tick) + 1)):
        if tick == 0:
            loads[3].wait()
        for st in range(len(stages) - 1, -1, -1):
            p = tick - st
            if 0 <= p < len(parts):
                stages[st](p)
        for hook in at_tick.get(tick, []):
            hook()
        if tick + 2 < len(parts):
            send(tick + 2)

    for k in range(1, n):
        dz_copy(k).wait_send()
        dn_copy(k).wait_send()
    for level in range(3):
        for copy in gain_copies(level):
            copy.wait_send()
    for p in range(len(parts)):
        if p >= len(parts) - 3:
            pair_copy(p).wait_send()
        if parts[p][2] != 0:
            peer_copy(p).wait_send()
        for t in range(m - 1):
            pl.when((i - t >= 0) & has_up)(lambda: gup_copy(p, t, i, fin(p)).wait_send())
            pl.when((i + t < m) & has_down)(lambda: gdown_copy(p, t, i, fin(p)).wait_send())
        sib_copy(p).wait_send()
        sib_copy(p).wait_recv()


def back(n, m, nq, nk, x, hidden, wo, wd, weights, qkv, heads, o, normed, hn, act, dy_all, dpre,
         gains, tables):
    rows, width = x.shape
    length = n * rows
    q, cols = weights[0].shape[2:]
    wide = dpre.shape[1]
    half = m * q
    dma = pltpu.SemaphoreType.DMA
    sd = jax.ShapeDtypeStruct
    hbm, vmem = pl.BlockSpec(memory_space=pl.ANY), pl.BlockSpec(memory_space=pltpu.VMEM)
    segments = [
        (act.shape[1] // 2 // half, m, q, width), (n, m, q, wide),
        (nq * HD // 2 // half, m, q, width), (n, m, q, cols),
    ]

    def cut(seg, at, k, sizes):
        out, c = [], 0
        for size in sizes:
            out.append((seg, at, k, c, size))
            c += size
        return out

    parts = cut(0, 0, 0, [width // 4, width // 4, width // 2])
    for a in range(1, segments[0][0]):
        parts += cut(0, a, 0, [width // 2] * 2)
    for k in range(n):
        parts += cut(1, k, k, [wide // 3] * 3)
    for a in range(segments[2][0]):
        parts += cut(2, a, 0, [width // 2] * 2)
    for k in range(n):
        parts += cut(3, k, k, [cols] if k < n - 1 else [cols // 2] * 2)
    total = len(parts)
    most = max(part[4] for part in parts)
    ring = m + 2
    count = 2 * width // HD + 2
    gain_shape = (count + -count % 8, HD)
    outs = [sd((m, v[0]) + v[2:], BF) for v in segments]
    like = lambda v: pltpu.VMEM(v.shape, v.dtype)
    operands = [x, hidden, wo, wd, *weights, qkv, *heads, o, normed, hn, act, dy_all, dpre]
    return pl.pallas_call(
        partial(back_kernel, n, m, nq, nk, 1.0 / math.sqrt(HD), parts),
        out_shape=tuple(
            [sd((rows, width), BF), sd((rows, width), F32), sd(gain_shape, F32)] + outs + outs
        ),
        in_specs=[hbm] * len(operands) + [vmem] * 8,
        out_specs=tuple([vmem] * 3 + [hbm] * 8),
        scratch_shapes=[pltpu.VMEM(v, BF) for v in segments]
        + [pltpu.VMEM(v[:1] + v[2:], BF) for v in segments]
        + [pltpu.VMEM((ring, m - 1, q, most), BF)] * 2
        + [pltpu.VMEM((3, m, q, most), BF)]
        + [like(v) for v in (x, hidden, wo, qkv, *heads, o, normed, hn, act, dy_all, dpre)]
        + [
            pltpu.VMEM((n, rows, width), BF), pltpu.VMEM((n - 1, rows, width), BF),
            pltpu.VMEM((n - 1, rows, width), BF), pltpu.VMEM((n, rows, width), BF),
            pltpu.VMEM((length, nq * HD), BF), pltpu.VMEM((length, cols), BF),
            pltpu.VMEM((2, m, q, wide), BF), pltpu.VMEM((2, wd.shape[0], 256), BF),
            pltpu.VMEM(gain_shape, F32), pltpu.VMEM((3, length, HD), F32),
            dma((total,)), dma((total,)),
            dma((total, m - 1)), dma((total, m - 1)), dma((total, m - 1)), dma((total, m - 1)),
            dma((total,)), dma((total,)),
            dma((total, m - 1)), dma((total, m - 1)), dma((total, m - 1)), dma((total, m - 1)),
            dma((total,)), dma((total,)), dma((total,)),
            pltpu.VMEM(gain_shape, F32), pltpu.VMEM((n,) + gain_shape, F32),
            pltpu.VMEM((m,) + gain_shape, F32), dma((n + m,)), dma((n + m,)),
            dma((13,)), dma((2,)),
        ]
        + [dma((n,))] * 8,
        compiler_params=pltpu.CompilerParams(
            collective_id=3, has_side_effects=True, vmem_limit_bytes=67043328
        ),
        name="back",
    )(*operands, *gains, *tables)


def front_kernel(
    n, m, nq, nk, scale,
    x_hbm, dy_hbm, wq, wk, wv, wg, wu, wo_hbm,
    ag, qg, kg, mg, cos2, sin2, trow, tcol,
    normed_hbm, qkv_hbm, qr_hbm, kr_hbm, vb_hbm, o_hbm, hidden_hbm, hn_hbm,
    qkv_mine_hbm, qkv_other_hbm, mlp_mine, mlp_other, dy_all,
    normed, qkv, qr, kr, vb, o, hidden, hn, qkv_mine, qkv_other,
    x_all, wo, bounce, dy_v, hn_all, part_own, part_s, part_r,
    x_ss, x_rs, w_ss, w_rs, up_ss, up_rs, down_ss, down_rs, sib_ss, sib_rs,
    own_sem, back_sem, load_sem, part_ss, part_rs, hn_ss, hn_rs, dy_ss, dy_rs, store_sem
):
    shard, rep = lax.axis_index("shard"), lax.axis_index("rep")
    i = rep // 2
    core = lax.rem(rep, 2)
    sibling = {"rep": 2 * i + 1 - core}
    above, below = {"rep": rep + 2}, {"rep": rep - 2}
    peers = [None] + [{"shard": shard ^ k} for k in range(1, n)]
    has_up, has_down = i < m - 1, i > 0
    rows, width = x_all.shape[1], x_all.shape[2]
    own = width // n
    half = own // 2

    barrier = pltpu.get_barrier_semaphore()

    def greet(dev):
        pl.semaphore_signal(barrier, inc=1, device_id=dev, device_id_type=MESH_ID)

    greet(sibling)
    for k in range(1, n):
        greet(peers[k])
    for d in range(1, m):
        greet({"rep": 2 * lax.rem(i + d, m) + core})
    pl.semaphore_wait(barrier, n + m - 1)

    def remote(src, dst, ssem, rsem, dev):
        return pltpu.make_async_remote_copy(
            src_ref=src, dst_ref=dst, send_sem=ssem, recv_sem=rsem,
            device_id=dev, device_id_type=MESH_ID,
        )

    results = [
        (normed, normed_hbm), (qkv_mine, qkv_mine_hbm), (qkv_other, qkv_other_hbm),
        (qkv, qkv_hbm), (qr, qr_hbm), (kr, kr_hbm), (vb, vb_hbm), (o, o_hbm), (hidden, hidden_hbm),
    ] + [(hn.at[pl.ds(k * rows, rows)], hn_hbm.at[pl.ds(k * rows, rows)]) for k in range(n)]
    stores = [
        pltpu.make_async_copy(src, dst, store_sem.at[f]) for f, (src, dst) in enumerate(results)
    ]

    ffl = wg.shape[3] // n
    groups = [
        ([wq, wk, wv], qkv_mine, qkv_other, 0, qkv.shape[1]),
        ([wg], mlp_mine, mlp_other, 0, ffl),
        ([wu], mlp_mine, mlp_other, ffl, ffl),
    ]

    def fields(g):
        weights, _, _, at, _ = groups[g]
        for w in weights:
            size = w.shape[3] // n
            yield w, at, size
            at += size

    def cols_of(k, size):
        return pl.ds(pl.multiple_of((shard ^ k) * size, size), size)

    def piece_copies(g, k):
        mine = groups[g][1]
        return [
            remote(
                w.at[core, i, :, cols_of(k, size)],
                mine.at[k, i, :, pl.ds(at, size)],
                w_ss.at[g, k, f], w_rs.at[g, k, f], peers[k],
            )
            for f, (w, at, size) in enumerate(fields(g))
        ]

    def own_copies(g):
        mine, other = groups[g][1:3]
        out = []
        for h, dst in enumerate((mine, other)):
            for f, (w, at, size) in enumerate(fields(g)):
                to = dst.at[0, :, :, pl.ds(at, size)] if g == 0 else bounce.at[h, :, :, pl.ds(at, size)]
                src = w.at[core if h == 0 else 1 - core, :, :, cols_of(0, size)]
                out.append(pltpu.make_async_copy(src, to, own_sem.at[g, h, f]))
        return out

    def back_copies():
        return [
            pltpu.make_async_copy(bounce.at[h], dst.at[0], back_sem.at[h])
            for h, dst in enumerate((mlp_mine, mlp_other))
        ]

    def region(g, ref, j):
        at, size = groups[g][3:]
        return ref.at[pl.ds(1, n - 1), j, :, pl.ds(at, size)]

    def up_copy(g, t, j):
        r = region(g, groups[g][1], j)
        return remote(r, r, up_ss.at[g, t], up_rs.at[g, t], above)

    def down_copy(g, t, j):
        r = region(g, groups[g][1], j)
        return remote(r, r, down_ss.at[g, t], down_rs.at[g, t], below)

    def sib_copy(g, j):
        mine, other = groups[g][1:3]
        return remote(region(g, mine, j), region(g, other, j), sib_ss.at[g, j], sib_rs.at[g, j], sibling)

    def gather_weights(g, t):
        if t == 0:
            for k in range(1, n):
                for copy in piece_copies(g, k):
                    copy.wait_recv()
            pl.when(has_up)(lambda: up_copy(g, 0, i).start())
            pl.when(has_down)(lambda: down_copy(g, 0, i).start())
            sib_copy(g, i).start()
            return

        @pl.when(i - t >= 0)
        def _():
            up_copy(g, t - 1, i - t).wait_recv()
            if t < m - 1:
                pl.when(has_up)(lambda: up_copy(g, t, i - t).start())
            sib_copy(g, i - t).start()

        @pl.when(i + t < m)
        def _():
            down_copy(g, t - 1, i + t).wait_recv()
            if t < m - 1:
                pl.when(has_down)(lambda: down_copy(g, t, i + t).start())
            sib_copy(g, i + t).start()

    def x_copy(k):
        return remote(x_hbm, x_all.at[k], x_ss.at[k], x_rs.at[k], peers[k])

    def dy_copy(k):
        return remote(dy_hbm, dy_all.at[k], dy_ss.at[k], dy_rs.at[k], peers[k])

    def hn_copy(k):
        return remote(hn_all.at[0], hn_all.at[k], hn_ss.at[k], hn_rs.at[k], peers[k])

    def part_copy(k):
        return remote(part_s.at[k], part_r.at[k], part_ss.at[k], part_rs.at[k], peers[k])

    load_x = pltpu.make_async_copy(x_hbm, x_all.at[0], load_sem.at[0])
    load_wo = pltpu.make_async_copy(wo_hbm, wo, load_sem.at[1])
    load_dy = pltpu.make_async_copy(dy_hbm, dy_v, load_sem.at[2])
    keep_dy = pltpu.make_async_copy(dy_v, dy_all.at[0], load_sem.at[3])

    def start_pieces(g):
        for k in range(1, n):
            for copy in piece_copies(g, k):
                copy.start()

    load_x.start()
    start_pieces(0)
    start_pieces(1)
    for k in range(1, n):
        x_copy(k).start()
    for copy in own_copies(0):
        copy.start()
    start_pieces(2)
    for k in range(1, n):
        dy_copy(k).start()
    load_wo.start()
    for g in (1, 2):
        for copy in own_copies(g):
            copy.start()
    load_dy.start()

    def place(k, h, kk):
        return pl.ds(
            pl.multiple_of((shard ^ kk) * own + (core if h == 0 else 1 - core) * half, half), half
        )

    hops = [(1, t) for t in range(1, m)] + [(2, t) for t in range(m)]
    hops.sort(key=lambda v: 2 * v[1] + v[0])

    def next_hops(count):
        for _ in range(min(count, len(hops))):
            gather_weights(*hops.pop(0))

    gather_weights(0, 0)
    for k in range(n):
        if k == 0:
            load_x.wait()
        else:
            x_copy(k).wait_recv()
        v = x_all[k].astype(F32)
        r = lax.rsqrt(jnp.mean(v * v, -1, keepdims=True) + EPSILON)
        for h in range(2):
            for kk in range(n):
                at = place(k, h, kk)
                normed[k * rows : (k + 1) * rows, (h * n + kk) * half : (h * n + kk + 1) * half] = (
                    x_all[k, :, at].astype(F32) * r * ag[:, at]
                ).astype(BF)
        if k + 1 < m - 1:
            gather_weights(0, k + 1)
        if k == min(n, m - 1) - 1:
            gather_weights(1, 0)
    for t in range(n + 1, m - 1):
        gather_weights(0, t)
    stores[0].start()
    gather_weights(0, m - 1)
    for copy in own_copies(0):
        copy.wait()
    for j in range(m):
        sib_copy(0, j).wait_recv()
    stores[1].start()
    stores[2].start()

    cols = qkv.shape[1]
    step = min(cols, 256)

    @pl.loop(0, cols // step)
    def _(b):
        at = pl.ds(pl.multiple_of(b * step, step), step)
        both = n * half
        qkv[:, at] = dot(
            normed[:, :both], qkv_mine[:, :, :, at].reshape(both, step)
        ) + dot(normed[:, both:], qkv_other[:, :, :, at].reshape(both, step))

    stores[3].start()
    for g in (1, 2):
        for copy in own_copies(g):
            copy.wait()
    for copy in back_copies():
        copy.start()
    load_dy.wait()
    keep_dy.start()
    for j in range(nk):
        attend_pair(qkv, j, nq, nk, qg, kg, cos2, sin2, trow, tcol, o, qr, kr, vb, scale)
        if j == 0:
            next_hops(2)
    for f in range(4, 8):
        stores[f].start()

    load_wo.wait()
    step = min(width, 512)

    @pl.loop(0, width // step)
    def _(b):
        at = pl.ds(pl.multiple_of(b * step, step), step)
        for k in range(n):
            value = dot(o[k * rows : (k + 1) * rows, :], wo[:, at])
            if k == 0:
                part_own[:, at] = value
            else:
                part_s[k, :, at] = value.astype(BF)

    for k in range(1, n):
        part_copy(k).start()
    next_hops(2)
    total = x_all[0].astype(F32) + part_own[...]
    for k in range(1, n):
        part_copy(k).wait_recv()
        total = total + part_r[k].astype(F32)
    hidden[...] = total
    stores[8].start()
    r = lax.rsqrt(jnp.mean(total * total, -1, keepdims=True) + EPSILON)
    hn_all[0] = (total * r * mg[...]).astype(BF)
    for k in range(1, n):
        hn_copy(k).start()
    next_hops(len(hops) - 1)
    for k in range(n):
        if k > 0:
            hn_copy(k).wait_recv()
        for h in range(2):
            for kk in range(n):
                hn[k * rows : (k + 1) * rows, (h * n + kk) * half : (h * n + kk + 1) * half] = (
                    hn_all[k, :, place(k, h, kk)]
                )
        stores[9 + k].start()
    next_hops(len(hops))

    for copy in back_copies() + stores:
        copy.wait()
    keep_dy.wait()
    for k in range(1, n):
        for g in range(3):
            for copy in piece_copies(g, k):
                copy.wait_send()
        x_copy(k).wait_send()
        part_copy(k).wait_send()
        hn_copy(k).wait_send()
        dy_copy(k).wait_send()
        dy_copy(k).wait_recv()
    for g in range(3):
        for j in range(m):
            sib_copy(g, j).wait_send()
            if g > 0:
                sib_copy(g, j).wait_recv()
        for t in range(m - 1):
            pl.when((i - t >= 0) & has_up)(lambda: up_copy(g, t, i).wait_send())
            pl.when((i + t < m) & has_down)(lambda: down_copy(g, t, i).wait_send())


def front(n, m, nq, nk, x, dy, weights, wo, gains, tables):
    rows, width = x.shape
    length = n * rows
    q = weights[0].shape[2]
    cols = [sum(w.shape[3] // n for w in ws) for ws in (weights[:3], weights[3:])]
    vmem, hbm = pl.BlockSpec(memory_space=pltpu.VMEM), pl.BlockSpec(memory_space=pl.ANY)
    dma = pltpu.SemaphoreType.DMA
    sd = jax.ShapeDtypeStruct
    outs = [
        sd((length, width), BF),
        sd((length, cols[0]), F32),
        sd((length, nq * HD), BF),
        sd((length, nk * HD), BF),
        sd((length, nk * HD), BF),
        sd((length, nq * HD), BF),
        sd((rows, width), F32),
        sd((length, width), BF),
        sd((n, m, q, cols[0]), BF),
        sd((n, m, q, cols[0]), BF),
        sd((n, m, q, cols[1]), BF),
        sd((n, m, q, cols[1]), BF),
        sd((n, rows, width), BF),
    ]
    return pl.pallas_call(
        partial(front_kernel, n, m, nq, nk, 1.0 / math.sqrt(HD)),
        out_shape=tuple(outs),
        in_specs=[hbm] * 8 + [vmem] * 8,
        out_specs=tuple([hbm] * len(outs)),
        scratch_shapes=[pltpu.VMEM(v.shape, v.dtype) for v in outs[:10]]
        + [
            pltpu.VMEM((n, rows, width), BF),
            pltpu.VMEM(wo.shape, BF),
            pltpu.VMEM((2, m, q, cols[1]), BF),
            pltpu.VMEM((rows, width), BF),
            pltpu.VMEM((n, rows, width), BF),
            pltpu.VMEM((rows, width), F32),
            pltpu.VMEM((n, rows, width), BF),
            pltpu.VMEM((n, rows, width), BF),
            dma((n,)), dma((n,)),
            dma((3, n, 3)), dma((3, n, 3)),
            dma((3, m)), dma((3, m)), dma((3, m)), dma((3, m)), dma((3, m)), dma((3, m)),
            dma((3, 2, 3)), dma((2,)), dma((4,)),
            dma((n,)), dma((n,)), dma((n,)), dma((n,)), dma((n,)), dma((n,)), dma((9 + n,)),
        ],
        compiler_params=pltpu.CompilerParams(
            collective_id=1, has_side_effects=True, vmem_limit_bytes=60 << 20
        ),
        name="front",
    )(x, dy, *weights, wo, *gains, *tables)


def build(n, reps):
    m = reps // 2

    def per_device(
        activations, segments, attn_gain, query_weight, key_weight, value_weight,
        query_gain, key_gain, out_weight, mlp_gain, gate_weight, up_weight, down_weight,
        cotangent,
    ):
        rows, width = activations.shape[1], activations.shape[2]
        length = segments.shape[1]
        shard = lax.axis_index("shard")
        core = lax.axis_index("rep") % 2
        own = width // n
        half = own // 2
        nq, nk = HQ // n, HK // n
        ffl = FF // n
        owner = [shard ^ k for k in range(n)]

        def cut(v, start, size, axis):
            return lax.dynamic_slice_in_dim(v, start, size, axis)

        def times(v, w):
            both = v.shape[1] // 2
            return dot(v[:, :both], w[0]) + dot(v[:, both:], w[1])

        seg_ids = segments[0]
        pos = positions(seg_ids)
        tokens = jnp.arange(length, dtype=jnp.int32)
        shuffle = lambda v: jnp.concatenate([cut(v, owner[k] * rows, rows, 0) for k in range(n)])
        index, seg_ids, pos = shuffle(tokens), shuffle(seg_ids), shuffle(pos)
        inv_freq = 1.0 / ROPE_BASE ** (jnp.arange(HD // 2, dtype=F32) * (2.0 / HD))
        angles = pos[:, None] * inv_freq[None, :]
        cosine, sine = jnp.cos(angles), jnp.sin(angles)
        cos2 = jnp.concatenate([cosine, cosine], 1)
        sin2 = jnp.concatenate([-sine, sine], 1)
        tcol = jnp.stack([index, seg_ids], 0)
        trow = jnp.stack([index, seg_ids], 1)
        qg, kg = query_gain[None], key_gain[None]

        cut_rows = lambda w: w.reshape(2, m, half // m, w.shape[1])
        (
            normed, qkv, qr, kr, vb, attn_out, hidden, normed_mlp,
            qkv_mine, qkv_other, mlp_mine, mlp_other, all_grads,
        ) = front(
            n, m, nq, nk, activations[0], cotangent[0],
            [cut_rows(w) for w in (query_weight, key_weight, value_weight, gate_weight, up_weight)],
            out_weight,
            [attn_gain[None], qg, kg, mlp_gain[None]],
            [cos2, sin2, trow, tcol],
        )
        w_mlp = [v.reshape(n * half, -1) for v in (mlp_mine, mlp_other)]
        flat_grads = all_grads.reshape(length, width)
        pre = times(normed_mlp, w_mlp)
        gate_pre, up_pre = pre[:, :ffl], pre[:, ffl:]
        sig = jax.nn.sigmoid(gate_pre)
        activated = (gate_pre * sig * up_pre).astype(BF)
        grad_act = dot_last(flat_grads, down_weight)
        grad_gate = (grad_act * up_pre * sig * (1.0 + gate_pre * (1.0 - sig))).astype(BF)
        grad_up = (grad_act * gate_pre * sig).astype(BF)
        grad_pre = jnp.concatenate([grad_gate, grad_up], 1)
        output, grad_input, gains, *summed = back(
            n, m, nq, nk, activations[0], hidden, out_weight, down_weight,
            [qkv_mine, qkv_other, mlp_mine, mlp_other], qkv, [qr, kr, vb], attn_out, normed,
            normed_mlp, activated, all_grads, grad_pre,
            [attn_gain[None], mlp_gain[None], qg, kg], [cos2, sin2, trow, tcol],
        )
        output, grad_input = output[None], grad_input[None]
        mines, others = summed[:4], summed[4:]

        pick = lambda seg, at=None, width=None: (
            (mines[seg], others[seg]) if at is None else (mines[seg], others[seg], at, width)
        )
        (
            grad_down, grad_out_weight, grad_gate_weight, grad_up_weight,
            grad_query_weight, grad_key_weight, grad_value_weight,
        ) = assemble(
            [pick(0), pick(2)],
            [
                pick(1, 0, ffl), pick(1, 1, ffl), pick(3, 0, nq * HD),
                pick(3, nq // nk, nk * HD), pick(3, nq // nk + 1, nk * HD),
            ],
            core,
            owner,
        )
        gains = gains.reshape(-1)
        grad_attn_gain, grad_mlp_gain = gains[:width], gains[width : 2 * width]
        grad_query_gain = gains[2 * width : 2 * width + HD]
        grad_key_gain = gains[2 * width + HD : 2 * width + 2 * HD]
        return (
            output,
            grad_input,
            grad_attn_gain,
            grad_query_weight,
            grad_key_weight,
            grad_value_weight,
            grad_query_gain,
            grad_key_gain,
            grad_out_weight,
            grad_mlp_gain,
            grad_gate_weight,
            grad_up_weight,
            grad_down,
        )

    return per_device


def solution(mesh):
    tok = P("rep", "shard", None)
    row = P("shard", None)
    return jax.shard_map(
        build(mesh.shape["shard"], mesh.shape["rep"]),
        mesh=mesh,
        in_specs=(
            tok, P("rep", None), P(), row, row, row, P(), P(), row, P(), row, row, row, tok,
        ),
        out_specs=(tok, tok, P(), row, row, row, P(), P(), row, P(), row, row, row),
        check_vma=False,
    )
```
